128 devices in a mesh: gx: 8 (over y, core), gy: 16 (over z, x).
Axes of the slice: x: 4, y: 4, z: 4, core: 2. Of those that a mesh axis runs over, the one named last changes fastest.
Arguments:
- spectra: bfloat16 [8, 16, 3, 2, 128, 4096], P('gx', 'gy'), may hold values from -1000 to 1000
- partner_codes: int32 [8, 16, 5], P('gx', 'gy'), may hold values from -1 to 4, as said below
- range_bits: int32 [8, 16, 5, 128, 5], P('gx', 'gy'), may hold values from 0 to 1073741823
- old_stacks: float32 [8, 16, 5, 8, 2, 128, 128], P('gx', 'gy'), may hold values from -6 to 6
Outputs:
- stacks: float32 [8, 16, 5, 8, 2, 128, 128], P('gx', 'gy')
The draws below stay inside these ranges and needn't reach their ends.
Inputs may be any that keep to these rules, and one draw needn't show every extreme that they name: `partner_codes`: each block lists code 0 first, then further distinct codes in increasing order, then -1 in the remaining slots; no listed code names a block outside the grid of 8 x 16 blocks; some block lists all 5 codes.
All inputs are finite; a program needn't handle non-finite values.
Results may differ from the reference program's by a relative error of at most 0.0014.
Values may be sent and summed in bfloat16 or wider, within the bound.
A program may use at most 192 MiB of HBM per device.

```python
import math
import jax
import jax.numpy as jnp
from jax import lax

ST = 128
F = 4096
BANDS = 8
SLOTS = 5
SEG = 3
BW = 512
WORDS = 5
NBX = 8
NBY = 16


def draw_spectra(key, part):
    first_key = jax.random.fold_in(key, 11)
    second_key = jax.random.fold_in(key, 12)
    third_key = jax.random.fold_in(key, 13)
    full_shape = (NBX, NBY, SEG, 2, ST, F)
    base_noise = jax.random.truncated_normal(first_key, -6.0, 6.0, full_shape, jnp.float32)
    spread = math.log(10.0)
    bin_scale = jnp.exp(spread * jax.random.uniform(second_key, (NBX, NBY, SEG, 1, ST, F), jnp.float32))
    band_scale = jnp.exp(math.log(10.0) * jax.random.uniform(third_key, (NBX, NBY, 1, 1, ST, BANDS, 1), jnp.float32))
    band_full = jnp.broadcast_to(band_scale, (NBX, NBY, 1, 1, ST, BANDS, BW)).reshape(NBX, NBY, 1, 1, ST, F)
    return (base_noise * bin_scale * band_full).astype(jnp.bfloat16)


def draw_partner_codes(key, part):
    row_pos = jnp.arange(NBX, dtype=jnp.int32)[:, None]
    col_pos = jnp.arange(NBY, dtype=jnp.int32)[None, :]
    first_level = jax.random.randint(jax.random.fold_in(key, 21), (NBX, NBY), 0, 10, dtype=jnp.int32)
    second_level = jax.random.randint(jax.random.fold_in(key, 22), (NBX, NBY), 0, 10, dtype=jnp.int32)
    density = first_level * second_level + first_level + second_level + 1
    trials = jax.random.randint(jax.random.fold_in(key, 23), (NBX, NBY, 4), 0, 100, dtype=jnp.int32)
    forced_row = jax.random.randint(jax.random.fold_in(key, 24), (), 1, NBX - 1, dtype=jnp.int32)
    forced_col = jax.random.randint(jax.random.fold_in(key, 25), (), 0, NBY - 1, dtype=jnp.int32)
    forced = (row_pos == forced_row) & (col_pos == forced_col)
    step_rows = [1, -1, 0, 1]
    step_cols = [0, 1, 1, 1]
    listed = [jnp.ones((NBX, NBY), dtype=bool)]
    for which in range(4):
        target_row = row_pos + step_rows[which]
        target_col = col_pos + step_cols[which]
        inside = (target_row >= 0) & (target_row < NBX) & (target_col < NBY)
        listed.append(inside & ((trials[:, :, which] < density) | forced))
    valid = jnp.stack(listed, -1).astype(jnp.int32)
    ranks = jnp.cumsum(valid, -1) - 1
    counts = jnp.sum(valid, -1)
    code_values = jnp.arange(5, dtype=jnp.int32)
    slots_out = []
    for slot_index in range(SLOTS):
        matched = valid * (ranks == slot_index).astype(jnp.int32)
        chosen = jnp.sum(matched * code_values, -1)
        slots_out.append(jnp.where(counts > slot_index, chosen, -1).astype(jnp.int32))
    return jnp.stack(slots_out, -1)


def touch_ends(drawn, key, smallest, largest):
    spot = [jax.random.randint(jax.random.fold_in(key, axis), (), 0, length) for axis, length in enumerate(drawn.shape)]
    widest = drawn.shape.index(max(drawn.shape))
    neighbour = spot[:widest] + [(spot[widest] + 1) % drawn.shape[widest]] + spot[widest + 1:]
    return drawn.at[tuple(spot)].set(smallest).at[tuple(neighbour)].set(largest)


def shard_levels(rng, extent, pieces, smallest, top_value):
    loudness, own = 1.0, jax.random.fold_in(rng, 6)
    for axis_at, shards_of in pieces:
        heights = jnp.exp(jax.random.uniform(jax.random.fold_in(own, axis_at), (shards_of,), jnp.float32, smallest / len(pieces), top_value / len(pieces)))
        loudness = loudness * jnp.repeat(heights, extent[axis_at] // shards_of).reshape([-1 if axis == axis_at else 1 for axis in range(len(extent))])
    return loudness


def centred(own_key, dims, width, limit, cuts=(), kind=jnp.bfloat16):
    array = width * jax.random.normal(own_key, dims, jnp.float32)
    if cuts:
        array = array * shard_levels(own_key, dims, cuts, -0.22, 0.18)
    return jnp.clip(array, -limit, limit).astype(kind)


def setup_inputs(seed: int = 0) -> dict:
    keys = jax.random.split(jax.random.key(seed), 5)
    return {
        "spectra": draw_spectra(jax.random.fold_in(keys[4], 71), 0),
        "partner_codes": draw_partner_codes(jax.random.fold_in(keys[4], 71), 0),
        "range_bits": touch_ends(jax.random.randint(keys[2], (NBX, NBY, SLOTS, ST, WORDS), 0, 1073741824), jax.random.fold_in(keys[2], 1), 0, 1073741823).astype(jnp.int32),
        "old_stacks": centred(keys[3], (NBX, NBY, SLOTS, BANDS, 2, ST, ST), 1.0, 6.0, ((0, 8), (1, 16)), jnp.float32),
    }


EPSILON = 1e-06

def whiten(spectrum, band_count):
    segments, components, stations, freq_bins = spectrum.shape
    grouped = spectrum.astype(jnp.float32).reshape(segments, components, stations, band_count, freq_bins // band_count)
    band_power = lax.optimization_barrier(jnp.mean(grouped * grouped, axis=(0, 1, 4)))
    scaled = grouped * lax.rsqrt(band_power + EPSILON)[None, None, :, :, None]
    return scaled.reshape(spectrum.shape).astype(jnp.bfloat16)

def cross_bands(first_block, second_block, band_count):
    segments, components, stations, freq_bins = first_block.shape
    band_width = freq_bins // band_count
    first_wide = first_block.astype(jnp.float32)
    turned = jnp.stack([first_wide[:, 1], -first_wide[:, 0]], axis=1)
    stacked = jnp.stack([first_wide, turned], 0).reshape(2, segments, components, stations, band_count, band_width)
    partner_wide = second_block.astype(jnp.float32).reshape(segments, components, stations, band_count, band_width)
    product = jnp.einsum('oscinw,scjnw->noij', stacked, partner_wide, precision=lax.Precision.HIGHEST)
    return product * (1.0 / math.sqrt(segments * band_width))

def unpack_range(range_words, stations):
    word_count = range_words.shape[-1]
    column_ids = jnp.arange(stations, dtype=jnp.int32)
    onehot = (column_ids[:, None] // 30 == jnp.arange(word_count, dtype=jnp.int32)[None, :]).astype(jnp.int32)
    selected = lax.optimization_barrier(jnp.sum(range_words[..., :, None, :] * onehot, axis=-1))
    flags = jnp.bitwise_and(jnp.right_shift(selected, column_ids % 30), 1)
    return flags.astype(jnp.float32)

def reference(spectra, partner_codes, range_bits, old_stacks):
    row_count = spectra.shape[0]
    col_count = spectra.shape[1]
    block_count = row_count * col_count
    band_count = old_stacks.shape[3]
    stations = old_stacks.shape[-1]
    slot_count = partner_codes.shape[-1]
    flat_spectra = spectra.reshape((block_count,) + spectra.shape[2:])
    whitened = lax.map(lambda spectrum: whiten(spectrum, band_count), flat_spectra).reshape(spectra.shape)

    def per_block(item):
        block_index, code_row, range_words, old_block = item
        row_pos = block_index // col_count
        col_pos = block_index % col_count
        own_block = whitened[row_pos, col_pos]
        unit_zero = jnp.zeros((band_count, 2, stations, stations), jnp.float32)
        crosses = []
        for slot_index in range(slot_count):
            pair_code = code_row[slot_index]
            step_row = (pair_code == 1).astype(jnp.int32) + (pair_code == 4).astype(jnp.int32) - (pair_code == 2).astype(jnp.int32)
            step_col = (pair_code >= 2).astype(jnp.int32)
            target_row = jnp.clip(row_pos + step_row, 0, row_count - 1)
            target_col = jnp.clip(col_pos + step_col, 0, col_count - 1)
            partner_block = whitened[target_row, target_col]
            pair_cross = lax.cond(pair_code >= 0, lambda operands: cross_bands(operands[0], operands[1], band_count).astype(jnp.float32), lambda operands: unit_zero, (own_block, partner_block))
            crosses.append(pair_cross)
        cross_all = jnp.stack(crosses, 0)
        in_range = unpack_range(range_words, stations)
        return old_block + in_range[:, None, None] * cross_all
    flat_items = (jnp.arange(block_count, dtype=jnp.int32), partner_codes.reshape(block_count, slot_count), range_bits.reshape((block_count,) + range_bits.shape[2:]), old_stacks.reshape((block_count,) + old_stacks.shape[2:]))
    updated = lax.map(per_block, flat_items)
    return updated.reshape(old_stacks.shape)
```

```python
import math

import jax
import jax.numpy as jnp
from jax import lax
from jax.experimental import pallas as pl
from jax.experimental.pallas import tpu as pltpu
from jax.sharding import PartitionSpec as P

EPSILON = 1e-06
MESH = pl.DeviceIdType.MESH
ROWS = 8
COLS = 16
ST = 128
SEG = 3
BANDS = 8
BW = 512
SLOTS = 5
WORDS = 5
SCALE = 1.0 / math.sqrt(SEG * BW)

OWN, OTHER, UPPER, LOWER, LEFT, RIGHT, PLACES = 0, 8, 12, 16, 20, 24, 28


def whiten(w, place):
    def rows_of(t, carry):
        first = pl.multiple_of(t * 16, 16)
        total = jnp.zeros((16, BW), jnp.float32)
        for s in range(SEG):
            for c in range(2):
                x = w[place, s, pl.ds(c * ST + first, 16), :].astype(jnp.float32)
                total = total + x * x
        power = jnp.sum(total, axis=-1, keepdims=True) * (1.0 / (SEG * 2 * BW))
        gain = lax.rsqrt(power + EPSILON)
        for s in range(SEG):
            for c in range(2):
                x = w[place, s, pl.ds(c * ST + first, 16), :].astype(jnp.float32)
                w[place, s, pl.ds(c * ST + first, 16), :] = (x * gain).astype(jnp.bfloat16)
        return carry

    lax.fori_loop(0, ST // 16, rows_of, 0)


def pair(w, x, y):
    total = None
    for s in range(SEG):
        part = lax.dot_general(
            w[x, s], w[y, s], (((1,), (1,)), ((), ())), preferred_element_type=jnp.float32
        )
        total = part if total is None else total + part
    real = (total[:ST, :ST] + total[ST:, ST:]) * SCALE
    imag = (total[ST:, :ST] - total[:ST, ST:]) * SCALE
    return real, imag


def kernel(
    codes, bits, spectra, old, out,
    w, cross, keep, mask, pick, sent_p, got_p, sent_q, got_q,
    load_sem, old_sem, out_sem,
    die_s, die_r, row_s, row_r, col_s, col_r,
    p_s, p_r, q_s, q_r, e_s, e_r, d_s, d_r,
):
    gx = lax.axis_index("gx")
    gy = lax.axis_index("gy")
    k = lax.rem(gx, 2)
    o = 1 - k
    base = gx - k
    right = lax.rem(gy + 1, COLS)
    left = lax.rem(gy + COLS - 1, COLS)
    above = lax.rem(base + ROWS - 2, ROWS)
    below = lax.rem(base + 2, ROWS)

    def band(b):
        return spectra.at[:, :, pl.ds(pl.multiple_of(b * BW, BW), BW)]

    def remote(src, dst, send, recv, row, col):
        return pltpu.make_async_remote_copy(
            src_ref=src, dst_ref=dst, send_sem=send, recv_sem=recv,
            device_id=(row, col), device_id_type=MESH,
        )

    def load(b):
        return pltpu.make_async_copy(band(b), w.at[OWN + b], load_sem.at[b])

    def load_old(b):
        return pltpu.make_async_copy(old.at[:, b], keep.at[b], old_sem.at[b])

    def store(b):
        return pltpu.make_async_copy(keep.at[b], out.at[:, b], out_sem.at[b])

    def die(i):
        return remote(band(2 * i + o), w.at[OTHER + i], die_s.at[i], die_r.at[i], base + o, gy)

    def across(b):
        h, j = (b % 4) // 2, b % 2
        at = (LEFT if b < 4 else RIGHT) + 2 * h + k
        return remote(
            band(b), w.at[at], row_s.at[b], row_r.at[at - LEFT],
            base + j, right if b < 4 else left,
        )

    def vertical(b):
        i, j = b // 2, b % 2
        at = LOWER - 4 * k + i
        chip = jnp.where(k == 0, above, below)
        return remote(band(b), w.at[at], col_s.at[b], col_r.at[at - UPPER], chip + j, gy)

    def return_p(h, i):
        return remote(
            sent_p.at[h, i], got_p.at[2 * h + k], p_s.at[h, i], p_r.at[2 * h + k],
            base + i, left,
        )

    def return_q(h, i):
        row = above + 1 if i == 0 else below
        return remote(
            sent_q.at[h, i], got_q.at[2 * h + k], q_s.at[h, i], q_r.at[2 * h + k], row, gy
        )

    def hand_e(i, b):
        return remote(
            cross.at[1, b, 1], cross.at[0, b, 1], e_s.at[i], e_r.at[i], base + o, gy
        )

    def hand_d(h, b, owner):
        part = pl.ds(3 - owner, 2)
        return remote(
            cross.at[1, b, part], cross.at[0, b, part], d_s.at[h], d_r.at[h], base + o, gy
        )

    def arrival(dst, sem):
        return remote(dst, dst, load_sem.at[0], sem, base + o, gy)

    barrier = pltpu.get_barrier_semaphore()
    greeted = [
        (base, left), (base + 1, left), (base, right), (base + 1, right), (base + o, gy),
        (jnp.where(k == 0, above, below), gy), (jnp.where(k == 0, above, below) + 1, gy),
        (jnp.where(k == 0, below, above + 1), gy),
    ]
    for where in greeted:
        pl.semaphore_signal(barrier, inc=1, device_id=where, device_id_type=MESH)

    def start_load(b, carry):
        load(b).start()
        return carry

    lax.fori_loop(0, BANDS, start_load, 0)
    pl.semaphore_wait(barrier, len(greeted))

    for b in range(4):
        across(b).start()
        across(4 + b).start()
    for b in (0, 4, 1, 5, 2, 6, 3, 7):
        vertical(b).start()
    for i in (0, 2, 1, 3):
        die(i).start()

    def start_old(b, carry):
        load_old(b).start()
        return carry

    lax.fori_loop(0, BANDS, start_old, 0)

    lane = lax.broadcasted_iota(jnp.int32, (ST, ST), 1)
    word = lane // 30
    shift = lane - word * 30
    for s in range(SLOTS):
        chosen = jnp.zeros((ST, ST), jnp.int32)
        for n in range(WORDS):
            chosen = jnp.where(word == n, bits[s, :, n:n + 1], chosen)
        mask[s] = (lax.shift_right_logical(chosen, shift) & 1).astype(jnp.float32)
    pick[0] = jnp.zeros((2 * ST, ST), jnp.float32)

    def own_band(b, carry):
        load(b).wait()
        whiten(w, OWN + b)
        real, imag = pair(w, OWN + b, OWN + b)
        cross[0, b, 0, :ST, :] = real
        cross[0, b, 0, ST:, :] = imag
        return carry

    lax.fori_loop(0, BANDS, own_band, 0)

    def chip_block(a, i):
        return jnp.where(a == k, OWN + 2 * i + k, OTHER + i)

    def put(owner, b, code, value):
        side = jnp.where(owner == k, 0, 1)
        cross[side, b, code, :ST, :] = value[0]
        cross[side, b, code, ST:, :] = value[1]

    def common(i):
        b = 2 * i + k
        arrival(w.at[OTHER + i], die_r.at[i]).wait_recv()
        arrival(w.at[UPPER + i], col_r.at[i]).wait_recv()
        arrival(w.at[LOWER + i], col_r.at[4 + i]).wait_recv()

        def whiten_one(n, carry):
            whiten(w, OTHER + 4 * n + i)
            return carry

        lax.fori_loop(0, 3, whiten_one, 0)

        def below_pair(a, carry):
            x = chip_block(a, i)
            y = jnp.where(a == 0, chip_block(1, i), LOWER + i)
            put(a, b, 1, pair(w, x, y))
            return carry

        lax.fori_loop(0, 2, below_pair, 0)

    def stage(h, carry):
        i = h
        b = 2 * i + k
        common(i)
        for n in range(2):
            arrival(w.at[LEFT + 2 * h + n], row_r.at[2 * h + n]).wait_recv()
        hand_e(i, b).start()
        for n in range(2):
            whiten(w, LEFT + 2 * h + n)

        def left_pair(n, carry):
            own, a = n // 2, n % 2
            real, imag = pair(w, LEFT + 2 * h + own, chip_block(a, i))
            sent_p[h, own, 1 + a - own, :ST, :] = real.astype(jnp.bfloat16)
            sent_p[h, own, 1 + a - own, ST:, :] = imag.astype(jnp.bfloat16)
            return carry

        lax.fori_loop(0, 4, left_pair, 0)

        def left_corner(own, carry):
            real, imag = pair(w, LEFT + 2 * h + own, UPPER + 4 * own + i)
            sent_p[h, own, 2 * own, :ST, :] = real.astype(jnp.bfloat16)
            sent_p[h, own, 2 * own, ST:, :] = imag.astype(jnp.bfloat16)
            return carry

        lax.fori_loop(0, 2, left_corner, 0)

        i = 2 + h
        b = 2 * i + k
        common(i)
        for n in range(2):
            return_p(h, n).start()
        for n in range(2):
            arrival(w.at[RIGHT + 2 * h + n], row_r.at[4 + 2 * h + n]).wait_recv()
        hand_e(i, b).start()
        for n in range(2):
            whiten(w, RIGHT + 2 * h + n)

        def right_corner(n, carry):
            real, imag = pair(w, UPPER + 4 * n + i, RIGHT + 2 * h + n)
            sent_q[h, n, :ST, :] = real.astype(jnp.bfloat16)
            sent_q[h, n, ST:, :] = imag.astype(jnp.bfloat16)
            return carry

        lax.fori_loop(0, 2, right_corner, 0)

        def right_pair(n, carry):
            a, far = n // 2, n % 2
            put(a, b, 3 + far - a, pair(w, chip_block(a, i), RIGHT + 2 * h + far))
            return carry

        lax.fori_loop(0, 4, right_pair, 0)
        for n in range(2):
            return_q(h, n).start()
        hand_d(h, b, o).start()
        return carry

    lax.fori_loop(0, 2, stage, 0)

    def combine(b):
        load_old(b).wait()
        for s in range(SLOTS):
            which = codes[s] + 1
            flags = mask[s]
            keep[b, s, :ST, :] = keep[b, s, :ST, :] + flags * pick[which, :ST, :]
            keep[b, s, ST:, :] = keep[b, s, ST:, :] + flags * pick[which, ST:, :]
        store(b).start()

    def finish_q(n, carry):
        b = 4 + n
        i, j = b // 2, lax.rem(b, 2)
        h = n // 2

        @pl.when(j == o)
        def _():
            arrival(cross.at[0, b, 1], e_r.at[i]).wait_recv()
            part = pl.ds(3 - k, 2)
            arrival(cross.at[0, b, part], d_r.at[h]).wait_recv()

        arrival(got_q.at[n], q_r.at[n]).wait_recv()
        pick[1] = cross[0, b, 0]
        pick[2] = cross[0, b, 1]
        pick[4] = cross[0, b, 3]
        pick[pl.ds(3 + 2 * o, 1)] = cross[0, b, pl.ds(2 + 2 * o, 1)]
        pick[pl.ds(3 + 2 * k, 1)] = got_q[pl.ds(n, 1)].astype(jnp.float32)
        combine(b)
        return carry

    lax.fori_loop(0, 4, finish_q, 0)

    def finish_p(b, carry):
        i, j = b // 2, lax.rem(b, 2)

        @pl.when(j == o)
        def _():
            arrival(cross.at[0, b, 1], e_r.at[i]).wait_recv()

        arrival(got_p.at[b], p_r.at[b]).wait_recv()
        pick[1] = cross[0, b, 0]
        pick[2] = cross[0, b, 1]
        for n in range(3):
            pick[3 + n] = got_p[b, n].astype(jnp.float32)
        combine(b)
        return carry

    lax.fori_loop(0, 4, finish_p, 0)

    for b in range(BANDS):
        across(b).wait_send()
        vertical(b).wait_send()
    for i in range(4):
        die(i).wait_send()
        hand_e(i, 2 * i + k).wait_send()
    for h in range(2):
        for n in range(2):
            return_p(h, n).wait_send()
            return_q(h, n).wait_send()
        hand_d(h, 4 + 2 * h + k, o).wait_send()
    for b in range(BANDS):
        store(b).wait()


def body(spectra, partner_codes, range_bits, old_stacks):
    codes = partner_codes.reshape(SLOTS)
    bits = range_bits.reshape(SLOTS, ST, WORDS)
    blocks = spectra.reshape(SEG, 2 * ST, BANDS * BW)
    old = old_stacks.reshape(SLOTS, BANDS, 2 * ST, ST)
    dma = pltpu.SemaphoreType.DMA
    updated = pl.pallas_call(
        kernel,
        out_shape=jax.ShapeDtypeStruct((SLOTS, BANDS, 2 * ST, ST), jnp.float32),
        in_specs=[
            pl.BlockSpec(memory_space=pltpu.SMEM),
            pl.BlockSpec(memory_space=pltpu.VMEM),
            pl.BlockSpec(memory_space=pl.ANY),
            pl.BlockSpec(memory_space=pl.ANY),
        ],
        out_specs=pl.BlockSpec(memory_space=pl.ANY),
        scratch_shapes=[
            pltpu.VMEM((PLACES, SEG, 2 * ST, BW), jnp.bfloat16),
            pltpu.VMEM((2, BANDS, SLOTS, 2 * ST, ST), jnp.float32),
            pltpu.VMEM((BANDS, SLOTS, 2 * ST, ST), jnp.float32),
            pltpu.VMEM((SLOTS, ST, ST), jnp.float32),
            pltpu.VMEM((SLOTS + 1, 2 * ST, ST), jnp.float32),
            pltpu.VMEM((2, 2, 3, 2 * ST, ST), jnp.bfloat16),
            pltpu.VMEM((4, 3, 2 * ST, ST), jnp.bfloat16),
            pltpu.VMEM((2, 2, 2 * ST, ST), jnp.bfloat16),
            pltpu.VMEM((4, 2 * ST, ST), jnp.bfloat16),
            dma((BANDS,)), dma((BANDS,)), dma((BANDS,)),
            dma((4,)), dma((4,)), dma((8,)), dma((8,)), dma((8,)), dma((8,)),
            dma((2, 2)), dma((4,)), dma((2, 2)), dma((4,)),
            dma((4,)), dma((4,)), dma((2,)), dma((2,)),
        ],
        compiler_params=pltpu.CompilerParams(
            collective_id=0, has_side_effects=True, vmem_limit_bytes=60 * 1024 * 1024
        ),
    )(codes, bits, blocks, old)
    return updated.reshape(old_stacks.shape)


def solution(mesh):
    return jax.shard_map(
        body,
        mesh=mesh,
        in_specs=(
            P("gx", "gy", None, None, None, None),
            P("gx", "gy", None),
            P("gx", "gy", None, None, None),
            P("gx", "gy", None, None, None, None, None),
        ),
        out_specs=P("gx", "gy", None, None, None, None, None),
        check_vma=False,
    )
```

```python
import math

import jax
import jax.numpy as jnp
from jax import lax
from jax.experimental import pallas as pl
from jax.experimental.pallas import tpu as pltpu
from jax.sharding import PartitionSpec as P

EPSILON = 1e-06
MESH = pl.DeviceIdType.MESH
ROWS = 8
COLS = 16
ST = 128
SEG = 3
BANDS = 8
BW = 512
SLOTS = 5
WORDS = 5
SCALE = 1.0 / math.sqrt(SEG * BW)

OWN, OTHER, UPPER, LOWER, LEFT, RIGHT, PLACES = 0, 8, 12, 16, 20, 24, 28


def whiten(w, place):
    def rows_of(t, carry):
        first = pl.multiple_of(t * 16, 16)
        total = jnp.zeros((16, BW), jnp.float32)
        for s in range(SEG):
            for c in range(2):
                x = w[place, s, pl.ds(c * ST + first, 16), :].astype(jnp.float32)
                total = total + x * x
        power = jnp.sum(total, axis=-1, keepdims=True) * (1.0 / (SEG * 2 * BW))
        gain = lax.rsqrt(power + EPSILON)
        for s in range(SEG):
            for c in range(2):
                x = w[place, s, pl.ds(c * ST + first, 16), :].astype(jnp.float32)
                w[place, s, pl.ds(c * ST + first, 16), :] = (x * gain).astype(jnp.bfloat16)
        return carry

    lax.fori_loop(0, ST // 16, rows_of, 0)


def pair(w, x, y):
    total = None
    for s in range(SEG):
        part = lax.dot_general(
            w[x, s], w[y, s], (((1,), (1,)), ((), ())), preferred_element_type=jnp.float32
        )
        total = part if total is None else total + part
    real = (total[:ST, :ST] + total[ST:, ST:]) * SCALE
    imag = (total[ST:, :ST] - total[:ST, ST:]) * SCALE
    return real, imag


def kernel(
    codes, bits, spectra, old, out,
    w, cross, mask, pick, sent_p, got_p, sent_q, got_q,
    load_sem, old_sem,
    die_s, die_r, row_s, row_r, col_s, col_r,
    p_s, p_r, q_s, q_r, e_s, e_r, d_s, d_r,
):
    gx = lax.axis_index("gx")
    gy = lax.axis_index("gy")
    k = lax.rem(gx, 2)
    o = 1 - k
    base = gx - k
    right = lax.rem(gy + 1, COLS)
    left = lax.rem(gy + COLS - 1, COLS)
    above = lax.rem(base + ROWS - 2, ROWS)
    below = lax.rem(base + 2, ROWS)

    def band(b):
        return spectra.at[:, :, pl.ds(pl.multiple_of(b * BW, BW), BW)]

    def remote(src, dst, send, recv, row, col):
        return pltpu.make_async_remote_copy(
            src_ref=src, dst_ref=dst, send_sem=send, recv_sem=recv,
            device_id=(row, col), device_id_type=MESH,
        )

    def load(b):
        return pltpu.make_async_copy(band(b), w.at[OWN + b], load_sem.at[b])

    def load_old(b):
        return pltpu.make_async_copy(old.at[:, b], out.at[:, b], old_sem.at[b])

    def die(i):
        return remote(band(2 * i + o), w.at[OTHER + i], die_s.at[i], die_r.at[i], base + o, gy)

    def across(b):
        h, j = (b % 4) // 2, b % 2
        at = (LEFT if b < 4 else RIGHT) + 2 * h + k
        return remote(
            band(b), w.at[at], row_s.at[b], row_r.at[at - LEFT],
            base + j, right if b < 4 else left,
        )

    def vertical(b):
        i, j = b // 2, b % 2
        at = LOWER - 4 * k + i
        chip = jnp.where(k == 0, above, below)
        return remote(band(b), w.at[at], col_s.at[b], col_r.at[at - UPPER], chip + j, gy)

    def return_p(h, i):
        return remote(
            sent_p.at[h, i], got_p.at[2 * h + k], p_s.at[h, i], p_r.at[2 * h + k],
            base + i, left,
        )

    def return_q(h, i):
        row = above + 1 if i == 0 else below
        return remote(
            sent_q.at[h, i], got_q.at[2 * h + k], q_s.at[h, i], q_r.at[2 * h + k], row, gy
        )

    def hand_e(i, b):
        return remote(
            cross.at[1, b, 1], cross.at[0, b, 1], e_s.at[i], e_r.at[i], base + o, gy
        )

    def hand_d(h, b, owner):
        part = pl.ds(3 - owner, 2)
        return remote(
            cross.at[1, b, part], cross.at[0, b, part], d_s.at[h], d_r.at[h], base + o, gy
        )

    def arrival(dst, sem):
        return remote(dst, dst, load_sem.at[0], sem, base + o, gy)

    barrier = pltpu.get_barrier_semaphore()
    greeted = [
        (base, left), (base + 1, left), (base, right), (base + 1, right), (base + o, gy),
        (jnp.where(k == 0, above, below), gy), (jnp.where(k == 0, above, below) + 1, gy),
        (jnp.where(k == 0, below, above + 1), gy),
    ]
    for where in greeted:
        pl.semaphore_signal(barrier, inc=1, device_id=where, device_id_type=MESH)

    def start_load(b, carry):
        load(b).start()
        return carry

    lax.fori_loop(0, BANDS, start_load, 0)
    pl.semaphore_wait(barrier, len(greeted))

    for b in range(4):
        across(b).start()
        across(4 + b).start()
    for b in (0, 4, 1, 5, 2, 6, 3, 7):
        vertical(b).start()
    for i in (0, 2, 1, 3):
        die(i).start()

    def start_old(b, carry):
        load_old(b).start()
        return carry

    lax.fori_loop(0, BANDS, start_old, 0)

    column = lax.broadcasted_iota(jnp.int32, (ST, ST), 0)
    word = column // 30
    shift = column - word * 30
    for s in range(SLOTS):
        chosen = jnp.zeros((ST, ST), jnp.int32)
        for n in range(WORDS):
            chosen = jnp.where(word == n, bits[s * WORDS + n], chosen)
        flags = (lax.shift_right_logical(chosen, shift) & 1).astype(jnp.float32)
        mask[s] = flags.T
    pick[0] = jnp.zeros((2 * ST, ST), jnp.float32)

    def own_band(b, carry):
        load(b).wait()
        whiten(w, OWN + b)
        real, imag = pair(w, OWN + b, OWN + b)
        cross[0, b, 0, :ST, :] = real
        cross[0, b, 0, ST:, :] = imag
        return carry

    lax.fori_loop(0, BANDS, own_band, 0)

    def chip_block(a, i):
        return jnp.where(a == k, OWN + 2 * i + k, OTHER + i)

    def put(owner, b, code, value):
        side = jnp.where(owner == k, 0, 1)
        cross[side, b, code, :ST, :] = value[0]
        cross[side, b, code, ST:, :] = value[1]

    def common(i):
        b = 2 * i + k
        arrival(w.at[OTHER + i], die_r.at[i]).wait_recv()
        arrival(w.at[UPPER + i], col_r.at[i]).wait_recv()
        arrival(w.at[LOWER + i], col_r.at[4 + i]).wait_recv()

        def whiten_one(n, carry):
            whiten(w, OTHER + 4 * n + i)
            return carry

        lax.fori_loop(0, 3, whiten_one, 0)

        def below_pair(a, carry):
            x = chip_block(a, i)
            y = jnp.where(a == 0, chip_block(1, i), LOWER + i)
            put(a, b, 1, pair(w, x, y))
            return carry

        lax.fori_loop(0, 2, below_pair, 0)

    def stage(h, carry):
        i = h
        b = 2 * i + k
        common(i)
        for n in range(2):
            arrival(w.at[LEFT + 2 * h + n], row_r.at[2 * h + n]).wait_recv()
        hand_e(i, b).start()
        for n in range(2):
            whiten(w, LEFT + 2 * h + n)

        def left_pair(n, carry):
            own, a = n // 2, n % 2
            real, imag = pair(w, LEFT + 2 * h + own, chip_block(a, i))
            sent_p[h, own, 1 + a - own, :ST, :] = real.astype(jnp.bfloat16)
            sent_p[h, own, 1 + a - own, ST:, :] = imag.astype(jnp.bfloat16)
            return carry

        lax.fori_loop(0, 4, left_pair, 0)

        def left_corner(own, carry):
            real, imag = pair(w, LEFT + 2 * h + own, UPPER + 4 * own + i)
            sent_p[h, own, 2 * own, :ST, :] = real.astype(jnp.bfloat16)
            sent_p[h, own, 2 * own, ST:, :] = imag.astype(jnp.bfloat16)
            return carry

        lax.fori_loop(0, 2, left_corner, 0)

        i = 2 + h
        b = 2 * i + k
        common(i)
        for n in range(2):
            return_p(h, n).start()
        for n in range(2):
            arrival(w.at[RIGHT + 2 * h + n], row_r.at[4 + 2 * h + n]).wait_recv()
        hand_e(i, b).start()
        for n in range(2):
            whiten(w, RIGHT + 2 * h + n)

        def right_corner(n, carry):
            real, imag = pair(w, UPPER + 4 * n + i, RIGHT + 2 * h + n)
            sent_q[h, n, :ST, :] = real.astype(jnp.bfloat16)
            sent_q[h, n, ST:, :] = imag.astype(jnp.bfloat16)
            return carry

        lax.fori_loop(0, 2, right_corner, 0)

        def right_pair(n, carry):
            a, far = n // 2, n % 2
            put(a, b, 3 + far - a, pair(w, chip_block(a, i), RIGHT + 2 * h + far))
            return carry

        lax.fori_loop(0, 4, right_pair, 0)
        for n in range(2):
            return_q(h, n).start()
        hand_d(h, b, o).start()
        return carry

    lax.fori_loop(0, 2, stage, 0)

    def combine(b):
        load_old(b).wait()
        for s in range(SLOTS):
            which = codes[s] + 1
            flags = mask[s]
            out[s, b, :ST, :] = out[s, b, :ST, :] + flags * pick[which, :ST, :]
            out[s, b, ST:, :] = out[s, b, ST:, :] + flags * pick[which, ST:, :]

    def finish_q(n, carry):
        b = 4 + n
        i, j = b // 2, lax.rem(b, 2)
        h = n // 2

        @pl.when(j == o)
        def _():
            arrival(cross.at[0, b, 1], e_r.at[i]).wait_recv()
            part = pl.ds(3 - k, 2)
            arrival(cross.at[0, b, part], d_r.at[h]).wait_recv()

        arrival(got_q.at[n], q_r.at[n]).wait_recv()
        pick[1] = cross[0, b, 0]
        pick[2] = cross[0, b, 1]
        pick[4] = cross[0, b, 3]
        pick[pl.ds(3 + 2 * o, 1)] = cross[0, b, pl.ds(2 + 2 * o, 1)]
        pick[pl.ds(3 + 2 * k, 1)] = got_q[pl.ds(n, 1)].astype(jnp.float32)
        combine(b)
        return carry

    lax.fori_loop(0, 4, finish_q, 0)

    def finish_p(b, carry):
        i, j = b // 2, lax.rem(b, 2)

        @pl.when(j == o)
        def _():
            arrival(cross.at[0, b, 1], e_r.at[i]).wait_recv()

        arrival(got_p.at[b], p_r.at[b]).wait_recv()
        pick[1] = cross[0, b, 0]
        pick[2] = cross[0, b, 1]
        for n in range(3):
            pick[3 + n] = got_p[b, n].astype(jnp.float32)
        combine(b)
        return carry

    lax.fori_loop(0, 4, finish_p, 0)

    for b in range(BANDS):
        across(b).wait_send()
        vertical(b).wait_send()
    for i in range(4):
        die(i).wait_send()
        hand_e(i, 2 * i + k).wait_send()
    for h in range(2):
        for n in range(2):
            return_p(h, n).wait_send()
            return_q(h, n).wait_send()
        hand_d(h, 4 + 2 * h + k, o).wait_send()


def body(spectra, partner_codes, range_bits, old_stacks):
    codes = partner_codes.reshape(SLOTS)
    bits = jnp.swapaxes(range_bits.reshape(SLOTS, ST, WORDS), 1, 2).reshape(SLOTS * WORDS, 1, ST)
    blocks = spectra.reshape(SEG, 2 * ST, BANDS * BW)
    old = old_stacks.reshape(SLOTS, BANDS, 2 * ST, ST)
    dma = pltpu.SemaphoreType.DMA
    updated = pl.pallas_call(
        kernel,
        out_shape=pltpu.VMEM((SLOTS, BANDS, 2 * ST, ST), jnp.float32),
        in_specs=[
            pl.BlockSpec(memory_space=pltpu.SMEM),
            pl.BlockSpec(memory_space=pltpu.VMEM),
            pl.BlockSpec(memory_space=pl.ANY),
            pl.BlockSpec(memory_space=pl.ANY),
        ],
        out_specs=pl.BlockSpec(memory_space=pltpu.VMEM),
        scratch_shapes=[
            pltpu.VMEM((PLACES, SEG, 2 * ST, BW), jnp.bfloat16),
            pltpu.VMEM((2, BANDS, SLOTS, 2 * ST, ST), jnp.float32),
            pltpu.VMEM((SLOTS, ST, ST), jnp.float32),
            pltpu.VMEM((SLOTS + 1, 2 * ST, ST), jnp.float32),
            pltpu.VMEM((2, 2, 3, 2 * ST, ST), jnp.bfloat16),
            pltpu.VMEM((4, 3, 2 * ST, ST), jnp.bfloat16),
            pltpu.VMEM((2, 2, 2 * ST, ST), jnp.bfloat16),
            pltpu.VMEM((4, 2 * ST, ST), jnp.bfloat16),
            dma((BANDS,)), dma((BANDS,)),
            dma((4,)), dma((4,)), dma((8,)), dma((8,)), dma((8,)), dma((8,)),
            dma((2, 2)), dma((4,)), dma((2, 2)), dma((4,)),
            dma((4,)), dma((4,)), dma((2,)), dma((2,)),
        ],
        compiler_params=pltpu.CompilerParams(
            collective_id=0, has_side_effects=True, vmem_limit_bytes=52 * 1024 * 1024
        ),
    )(codes, bits, blocks, old)
    return updated.reshape(old_stacks.shape)


def solution(mesh):
    return jax.shard_map(
        body,
        mesh=mesh,
        in_specs=(
            P("gx", "gy", None, None, None, None),
            P("gx", "gy", None),
            P("gx", "gy", None, None, None),
            P("gx", "gy", None, None, None, None, None),
        ),
        out_specs=P("gx", "gy", None, None, None, None, None),
        check_vma=False,
    )
```

```python
import math

import jax
import jax.numpy as jnp
from jax import lax
from jax.experimental import pallas as pl
from jax.experimental.pallas import tpu as pltpu
from jax.sharding import PartitionSpec as P

EPSILON = 1e-06
MESH = pl.DeviceIdType.MESH
ROWS = 8
COLS = 16
ST = 128
SEG = 3
BANDS = 8
BW = 512
SLOTS = 5
WORDS = 5
SCALE = 1.0 / math.sqrt(SEG * BW)

OWN, OTHER, UPPER, LOWER, LEFT, RIGHT, PLACES = 0, 8, 12, 16, 20, 24, 28


def whiten(w, place):
    def rows_of(t, carry):
        first = pl.multiple_of(t * 16, 16)
        total = jnp.zeros((16, BW), jnp.float32)
        for s in range(SEG):
            for c in range(2):
                x = w[place, s, pl.ds(c * ST + first, 16), :].astype(jnp.float32)
                total = total + x * x
        power = jnp.sum(total, axis=-1, keepdims=True) * (1.0 / (SEG * 2 * BW))
        gain = lax.rsqrt(power + EPSILON)
        for s in range(SEG):
            for c in range(2):
                x = w[place, s, pl.ds(c * ST + first, 16), :].astype(jnp.float32)
                w[place, s, pl.ds(c * ST + first, 16), :] = (x * gain).astype(jnp.bfloat16)
        return carry

    lax.fori_loop(0, ST // 16, rows_of, 0)


def pair(w, x, y):
    total = None
    for s in range(SEG):
        part = lax.dot_general(
            w[x, s], w[y, s], (((1,), (1,)), ((), ())), preferred_element_type=jnp.float32
        )
        total = part if total is None else total + part
    real = (total[:ST, :ST] + total[ST:, ST:]) * SCALE
    imag = (total[ST:, :ST] - total[:ST, ST:]) * SCALE
    return real, imag


def kernel(
    codes, bits, spectra, old, out,
    w, cross, mask, pick, sent_p, got_p, sent_q, got_q,
    load_sem, old_sem,
    die_s, die_r, row_s, row_r, col_s, col_r,
    p_s, p_r, q_s, q_r, e_s, e_r, d_s, d_r,
):
    gx = lax.axis_index("gx")
    gy = lax.axis_index("gy")
    k = lax.rem(gx, 2)
    o = 1 - k
    base = gx - k
    right = lax.rem(gy + 1, COLS)
    left = lax.rem(gy + COLS - 1, COLS)
    above = lax.rem(base + ROWS - 2, ROWS)
    below = lax.rem(base + 2, ROWS)

    def band(b):
        return spectra.at[:, :, pl.ds(pl.multiple_of(b * BW, BW), BW)]

    def remote(src, dst, send, recv, row, col):
        return pltpu.make_async_remote_copy(
            src_ref=src, dst_ref=dst, send_sem=send, recv_sem=recv,
            device_id=(row, col), device_id_type=MESH,
        )

    def load(b):
        return pltpu.make_async_copy(band(b), w.at[OWN + b], load_sem.at[b])

    def load_old(b):
        return pltpu.make_async_copy(old.at[:, b], out.at[:, b], old_sem.at[b])

    def die(i):
        return remote(band(2 * i + o), w.at[OTHER + i], die_s.at[i], die_r.at[i], base + o, gy)

    def across(b):
        h, j = (b % 4) // 2, b % 2
        at = (LEFT if b < 4 else RIGHT) + 2 * h + k
        return remote(
            band(b), w.at[at], row_s.at[b], row_r.at[at - LEFT],
            base + j, right if b < 4 else left,
        )

    def vertical(b):
        i, j = b // 2, b % 2
        at = LOWER - 4 * k + i
        chip = jnp.where(k == 0, above, below)
        return remote(band(b), w.at[at], col_s.at[b], col_r.at[at - UPPER], chip + j, gy)

    def return_p(h, i):
        return remote(
            sent_p.at[h, i], got_p.at[2 * h + k], p_s.at[h, i], p_r.at[2 * h + k],
            base + i, left,
        )

    def return_q(h, i):
        row = above + 1 if i == 0 else below
        return remote(
            sent_q.at[h, i], got_q.at[2 * h + k], q_s.at[h, i], q_r.at[2 * h + k], row, gy
        )

    def hand_e(i, b):
        return remote(
            cross.at[1, b, 1], cross.at[0, b, 1], e_s.at[i], e_r.at[i], base + o, gy
        )

    def hand_d(h, b, owner):
        part = pl.ds(3 - owner, 2)
        return remote(
            cross.at[1, b, part], cross.at[0, b, part], d_s.at[h], d_r.at[h], base + o, gy
        )

    def arrival(dst, sem):
        return remote(dst, dst, load_sem.at[0], sem, base + o, gy)

    barrier = pltpu.get_barrier_semaphore()
    greeted = [
        (base, left), (base + 1, left), (base, right), (base + 1, right), (base + o, gy),
        (jnp.where(k == 0, above, below), gy), (jnp.where(k == 0, above, below) + 1, gy),
        (jnp.where(k == 0, below, above + 1), gy),
    ]
    for where in greeted:
        pl.semaphore_signal(barrier, inc=1, device_id=where, device_id_type=MESH)

    def start_load(b, carry):
        load(b).start()
        return carry

    lax.fori_loop(0, BANDS, start_load, 0)
    pl.semaphore_wait(barrier, len(greeted))

    for b in range(4):
        across(b).start()
        across(4 + b).start()
    for b in (0, 4, 1, 5, 2, 6, 3, 7):
        vertical(b).start()
    for i in (0, 2, 1, 3):
        die(i).start()

    def start_old(b, carry):
        load_old(b).start()
        return carry

    lax.fori_loop(0, BANDS, start_old, 0)

    column = lax.broadcasted_iota(jnp.int32, (ST, ST), 0)
    word = column // 30
    shift = column - word * 30
    for s in range(SLOTS):
        chosen = jnp.zeros((ST, ST), jnp.int32)
        for n in range(WORDS):
            chosen = jnp.where(word == n, bits[s * WORDS + n], chosen)
        flags = (lax.shift_right_logical(chosen, shift) & 1).astype(jnp.float32)
        mask[s] = flags.T
    pick[0] = jnp.zeros((2 * ST, ST), jnp.float32)

    def own_band(b, carry):
        load(b).wait()
        whiten(w, OWN + b)
        real, imag = pair(w, OWN + b, OWN + b)
        cross[0, b, 0, :ST, :] = real
        cross[0, b, 0, ST:, :] = imag
        return carry

    lax.fori_loop(0, BANDS, own_band, 0)

    def chip_block(a, i):
        return jnp.where(a == k, OWN + 2 * i + k, OTHER + i)

    def put(owner, b, code, value):
        side = jnp.where(owner == k, 0, 1)
        cross[side, b, code, :ST, :] = value[0]
        cross[side, b, code, ST:, :] = value[1]

    def common(i):
        b = 2 * i + k
        arrival(w.at[OTHER + i], die_r.at[i]).wait_recv()
        arrival(w.at[UPPER + i], col_r.at[i]).wait_recv()
        arrival(w.at[LOWER + i], col_r.at[4 + i]).wait_recv()

        def whiten_one(n, carry):
            whiten(w, OTHER + 4 * n + i)
            return carry

        lax.fori_loop(0, 3, whiten_one, 0)

        def below_pair(a, carry):
            x = chip_block(a, i)
            y = jnp.where(a == 0, chip_block(1, i), LOWER + i)
            put(a, b, 1, pair(w, x, y))
            return carry

        lax.fori_loop(0, 2, below_pair, 0)

    def stage(h, carry):
        i = h
        b = 2 * i + k
        common(i)
        for n in range(2):
            arrival(w.at[LEFT + 2 * h + n], row_r.at[2 * h + n]).wait_recv()
        hand_e(i, b).start()
        for n in range(2):
            whiten(w, LEFT + 2 * h + n)

        def left_pair(n, carry):
            own, a = n // 2, n % 2
            real, imag = pair(w, LEFT + 2 * h + own, chip_block(a, i))
            sent_p[h, own, 1 + a - own, :ST, :] = real.astype(jnp.bfloat16)
            sent_p[h, own, 1 + a - own, ST:, :] = imag.astype(jnp.bfloat16)
            return carry

        lax.fori_loop(0, 4, left_pair, 0)

        def left_corner(own, carry):
            real, imag = pair(w, LEFT + 2 * h + own, UPPER + 4 * own + i)
            sent_p[h, own, 2 * own, :ST, :] = real.astype(jnp.bfloat16)
            sent_p[h, own, 2 * own, ST:, :] = imag.astype(jnp.bfloat16)
            return carry

        lax.fori_loop(0, 2, left_corner, 0)

        i = 2 + h
        b = 2 * i + k
        common(i)
        for n in range(2):
            return_p(h, n).start()
        for n in range(2):
            arrival(w.at[RIGHT + 2 * h + n], row_r.at[4 + 2 * h + n]).wait_recv()
        hand_e(i, b).start()
        for n in range(2):
            whiten(w, RIGHT + 2 * h + n)

        def right_corner(n, carry):
            real, imag = pair(w, UPPER + 4 * n + i, RIGHT + 2 * h + n)
            sent_q[h, n, :ST, :] = real.astype(jnp.bfloat16)
            sent_q[h, n, ST:, :] = imag.astype(jnp.bfloat16)
            return carry

        lax.fori_loop(0, 2, right_corner, 0)

        def right_pair(n, carry):
            a, far = n // 2, n % 2
            put(a, b, 3 + far - a, pair(w, chip_block(a, i), RIGHT + 2 * h + far))
            return carry

        lax.fori_loop(0, 4, right_pair, 0)
        for n in range(2):
            return_q(h, n).start()
        hand_d(h, b, o).start()
        return carry

    lax.fori_loop(0, 2, stage, 0)

    def combine(b):
        load_old(b).wait()
        for s in range(SLOTS):
            which = codes[s] + 1
            flags = mask[s]
            out[s, b, :ST, :] = out[s, b, :ST, :] + flags * pick[which, :ST, :]
            out[s, b, ST:, :] = out[s, b, ST:, :] + flags * pick[which, ST:, :]

    def finish_q(n, carry):
        b = 4 + n
        i, j = b // 2, lax.rem(b, 2)
        h = n // 2

        @pl.when(j == o)
        def _():
            arrival(cross.at[0, b, 1], e_r.at[i]).wait_recv()
            part = pl.ds(3 - k, 2)
            arrival(cross.at[0, b, part], d_r.at[h]).wait_recv()

        arrival(got_q.at[n], q_r.at[n]).wait_recv()
        pick[1] = cross[0, b, 0]
        pick[2] = cross[0, b, 1]
        pick[4] = cross[0, b, 3]
        pick[pl.ds(3 + 2 * o, 1)] = cross[0, b, pl.ds(2 + 2 * o, 1)]
        pick[pl.ds(3 + 2 * k, 1)] = got_q[pl.ds(n, 1)].astype(jnp.float32)
        combine(b)
        return carry

    lax.fori_loop(0, 4, finish_q, 0)

    def finish_p(b, carry):
        i, j = b // 2, lax.rem(b, 2)

        @pl.when(j == o)
        def _():
            arrival(cross.at[0, b, 1], e_r.at[i]).wait_recv()

        arrival(got_p.at[b], p_r.at[b]).wait_recv()
        pick[1] = cross[0, b, 0]
        pick[2] = cross[0, b, 1]
        for n in range(3):
            pick[3 + n] = got_p[b, n].astype(jnp.float32)
        combine(b)
        return carry

    lax.fori_loop(0, 4, finish_p, 0)

    for b in range(BANDS):
        across(b).wait_send()
        vertical(b).wait_send()
    for i in range(4):
        die(i).wait_send()
        hand_e(i, 2 * i + k).wait_send()
    for h in range(2):
        for n in range(2):
            return_p(h, n).wait_send()
            return_q(h, n).wait_send()
        hand_d(h, 4 + 2 * h + k, o).wait_send()


def body(spectra, partner_codes, range_bits, old_stacks):
    codes = partner_codes.reshape(SLOTS)
    bits = jnp.transpose(range_bits, (0, 2, 4, 1, 3)).reshape(SLOTS * WORDS, 1, ST)
    blocks = spectra.reshape(SEG, 2 * ST, BANDS * BW)
    old = old_stacks.reshape(SLOTS, BANDS, 2 * ST, ST)
    dma = pltpu.SemaphoreType.DMA
    updated = pl.pallas_call(
        kernel,
        out_shape=pltpu.VMEM((SLOTS, BANDS, 2 * ST, ST), jnp.float32),
        in_specs=[
            pl.BlockSpec(memory_space=pltpu.SMEM),
            pl.BlockSpec(memory_space=pltpu.VMEM),
            pl.BlockSpec(memory_space=pl.ANY),
            pl.BlockSpec(memory_space=pl.ANY),
        ],
        out_specs=pl.BlockSpec(memory_space=pltpu.VMEM),
        scratch_shapes=[
            pltpu.VMEM((PLACES, SEG, 2 * ST, BW), jnp.bfloat16),
            pltpu.VMEM((2, BANDS, SLOTS, 2 * ST, ST), jnp.float32),
            pltpu.VMEM((SLOTS, ST, ST), jnp.float32),
            pltpu.VMEM((SLOTS + 1, 2 * ST, ST), jnp.float32),
            pltpu.VMEM((2, 2, 3, 2 * ST, ST), jnp.bfloat16),
            pltpu.VMEM((4, 3, 2 * ST, ST), jnp.bfloat16),
            pltpu.VMEM((2, 2, 2 * ST, ST), jnp.bfloat16),
            pltpu.VMEM((4, 2 * ST, ST), jnp.bfloat16),
            dma((BANDS,)), dma((BANDS,)),
            dma((4,)), dma((4,)), dma((8,)), dma((8,)), dma((8,)), dma((8,)),
            dma((2, 2)), dma((4,)), dma((2, 2)), dma((4,)),
            dma((4,)), dma((4,)), dma((2,)), dma((2,)),
        ],
        compiler_params=pltpu.CompilerParams(
            collective_id=0, has_side_effects=True, vmem_limit_bytes=52 * 1024 * 1024
        ),
    )(codes, bits, blocks, old)
    return updated.reshape(old_stacks.shape)


def solution(mesh):
    return jax.shard_map(
        body,
        mesh=mesh,
        in_specs=(
            P("gx", "gy", None, None, None, None),
            P("gx", "gy", None),
            P("gx", "gy", None, None, None),
            P("gx", "gy", None, None, None, None, None),
        ),
        out_specs=P("gx", "gy", None, None, None, None, None),
        check_vma=False,
    )
```

```python
import math

import jax
import jax.numpy as jnp
from jax import lax
from jax.experimental import pallas as pl
from jax.experimental.pallas import tpu as pltpu
from jax.sharding import PartitionSpec as P

EPSILON = 1e-06
MESH = pl.DeviceIdType.MESH
ROWS = 8
COLS = 16
ST = 128
SEG = 3
BANDS = 8
BW = 512
SLOTS = 5
WORDS = 5
SCALE = 1.0 / math.sqrt(SEG * BW)

OWN, OTHER, UPPER, LOWER, LEFT, RIGHT, PLACES = 0, 8, 12, 16, 20, 24, 28


def whiten(w, place):
    def rows_of(t, carry):
        first = pl.multiple_of(t * 16, 16)
        total = jnp.zeros((16, BW), jnp.float32)
        for s in range(SEG):
            for c in range(2):
                x = w[place, s, pl.ds(c * ST + first, 16), :].astype(jnp.float32)
                total = total + x * x
        power = jnp.sum(total, axis=-1, keepdims=True) * (1.0 / (SEG * 2 * BW))
        gain = lax.rsqrt(power + EPSILON)
        for s in range(SEG):
            for c in range(2):
                x = w[place, s, pl.ds(c * ST + first, 16), :].astype(jnp.float32)
                w[place, s, pl.ds(c * ST + first, 16), :] = (x * gain).astype(jnp.bfloat16)
        return carry

    lax.fori_loop(0, ST // 16, rows_of, 0)


def pair(w, x, y):
    total = None
    for s in range(SEG):
        part = lax.dot_general(
            w[x, s], w[y, s], (((1,), (1,)), ((), ())), preferred_element_type=jnp.float32
        )
        total = part if total is None else total + part
    real = (total[:ST, :ST] + total[ST:, ST:]) * SCALE
    imag = (total[ST:, :ST] - total[:ST, ST:]) * SCALE
    return real, imag


def kernel(
    codes, bits, spectra, old, out,
    w, cross, mask, pick, sent_p, got_p, sent_q, got_q,
    load_sem, old_sem,
    die_s, die_r, row_s, row_r, col_s, col_r,
    p_s, p_r, q_s, q_r, e_s, e_r, d_s, d_r,
):
    gx = lax.axis_index("gx")
    gy = lax.axis_index("gy")
    k = lax.rem(gx, 2)
    o = 1 - k
    base = gx - k
    right = lax.rem(gy + 1, COLS)
    left = lax.rem(gy + COLS - 1, COLS)
    above = lax.rem(base + ROWS - 2, ROWS)
    below = lax.rem(base + 2, ROWS)
    has_left, has_right = gy > 0, gy < COLS - 1
    has_above, has_below = base > 0, base < ROWS - 2
    swaps = jnp.where(k == 0, base > 0, base < ROWS - 2)
    hears = jnp.where(k == 0, base < ROWS - 2, base > 0)

    def band(b):
        return spectra.at[:, :, pl.ds(pl.multiple_of(b * BW, BW), BW)]

    def remote(src, dst, send, recv, row, col):
        return pltpu.make_async_remote_copy(
            src_ref=src, dst_ref=dst, send_sem=send, recv_sem=recv,
            device_id=(row, col), device_id_type=MESH,
        )

    def load(b):
        return pltpu.make_async_copy(band(b), w.at[OWN + b], load_sem.at[b])

    def load_old(b):
        return pltpu.make_async_copy(old.at[:, b], out.at[:, b], old_sem.at[b])

    def die(i):
        return remote(band(2 * i + o), w.at[OTHER + i], die_s.at[i], die_r.at[i], base + o, gy)

    def across(b):
        h, j = (b % 4) // 2, b % 2
        at = (LEFT if b < 4 else RIGHT) + 2 * h + k
        return remote(
            band(b), w.at[at], row_s.at[b], row_r.at[at - LEFT],
            base + j, right if b < 4 else left,
        )

    def vertical(b):
        i, j = b // 2, b % 2
        at = LOWER - 4 * k + i
        chip = jnp.where(k == 0, above, below)
        return remote(band(b), w.at[at], col_s.at[b], col_r.at[at - UPPER], chip + j, gy)

    def return_p(h, i):
        return remote(
            sent_p.at[h, i], got_p.at[2 * h + k], p_s.at[h, i], p_r.at[2 * h + k],
            base + i, left,
        )

    def return_q(h, i):
        row = above + 1 if i == 0 else below
        return remote(
            sent_q.at[h, i], got_q.at[2 * h + k], q_s.at[h, i], q_r.at[2 * h + k], row, gy
        )

    def hand_e(i, b):
        return remote(
            cross.at[1, b, 1], cross.at[0, b, 1], e_s.at[i], e_r.at[i], base + o, gy
        )

    def hand_d(h, b, owner):
        part = pl.ds(3 - owner, 2)
        return remote(
            cross.at[1, b, part], cross.at[0, b, part], d_s.at[h], d_r.at[h], base + o, gy
        )

    def arrival(dst, sem):
        return remote(dst, dst, load_sem.at[0], sem, base + o, gy)

    barrier = pltpu.get_barrier_semaphore()
    def greet(there, row, col):
        @pl.when(there)
        def _():
            pl.semaphore_signal(barrier, inc=1, device_id=(row, col), device_id_type=MESH)

    chip = jnp.where(k == 0, above, below)
    pl.semaphore_signal(barrier, inc=1, device_id=(base + o, gy), device_id_type=MESH)
    for n in range(2):
        greet(swaps, chip + n, gy)
        greet(has_left, base + n, left)
        greet(has_right, base + n, right)
    greet(hears, jnp.where(k == 0, below, above + 1), gy)
    partners = (
        1 + hears.astype(jnp.int32)
        + 2 * (swaps.astype(jnp.int32) + has_left.astype(jnp.int32) + has_right.astype(jnp.int32))
    )

    def start_load(b, carry):
        load(b).start()
        return carry

    lax.fori_loop(0, BANDS, start_load, 0)
    pl.semaphore_wait(barrier, partners)

    @pl.when(has_right)
    def _():
        for b in range(4):
            across(b).start()

    @pl.when(has_left)
    def _():
        for b in range(4):
            across(4 + b).start()

    @pl.when(swaps)
    def _():
        for b in (0, 4, 1, 5, 2, 6, 3, 7):
            vertical(b).start()

    for i in (0, 2, 1, 3):
        die(i).start()

    def start_old(b, carry):
        load_old(b).start()
        return carry

    lax.fori_loop(0, BANDS, start_old, 0)

    column = lax.broadcasted_iota(jnp.int32, (ST, ST), 0)
    word = column // 30
    shift = column - word * 30
    for s in range(SLOTS):
        chosen = jnp.zeros((ST, ST), jnp.int32)
        for n in range(WORDS):
            chosen = jnp.where(word == n, bits[s * WORDS + n], chosen)
        flags = (lax.shift_right_logical(chosen, shift) & 1).astype(jnp.float32)
        mask[s] = flags.T
    pick[0] = jnp.zeros((2 * ST, ST), jnp.float32)

    def own_band(b, carry):
        load(b).wait()
        whiten(w, OWN + b)
        real, imag = pair(w, OWN + b, OWN + b)
        cross[0, b, 0, :ST, :] = real
        cross[0, b, 0, ST:, :] = imag
        return carry

    lax.fori_loop(0, BANDS, own_band, 0)

    def chip_block(a, i):
        return jnp.where(a == k, OWN + 2 * i + k, OTHER + i)

    def put(owner, b, code, value):
        side = jnp.where(owner == k, 0, 1)
        cross[side, b, code, :ST, :] = value[0]
        cross[side, b, code, ST:, :] = value[1]

    def common(i):
        b = 2 * i + k
        arrival(w.at[OTHER + i], die_r.at[i]).wait_recv()

        @pl.when(has_above)
        def _():
            arrival(w.at[UPPER + i], col_r.at[i]).wait_recv()

        @pl.when(has_below)
        def _():
            arrival(w.at[LOWER + i], col_r.at[4 + i]).wait_recv()

        def whiten_one(n, carry):
            whiten(w, OTHER + 4 * n + i)
            return carry

        lax.fori_loop(0, 3, whiten_one, 0)

        def below_pair(a, carry):
            x = chip_block(a, i)
            y = jnp.where(a == 0, chip_block(1, i), LOWER + i)
            put(a, b, 1, pair(w, x, y))
            return carry

        lax.fori_loop(0, 2, below_pair, 0)

    def from_left(h, i):
        for n in range(2):
            arrival(w.at[LEFT + 2 * h + n], row_r.at[2 * h + n]).wait_recv()
        for n in range(2):
            whiten(w, LEFT + 2 * h + n)

        def left_pair(n, carry):
            own, a = n // 2, n % 2
            real, imag = pair(w, LEFT + 2 * h + own, chip_block(a, i))
            sent_p[h, own, 1 + a - own, :ST, :] = real.astype(jnp.bfloat16)
            sent_p[h, own, 1 + a - own, ST:, :] = imag.astype(jnp.bfloat16)
            return carry

        lax.fori_loop(0, 4, left_pair, 0)

        def left_corner(own, carry):
            real, imag = pair(w, LEFT + 2 * h + own, UPPER + 4 * own + i)
            sent_p[h, own, 2 * own, :ST, :] = real.astype(jnp.bfloat16)
            sent_p[h, own, 2 * own, ST:, :] = imag.astype(jnp.bfloat16)
            return carry

        lax.fori_loop(0, 2, left_corner, 0)

    def from_right(h, i, b):
        for n in range(2):
            arrival(w.at[RIGHT + 2 * h + n], row_r.at[4 + 2 * h + n]).wait_recv()
        for n in range(2):
            whiten(w, RIGHT + 2 * h + n)

        def right_corner(n, carry):
            real, imag = pair(w, UPPER + 4 * n + i, RIGHT + 2 * h + n)
            sent_q[h, n, :ST, :] = real.astype(jnp.bfloat16)
            sent_q[h, n, ST:, :] = imag.astype(jnp.bfloat16)
            return carry

        lax.fori_loop(0, 2, right_corner, 0)

        def right_pair(n, carry):
            a, far = n // 2, n % 2
            put(a, b, 3 + far - a, pair(w, chip_block(a, i), RIGHT + 2 * h + far))
            return carry

        lax.fori_loop(0, 4, right_pair, 0)

        @pl.when(has_above)
        def _():
            return_q(h, 0).start()

        @pl.when(has_below)
        def _():
            return_q(h, 1).start()

        hand_d(h, b, o).start()

    def stage(h, carry):
        common(h)

        @pl.when(has_left)
        def _():
            from_left(h, h)

        hand_e(h, 2 * h + k).start()
        i = 2 + h
        common(i)

        @pl.when(has_left)
        def _():
            for n in range(2):
                return_p(h, n).start()

        @pl.when(has_right)
        def _():
            from_right(h, i, 2 * i + k)

        hand_e(i, 2 * i + k).start()
        return carry

    lax.fori_loop(0, 2, stage, 0)

    def combine(b):
        load_old(b).wait()
        for s in range(SLOTS):
            which = codes[s] + 1
            flags = mask[s]
            out[s, b, :ST, :] = out[s, b, :ST, :] + flags * pick[which, :ST, :]
            out[s, b, ST:, :] = out[s, b, ST:, :] + flags * pick[which, ST:, :]

    def finish_q(n, carry):
        b = 4 + n
        i, j = b // 2, lax.rem(b, 2)
        h = n // 2

        @pl.when(j == o)
        def _():
            arrival(cross.at[0, b, 1], e_r.at[i]).wait_recv()

        @pl.when((j == o) & has_right)
        def _():
            part = pl.ds(3 - k, 2)
            arrival(cross.at[0, b, part], d_r.at[h]).wait_recv()

        @pl.when(swaps & has_right)
        def _():
            arrival(got_q.at[n], q_r.at[n]).wait_recv()

        pick[1] = cross[0, b, 0]
        pick[2] = cross[0, b, 1]
        pick[4] = cross[0, b, 3]
        pick[pl.ds(3 + 2 * o, 1)] = cross[0, b, pl.ds(2 + 2 * o, 1)]
        pick[pl.ds(3 + 2 * k, 1)] = got_q[pl.ds(n, 1)].astype(jnp.float32)
        combine(b)
        return carry

    lax.fori_loop(0, 4, finish_q, 0)

    def finish_p(b, carry):
        i, j = b // 2, lax.rem(b, 2)

        @pl.when(j == o)
        def _():
            arrival(cross.at[0, b, 1], e_r.at[i]).wait_recv()

        @pl.when(has_right)
        def _():
            arrival(got_p.at[b], p_r.at[b]).wait_recv()

        pick[1] = cross[0, b, 0]
        pick[2] = cross[0, b, 1]
        for n in range(3):
            pick[3 + n] = got_p[b, n].astype(jnp.float32)
        combine(b)
        return carry

    lax.fori_loop(0, 4, finish_p, 0)

    for i in range(4):
        die(i).wait_send()
        hand_e(i, 2 * i + k).wait_send()

    @pl.when(swaps)
    def _():
        for b in range(BANDS):
            vertical(b).wait_send()

    @pl.when(has_left)
    def _():
        for b in range(4):
            across(4 + b).wait_send()
        for h in range(2):
            for n in range(2):
                return_p(h, n).wait_send()

    @pl.when(has_right)
    def _():
        for b in range(4):
            across(b).wait_send()
        for h in range(2):
            hand_d(h, 4 + 2 * h + k, o).wait_send()

    for h in range(2):

        @pl.when(has_right & has_above)
        def _():
            return_q(h, 0).wait_send()

        @pl.when(has_right & has_below)
        def _():
            return_q(h, 1).wait_send()


def body(spectra, partner_codes, range_bits, old_stacks):
    codes = partner_codes.reshape(SLOTS)
    bits = jnp.transpose(range_bits, (0, 2, 4, 1, 3)).reshape(SLOTS * WORDS, 1, ST)
    blocks = spectra.reshape(SEG, 2 * ST, BANDS * BW)
    old = old_stacks.reshape(SLOTS, BANDS, 2 * ST, ST)
    dma = pltpu.SemaphoreType.DMA
    updated = pl.pallas_call(
        kernel,
        out_shape=pltpu.VMEM((SLOTS, BANDS, 2 * ST, ST), jnp.float32),
        in_specs=[
            pl.BlockSpec(memory_space=pltpu.SMEM),
            pl.BlockSpec(memory_space=pltpu.VMEM),
            pl.BlockSpec(memory_space=pl.ANY),
            pl.BlockSpec(memory_space=pl.ANY),
        ],
        out_specs=pl.BlockSpec(memory_space=pltpu.VMEM),
        scratch_shapes=[
            pltpu.VMEM((PLACES, SEG, 2 * ST, BW), jnp.bfloat16),
            pltpu.VMEM((2, BANDS, SLOTS, 2 * ST, ST), jnp.float32),
            pltpu.VMEM((SLOTS, ST, ST), jnp.float32),
            pltpu.VMEM((SLOTS + 1, 2 * ST, ST), jnp.float32),
            pltpu.VMEM((2, 2, 3, 2 * ST, ST), jnp.bfloat16),
            pltpu.VMEM((4, 3, 2 * ST, ST), jnp.bfloat16),
            pltpu.VMEM((2, 2, 2 * ST, ST), jnp.bfloat16),
            pltpu.VMEM((4, 2 * ST, ST), jnp.bfloat16),
            dma((BANDS,)), dma((BANDS,)),
            dma((4,)), dma((4,)), dma((8,)), dma((8,)), dma((8,)), dma((8,)),
            dma((2, 2)), dma((4,)), dma((2, 2)), dma((4,)),
            dma((4,)), dma((4,)), dma((2,)), dma((2,)),
        ],
        compiler_params=pltpu.CompilerParams(
            collective_id=0, has_side_effects=True, vmem_limit_bytes=52 * 1024 * 1024
        ),
    )(codes, bits, blocks, old)
    return updated.reshape(old_stacks.shape)


def solution(mesh):
    return jax.shard_map(
        body,
        mesh=mesh,
        in_specs=(
            P("gx", "gy", None, None, None, None),
            P("gx", "gy", None),
            P("gx", "gy", None, None, None),
            P("gx", "gy", None, None, None, None, None),
        ),
        out_specs=P("gx", "gy", None, None, None, None, None),
        check_vma=False,
    )
```

```python
import math

import jax
import jax.numpy as jnp
from jax import lax
from jax.experimental import pallas as pl
from jax.experimental.pallas import tpu as pltpu
from jax.sharding import PartitionSpec as P

EPSILON = 1e-06
MESH = pl.DeviceIdType.MESH
ROWS = 8
COLS = 16
ST = 128
SEG = 3
BANDS = 8
BW = 512
SLOTS = 5
WORDS = 5
SCALE = 1.0 / math.sqrt(SEG * BW)

OWN, OTHER, UPPER, LOWER, LEFT, RIGHT, HALF, PLACES = 0, 8, 12, 16, 20, 24, 28, 30
CUT = 4
HB = BW // 2
HR = ST // 2


def whiten(w, place):
    def rows_of(t, carry):
        rows = pl.ds(pl.multiple_of(t * 16, 16), 16)
        total = jnp.zeros((16, BW), jnp.float32)
        for s in range(SEG):
            for c in range(2):
                x = w[place, s, c, rows, :].astype(jnp.float32)
                total = total + x * x
        power = jnp.sum(total, axis=-1, keepdims=True) * (1.0 / (SEG * 2 * BW))
        gain = lax.rsqrt(power + EPSILON)
        for s in range(SEG):
            for c in range(2):
                x = w[place, s, c, rows, :].astype(jnp.float32)
                w[place, s, c, rows, :] = (x * gain).astype(jnp.bfloat16)
        return carry

    lax.fori_loop(0, ST // 16, rows_of, 0, unroll=4)


def pair(w, x, y, first=0, rows=ST, bins=BW):
    total = None
    for s in range(SEG):
        part = lax.dot_general(
            w[x, s, :, first:first + rows, :bins].reshape(2 * rows, bins),
            w[y, s, :, :, :bins].reshape(2 * ST, bins),
            (((1,), (1,)), ((), ())), preferred_element_type=jnp.float32,
        )
        total = part if total is None else total + part
    real = (total[:rows, :ST] + total[rows:, ST:]) * SCALE
    imag = (total[rows:, :ST] - total[:rows, ST:]) * SCALE
    return real, imag


def turn(h, core):
    return jnp.where(h == 0, 6 - core, CUT + 3 * core)


def kernel(
    codes, bits, spectra, old, out,
    w, cross, mask, pick, sent_p, got_p, sent_q, got_q, sent_m, got_m,
    load_sem, old_sem,
    die_s, die_r, row_s, row_r, col_s, col_r,
    p_s, p_r, q_s, q_r, e_s, e_r, d_s, d_r,
    half_s, half_r, m_s, m_r, ready_right, ready_below,
):
    gx = lax.axis_index("gx")
    gy = lax.axis_index("gy")
    k = lax.rem(gx, 2)
    o = 1 - k
    base = gx - k
    right = lax.rem(gy + 1, COLS)
    left = lax.rem(gy + COLS - 1, COLS)
    above = lax.rem(base + ROWS - 2, ROWS)
    below = lax.rem(base + 2, ROWS)
    has_left, has_right = gy > 0, gy < COLS - 1
    has_above, has_below = base > 0, base < ROWS - 2
    swaps = jnp.where(k == 0, base > 0, base < ROWS - 2)
    hears = jnp.where(k == 0, base < ROWS - 2, base > 0)

    def band(b):
        return spectra.at[:, :, :, pl.ds(pl.multiple_of(b * BW, BW), BW)]

    def remote(src, dst, send, recv, row, col):
        return pltpu.make_async_remote_copy(
            src_ref=src, dst_ref=dst, send_sem=send, recv_sem=recv,
            device_id=(row, col), device_id_type=MESH,
        )

    def load(b):
        return pltpu.make_async_copy(band(b), w.at[OWN + b], load_sem.at[b])

    def load_old(b):
        return pltpu.make_async_copy(old.at[:, b], out.at[:, b], old_sem.at[b])

    def die(i):
        return remote(band(2 * i + o), w.at[OTHER + i], die_s.at[i], die_r.at[i], base + o, gy)

    def across(b):
        if b == CUT:
            part = pl.ds(HB, HB)
            at = RIGHT + 2 + k
            return remote(
                w.at[OWN + CUT, :, :, :, part], w.at[at, :, :, :, part],
                row_s.at[b], row_r.at[at - LEFT], base, left,
            )
        h, j = {0: 0, 1: 0, 2: 1, 3: 1, 6: 0, 5: 0, 7: 1}[b], b % 2
        at = (LEFT if b < CUT else RIGHT) + 2 * h + k
        return remote(
            band(b), w.at[at], row_s.at[b], row_r.at[at - LEFT],
            base + j, right if b < CUT else left,
        )

    def half(c):
        rows, part = pl.ds(c * HR, HR), pl.ds(0, HB)
        return remote(
            w.at[OWN + CUT, :, :, rows, part], w.at[HALF + k, :, :, rows, part],
            half_s.at[c], half_r.at[c, k], base, right,
        )

    def return_m(c, i):
        rows = pl.ds(c * HR, HR)
        return remote(
            sent_m.at[i, :, :, rows], got_m.at[:, :, rows], m_s.at[c, i], m_r.at[c],
            base + i, left,
        )

    def vertical(b):
        i, j = b // 2, b % 2
        at = LOWER - 4 * k + i
        chip = jnp.where(k == 0, above, below)
        return remote(band(b), w.at[at], col_s.at[b], col_r.at[at - UPPER], chip + j, gy)

    def return_p(h, i):
        return remote(
            sent_p.at[h, i], got_p.at[2 * h + k], p_s.at[h, i], p_r.at[2 * h + k],
            base + i, left,
        )

    def return_q(h, i):
        row = above + 1 if i == 0 else below
        return remote(
            sent_q.at[h, i], got_q.at[2 * h + k], q_s.at[h, i], q_r.at[2 * h + k], row, gy
        )

    def hand_e(i, b):
        return remote(
            cross.at[1, b, 1], cross.at[0, b, 1], e_s.at[i], e_r.at[i], base + o, gy
        )

    def hand_d(h, b, owner):
        part = pl.ds(3 - owner, 2)
        return remote(
            cross.at[1, b, part], cross.at[0, b, part], d_s.at[h], d_r.at[h], base + o, gy
        )

    def arrival(dst, sem):
        return remote(dst, dst, load_sem.at[0], sem, base + o, gy)

    barrier = pltpu.get_barrier_semaphore()

    def greet(there, sem, row, col):
        @pl.when(there)
        def _():
            pl.semaphore_signal(sem, inc=1, device_id=(row, col), device_id_type=MESH)

    def count(there):
        return there.astype(jnp.int32)

    pl.semaphore_signal(barrier, inc=1, device_id=(base + o, gy), device_id_type=MESH)
    for n in range(2):
        greet(has_right, barrier, base + n, right)
    greet(has_below, barrier, below, gy)
    greet(has_below & (k == 1), barrier, below + 1, gy)

    def start_load(b, carry):
        load(lax.rem(b + CUT, BANDS)).start()
        return carry

    lax.fori_loop(0, BANDS, start_load, 0)
    pl.semaphore_wait(barrier, 1 + 2 * count(has_left) + (2 - k) * count(has_above))
    for n in range(2):
        greet(has_left, ready_right, base + n, left)
    greet(has_above, ready_below, above + 1, gy)
    greet(has_above & (k == 0), ready_below, above, gy)

    vertical_order = (0, 5, 1, 7, 2, 6, 4, 3)

    @pl.when(has_left)
    def _():
        for b in (5, 7, 6):
            across(b).start()

    @pl.when(has_above & (k == 0))
    def _():
        for b in vertical_order:
            vertical(b).start()

    for i in (0, 3, 2, 1):
        die(i).start()

    @pl.when(has_right)
    def _():
        pl.semaphore_wait(ready_right, 2)
        for b in range(4):
            across(b).start()

    @pl.when(has_below)
    def _():
        pl.semaphore_wait(ready_below, 1 + k)

    @pl.when(has_below & (k == 1))
    def _():
        for b in vertical_order:
            vertical(b).start()

    def start_old(b, carry):
        load_old(b).start()
        return carry

    lax.fori_loop(0, BANDS, start_old, 0)

    column = lax.broadcasted_iota(jnp.int32, (ST, ST), 0)
    word = column // 30
    shift = column - word * 30
    for s in range(SLOTS):
        chosen = jnp.zeros((ST, ST), jnp.int32)
        for n in range(WORDS):
            chosen = jnp.where(word == n, bits[s * WORDS + n], chosen)
        flags = (lax.shift_right_logical(chosen, shift) & 1).astype(jnp.float32)
        mask[s] = flags.T
    pick[0] = jnp.zeros((2 * ST, ST), jnp.float32)

    def own_band(n, carry):
        b = lax.rem(n + CUT, BANDS)
        load(b).wait()
        whiten(w, OWN + b)

        @pl.when(n == 1)
        def _():
            @pl.when(has_left)
            def _():
                across(CUT).start()

            @pl.when(has_right)
            def _():
                for c in range(2):
                    half(c).start()

        real, imag = pair(w, OWN + b, OWN + b)
        cross[0, b, 0, :ST, :] = real
        cross[0, b, 0, ST:, :] = imag
        return carry

    lax.fori_loop(0, BANDS, own_band, 0)

    @pl.when(k == 0)
    def _():
        for n in range(2):
            w[RIGHT + 2 + n, :, :, :, :HB] = jnp.zeros((SEG, 2, ST, HB), jnp.bfloat16)

    def chip_block(a, i):
        return jnp.where(a == k, OWN + 2 * i + k, OTHER + i)

    def put(owner, b, code, value):
        side = jnp.where(owner == k, 0, 1)
        cross[side, b, code, :ST, :] = value[0]
        cross[side, b, code, ST:, :] = value[1]

    def common(i):
        arrival(w.at[OTHER + i], die_r.at[i]).wait_recv()

        @pl.when(has_above)
        def _():
            arrival(w.at[UPPER + i], col_r.at[i]).wait_recv()

        @pl.when(has_below)
        def _():
            arrival(w.at[LOWER + i], col_r.at[4 + i]).wait_recv()

        def whiten_one(n, carry):
            whiten(w, OTHER + 4 * n + i)
            return carry

        lax.fori_loop(0, 3, whiten_one, 0)

    def whiten_two(place):
        def whiten_one(n, carry):
            whiten(w, place + n)
            return carry

        lax.fori_loop(0, 2, whiten_one, 0)

    def own_column(i):
        def below_pair(a, carry):
            x = chip_block(a, i)
            y = jnp.where(a == 0, chip_block(1, i), LOWER + i)
            put(a, 2 * i + k, 1, pair(w, x, y))
            return carry

        lax.fori_loop(0, 2, below_pair, 0)

    def from_left(h, i):
        for n in range(2):
            arrival(w.at[LEFT + 2 * h + n], row_r.at[2 * h + n]).wait_recv()
        whiten_two(LEFT + 2 * h)

        def left_pair(n, carry):
            own, a = n // 2, n % 2
            real, imag = pair(w, LEFT + 2 * h + own, chip_block(a, i))
            sent_p[h, own, 1 + a - own, :ST, :] = real.astype(jnp.bfloat16)
            sent_p[h, own, 1 + a - own, ST:, :] = imag.astype(jnp.bfloat16)
            return carry

        lax.fori_loop(0, 4, left_pair, 0)

        def left_corner(own, carry):
            real, imag = pair(w, LEFT + 2 * h + own, UPPER + 4 * own + i)
            sent_p[h, own, 2 * own, :ST, :] = real.astype(jnp.bfloat16)
            sent_p[h, own, 2 * own, ST:, :] = imag.astype(jnp.bfloat16)
            return carry

        lax.fori_loop(0, 2, left_corner, 0)

    def from_right(h, i, b):
        cut = (h == 1) & (k == 0)

        @pl.when(cut)
        def _():
            for n in range(2):
                part = w.at[RIGHT + 2 + n, :, :, :, pl.ds(HB, HB)]
                arrival(part, row_r.at[6 + n]).wait_recv()

        @pl.when(jnp.logical_not(cut))
        def _():
            for n in range(2):
                arrival(w.at[RIGHT + 2 * h + n], row_r.at[4 + 2 * h + n]).wait_recv()
            whiten_two(RIGHT + 2 * h)

        def right_corner(n, carry):
            real, imag = pair(w, UPPER + 4 * n + i, RIGHT + 2 * h + n)
            sent_q[h, n, :ST, :] = real.astype(jnp.bfloat16)
            sent_q[h, n, ST:, :] = imag.astype(jnp.bfloat16)
            return carry

        lax.fori_loop(0, 2, right_corner, 0)

        def right_pair(n, carry):
            a, far = n // 2, n % 2
            put(a, b, 3 + far - a, pair(w, chip_block(a, i), RIGHT + 2 * h + far))
            return carry

        lax.fori_loop(0, 4, right_pair, 0)

        @pl.when(has_above)
        def _():
            return_q(h, 0).start()

        @pl.when(has_below)
        def _():
            return_q(h, 1).start()

        hand_d(h, b, o).start()

    def stage(h, carry):
        common(h)

        @pl.when(has_left)
        def _():
            from_left(h, h)

        own_column(h)

        @pl.when(has_left)
        def _():
            for n in range(2):
                return_p(h, n).start()

        b = turn(h, k)
        i = b // 2
        hand_e(h, 2 * h + k).start()
        common(i)
        own_column(i)

        @pl.when(has_right)
        def _():
            from_right(h, i, b)

        hand_e(i, b).start()
        return carry

    lax.fori_loop(0, 2, stage, 0)

    def half_products(c):
        i = CUT // 2
        for n in range(2):
            part = w.at[HALF + n, :, :, pl.ds(c * HR, HR), pl.ds(0, HB)]
            arrival(part, half_r.at[c, n]).wait_recv()

        def half_put(own, code, y):
            real, imag = pair(w, HALF + own, y, c * HR, HR, HB)
            sent_m[own, code, 0, c * HR:(c + 1) * HR, :] = real.astype(jnp.bfloat16)
            sent_m[own, code, 1, c * HR:(c + 1) * HR, :] = imag.astype(jnp.bfloat16)

        def half_pair(n, carry):
            own, a = n // 2, n % 2
            half_put(own, 1 + a - own, chip_block(a, i))
            return carry

        lax.fori_loop(0, 4, half_pair, 0)

        def half_corner(own, carry):
            half_put(own, 2 * own, UPPER + 4 * own + i)
            return carry

        lax.fori_loop(0, 2, half_corner, 0)

    def combine(b):
        load_old(b).wait()
        for s in range(SLOTS):
            which = codes[s] + 1
            flags = mask[s]
            out[s, b, :ST, :] = out[s, b, :ST, :] + flags * pick[which, :ST, :]
            out[s, b, ST:, :] = out[s, b, ST:, :] + flags * pick[which, ST:, :]

    def await_q(n, b):
        h, j = n // 2, lax.rem(n, 2)

        @pl.when(j == o)
        def _():
            arrival(cross.at[0, b, 1], e_r.at[b // 2]).wait_recv()

        @pl.when((j == o) & has_right)
        def _():
            arrival(cross.at[0, b, pl.ds(3 - k, 2)], d_r.at[h]).wait_recv()

        @pl.when(swaps & has_right)
        def _():
            arrival(got_q.at[n], q_r.at[n]).wait_recv()

    def finish_q(n):
        b = turn(n // 2, lax.rem(n, 2))
        await_q(n, b)
        pick[1] = cross[0, b, 0]
        pick[2] = cross[0, b, 1]
        pick[4] = cross[0, b, 3]
        pick[pl.ds(3 + 2 * o, 1)] = cross[0, b, pl.ds(2 + 2 * o, 1)]
        pick[pl.ds(3 + 2 * k, 1)] = got_q[pl.ds(n, 1)].astype(jnp.float32)
        combine(b)

    for c in range(2):

        @pl.when(has_left & (k == 0))
        def _():
            half_products(c)

        finish_q(c)

        @pl.when(has_left & (k == 0))
        def _():
            for n in range(2):
                return_m(c, n).start()

    finish_q(3)

    def finish_p(b, carry):
        i, j = b // 2, lax.rem(b, 2)

        @pl.when(j == o)
        def _():
            arrival(cross.at[0, b, 1], e_r.at[i]).wait_recv()

        @pl.when(has_right)
        def _():
            arrival(got_p.at[b], p_r.at[b]).wait_recv()

        pick[1] = cross[0, b, 0]
        pick[2] = cross[0, b, 1]
        for n in range(3):
            pick[3 + n] = got_p[b, n].astype(jnp.float32)
        combine(b)
        return carry

    lax.fori_loop(0, 4, finish_p, 0)

    await_q(2, CUT)

    @pl.when(has_right)
    def _():
        for c in range(2):
            arrival(got_m.at[:, :, pl.ds(c * HR, HR)], m_r.at[c]).wait_recv()

    pick[1] = cross[0, CUT, 0]
    pick[2] = cross[0, CUT, 1]
    for n in range(3):
        partial = got_m[n].reshape(2 * ST, ST).astype(jnp.float32)
        near = got_q[2].astype(jnp.float32)
        pick[3 + n] = partial + jnp.where(k * 2 == n, near, cross[0, CUT, 2 + n])
    combine(CUT)

    for i in range(4):
        die(i).wait_send()
        hand_e(i, 2 * i + k).wait_send()

    @pl.when(swaps)
    def _():
        for b in range(BANDS):
            vertical(b).wait_send()

    @pl.when(has_left)
    def _():
        for b in range(4):
            across(4 + b).wait_send()
        for h in range(2):
            for n in range(2):
                return_p(h, n).wait_send()

    @pl.when(has_left & (k == 0))
    def _():
        for c in range(2):
            for n in range(2):
                return_m(c, n).wait_send()

    @pl.when(has_right)
    def _():
        for b in range(4):
            across(b).wait_send()
        for h in range(2):
            hand_d(h, turn(h, k), o).wait_send()
        for c in range(2):
            half(c).wait_send()

    for h in range(2):

        @pl.when(has_right & has_above)
        def _():
            return_q(h, 0).wait_send()

        @pl.when(has_right & has_below)
        def _():
            return_q(h, 1).wait_send()


def body(spectra, partner_codes, range_bits, old_stacks):
    codes = partner_codes.reshape(SLOTS)
    bits = jnp.transpose(range_bits, (0, 2, 4, 1, 3)).reshape(SLOTS * WORDS, 1, ST)
    blocks = spectra.reshape(SEG, 2, ST, BANDS * BW)
    old = old_stacks.reshape(SLOTS, BANDS, 2 * ST, ST)
    dma = pltpu.SemaphoreType.DMA
    updated = pl.pallas_call(
        kernel,
        out_shape=pltpu.VMEM((SLOTS, BANDS, 2 * ST, ST), jnp.float32),
        in_specs=[
            pl.BlockSpec(memory_space=pltpu.SMEM),
            pl.BlockSpec(memory_space=pltpu.VMEM),
            pl.BlockSpec(memory_space=pl.ANY),
            pl.BlockSpec(memory_space=pl.ANY),
        ],
        out_specs=pl.BlockSpec(memory_space=pltpu.VMEM),
        scratch_shapes=[
            pltpu.VMEM((PLACES, SEG, 2, ST, BW), jnp.bfloat16),
            pltpu.VMEM((2, BANDS, SLOTS, 2 * ST, ST), jnp.float32),
            pltpu.VMEM((SLOTS, ST, ST), jnp.float32),
            pltpu.VMEM((SLOTS + 1, 2 * ST, ST), jnp.float32),
            pltpu.VMEM((2, 2, 3, 2 * ST, ST), jnp.bfloat16),
            pltpu.VMEM((4, 3, 2 * ST, ST), jnp.bfloat16),
            pltpu.VMEM((2, 2, 2 * ST, ST), jnp.bfloat16),
            pltpu.VMEM((4, 2 * ST, ST), jnp.bfloat16),
            pltpu.VMEM((2, 3, 2, ST, ST), jnp.bfloat16),
            pltpu.VMEM((3, 2, ST, ST), jnp.bfloat16),
            dma((BANDS,)), dma((BANDS,)),
            dma((4,)), dma((4,)), dma((8,)), dma((8,)), dma((8,)), dma((8,)),
            dma((2, 2)), dma((4,)), dma((2, 2)), dma((4,)),
            dma((4,)), dma((4,)), dma((2,)), dma((2,)),
            dma((2,)), dma((2, 2)), dma((2, 2)), dma((2,)),
            pltpu.SemaphoreType.REGULAR, pltpu.SemaphoreType.REGULAR,
        ],
        compiler_params=pltpu.CompilerParams(
            collective_id=0, has_side_effects=True, vmem_limit_bytes=52 * 1024 * 1024
        ),
    )(codes, bits, blocks, old)
    return updated.reshape(old_stacks.shape)


def solution(mesh):
    return jax.shard_map(
        body,
        mesh=mesh,
        in_specs=(
            P("gx", "gy", None, None, None, None),
            P("gx", "gy", None),
            P("gx", "gy", None, None, None),
            P("gx", "gy", None, None, None, None, None),
        ),
        out_specs=P("gx", "gy", None, None, None, None, None),
        check_vma=False,
    )
```

```python
import math

import jax
import jax.numpy as jnp
from jax import lax
from jax.experimental import pallas as pl
from jax.experimental.pallas import tpu as pltpu
from jax.sharding import PartitionSpec as P

EPSILON = 1e-06
MESH = pl.DeviceIdType.MESH
ROWS = 8
COLS = 16
ST = 128
SEG = 3
BANDS = 8
BW = 512
SLOTS = 5
WORDS = 5
SCALE = 1.0 / math.sqrt(SEG * BW)

OWN, OTHER, UPPER, LOWER, LEFT, RIGHT, HALF, PLACES = 0, 8, 12, 16, 20, 24, 28, 30
CUT = 4
HB = BW // 2
HR = ST // 2


def whiten(w, place):
    def rows_of(t, carry):
        rows = pl.ds(pl.multiple_of(t * 16, 16), 16)
        total = jnp.zeros((16, BW), jnp.float32)
        for s in range(SEG):
            for c in range(2):
                x = w[place, s, c, rows, :].astype(jnp.float32)
                total = total + x * x
        power = jnp.sum(total, axis=-1, keepdims=True) * (1.0 / (SEG * 2 * BW))
        gain = lax.rsqrt(power + EPSILON)
        for s in range(SEG):
            for c in range(2):
                x = w[place, s, c, rows, :].astype(jnp.float32)
                w[place, s, c, rows, :] = (x * gain).astype(jnp.bfloat16)
        return carry

    lax.fori_loop(0, ST // 16, rows_of, 0, unroll=4)


def pair(w, x, y, first=0, rows=ST, bins=BW):
    total = None
    for s in range(SEG):
        part = lax.dot_general(
            w[x, s, :, first:first + rows, :bins].reshape(2 * rows, bins),
            w[y, s, :, :, :bins].reshape(2 * ST, bins),
            (((1,), (1,)), ((), ())), preferred_element_type=jnp.float32,
        )
        total = part if total is None else total + part
    real = (total[:rows, :ST] + total[rows:, ST:]) * SCALE
    imag = (total[rows:, :ST] - total[:rows, ST:]) * SCALE
    return real, imag


def turn(h, core):
    return jnp.where(h == 0, 6 - core, CUT + 3 * core)


def kernel(
    codes, bits, spectra, old, out,
    w, cross, mask, pick, sent_p, got_p, sent_q, got_q, sent_m, got_m,
    load_sem, old_sem,
    die_s, die_r, row_s, row_r, col_s, col_r,
    p_s, p_r, q_s, q_r, e_s, e_r, d_s, d_r,
    half_s, half_r, m_s, m_r, ready_right, ready_below,
):
    gx = lax.axis_index("gx")
    gy = lax.axis_index("gy")
    k = lax.rem(gx, 2)
    o = 1 - k
    base = gx - k
    right = lax.rem(gy + 1, COLS)
    left = lax.rem(gy + COLS - 1, COLS)
    above = lax.rem(base + ROWS - 2, ROWS)
    below = lax.rem(base + 2, ROWS)
    has_left, has_right = gy > 0, gy < COLS - 1
    has_above, has_below = base > 0, base < ROWS - 2
    swaps = jnp.where(k == 0, base > 0, base < ROWS - 2)

    def remote(src, dst, send, recv, row, col):
        return pltpu.make_async_remote_copy(
            src_ref=src, dst_ref=dst, send_sem=send, recv_sem=recv,
            device_id=(row, col), device_id_type=MESH,
        )

    def load(b):
        bins = pl.ds(b * BW, BW)
        return pltpu.make_async_copy(spectra.at[:, :, :, bins], w.at[OWN + b], load_sem.at[b])

    def load_old(b):
        return pltpu.make_async_copy(old.at[:, b], out.at[:, b], old_sem.at[b])

    def die(i):
        return remote(
            w.at[OWN + 2 * i + o], w.at[OTHER + i], die_s.at[i], die_r.at[i], base + o, gy
        )

    def across(b):
        if b == CUT:
            part = pl.ds(HB, HB)
            at = RIGHT + 2 + k
            return remote(
                w.at[OWN + CUT, :, :, :, part], w.at[at, :, :, :, part],
                row_s.at[b], row_r.at[at - LEFT], base, left,
            )
        h, j = {0: 0, 1: 0, 2: 1, 3: 1, 6: 0, 5: 0, 7: 1}[b], b % 2
        at = (LEFT if b < CUT else RIGHT) + 2 * h + k
        return remote(
            w.at[OWN + b], w.at[at], row_s.at[b], row_r.at[at - LEFT],
            base + j, right if b < CUT else left,
        )

    def half(c):
        rows, part = pl.ds(c * HR, HR), pl.ds(0, HB)
        return remote(
            w.at[OWN + CUT, :, :, rows, part], w.at[HALF + k, :, :, rows, part],
            half_s.at[c], half_r.at[c, k], base, right,
        )

    def return_m(c, i):
        rows = pl.ds(c * HR, HR)
        return remote(
            sent_m.at[i, :, :, rows], got_m.at[:, :, rows], m_s.at[c, i], m_r.at[c],
            base + i, left,
        )

    def chip_block(a, i):
        return jnp.where(a == k, OWN + 2 * i + k, OTHER + i)

    def vertical(a, i):
        row, at = (above, LOWER) if a == 0 else (below, UPPER)
        return remote(
            w.at[chip_block(a, i)], w.at[at + i], col_s.at[a, i], col_r.at[at + i - UPPER],
            row + k, gy,
        )

    def return_p(h, i):
        return remote(
            sent_p.at[h, i], got_p.at[2 * h + k], p_s.at[h, i], p_r.at[2 * h + k],
            base + i, left,
        )

    def return_q(h, i):
        row = above + 1 if i == 0 else below
        return remote(
            sent_q.at[h, i], got_q.at[2 * h + k], q_s.at[h, i], q_r.at[2 * h + k], row, gy
        )

    def hand_e(i, b):
        return remote(
            cross.at[1, b, 1], cross.at[0, b, 1], e_s.at[i], e_r.at[i], base + o, gy
        )

    def hand_d(h, b, owner):
        part = pl.ds(3 - owner, 2)
        return remote(
            cross.at[1, b, part], cross.at[0, b, part], d_s.at[h], d_r.at[h], base + o, gy
        )

    def arrival(dst, sem):
        return remote(dst, dst, load_sem.at[0], sem, base + o, gy)

    barrier = pltpu.get_barrier_semaphore()

    def greet(there, sem, row, col):
        @pl.when(there)
        def _():
            pl.semaphore_signal(sem, inc=1, device_id=(row, col), device_id_type=MESH)

    def count(there):
        return there.astype(jnp.int32)

    pl.semaphore_signal(barrier, inc=1, device_id=(base + o, gy), device_id_type=MESH)
    for n in range(2):
        greet(has_right, barrier, base + n, right)
    greet(has_below, barrier, below, gy)
    greet(has_below & (k == 1), barrier, below + 1, gy)

    order = (5, 0, 1, 6, 7, 2, CUT, 3)
    for b in order:
        load(b).start()

    def answer():
        pl.semaphore_wait(barrier, 1 + 2 * count(has_left) + (2 - k) * count(has_above))
        for n in range(2):
            greet(has_left, ready_right, base + n, left)
        greet(has_above, ready_below, above + 1, gy)
        greet(has_above & (k == 0), ready_below, above, gy)

    def send(b):
        if b > CUT:

            @pl.when(has_left)
            def _():
                across(b).start()

        @pl.when(k != b % 2)
        def _():
            die(b // 2).start()

        there = has_above if b % 2 == 0 else has_below

        @pl.when(there & (k == b % 2))
        def _():
            vertical(b % 2, b // 2).start()

        if b < CUT:

            @pl.when(has_right)
            def _():
                across(b).start()

        if b == CUT:

            @pl.when(has_left)
            def _():
                across(b).start()

    for n, b in enumerate(order):
        load(b).wait()
        whiten(w, OWN + b)
        if n == 1:
            answer()

            @pl.when(has_right)
            def _():
                pl.semaphore_wait(ready_right, 2)

            @pl.when(has_below)
            def _():
                pl.semaphore_wait(ready_below, 1 + k)

        if n >= 1:
            send(order[n - 1])

    def start_old(b, carry):
        load_old(b).start()
        return carry

    lax.fori_loop(0, BANDS, start_old, 0)

    send(order[-1])

    @pl.when(has_right)
    def _():
        for c in range(2):
            half(c).start()

    def pass_on(a):
        for n in range(4):
            i = ((2, 0, 3, 1), (0, 3, 1, 2))[a][n]
            arrival(w.at[OTHER + i], die_r.at[i]).wait_recv()

            @pl.when(has_below if a == 1 else has_above)
            def _():
                vertical(a, i).start()

    for a in range(2):

        @pl.when(a != k)
        def _():
            pass_on(a)

    column = lax.broadcasted_iota(jnp.int32, (ST, ST), 0)
    word = column // 30
    shift = column - word * 30
    for s in range(SLOTS):
        chosen = jnp.zeros((ST, ST), jnp.int32)
        for n in range(WORDS):
            chosen = jnp.where(word == n, bits[s * WORDS + n], chosen)
        flags = (lax.shift_right_logical(chosen, shift) & 1).astype(jnp.float32)
        mask[s] = flags.T
    pick[0] = jnp.zeros((2 * ST, ST), jnp.float32)

    def own_band(b, carry):
        real, imag = pair(w, OWN + b, OWN + b)
        cross[0, b, 0, :ST, :] = real
        cross[0, b, 0, ST:, :] = imag
        return carry

    lax.fori_loop(0, BANDS, own_band, 0)

    @pl.when(k == 0)
    def _():
        for n in range(2):
            w[RIGHT + 2 + n, :, :, :, :HB] = jnp.zeros((SEG, 2, ST, HB), jnp.bfloat16)

    def put(owner, b, code, value):
        side = jnp.where(owner == k, 0, 1)
        cross[side, b, code, :ST, :] = value[0]
        cross[side, b, code, ST:, :] = value[1]

    def common(i):
        @pl.when(has_above)
        def _():
            arrival(w.at[UPPER + i], col_r.at[i]).wait_recv()

        @pl.when(has_below)
        def _():
            arrival(w.at[LOWER + i], col_r.at[4 + i]).wait_recv()

    def own_column(i):
        def below_pair(a, carry):
            x = chip_block(a, i)
            y = jnp.where(a == 0, chip_block(1, i), LOWER + i)
            put(a, 2 * i + k, 1, pair(w, x, y))
            return carry

        lax.fori_loop(0, 2, below_pair, 0)

    def from_left(h, i):
        for n in range(2):
            arrival(w.at[LEFT + 2 * h + n], row_r.at[2 * h + n]).wait_recv()

        def left_pair(n, carry):
            own, a = n // 2, n % 2
            real, imag = pair(w, LEFT + 2 * h + own, chip_block(a, i))
            sent_p[h, own, 1 + a - own, :ST, :] = real.astype(jnp.bfloat16)
            sent_p[h, own, 1 + a - own, ST:, :] = imag.astype(jnp.bfloat16)
            return carry

        lax.fori_loop(0, 4, left_pair, 0)

        def left_corner(own, carry):
            real, imag = pair(w, LEFT + 2 * h + own, UPPER + 4 * own + i)
            sent_p[h, own, 2 * own, :ST, :] = real.astype(jnp.bfloat16)
            sent_p[h, own, 2 * own, ST:, :] = imag.astype(jnp.bfloat16)
            return carry

        lax.fori_loop(0, 2, left_corner, 0)

    def from_right(h, i, b):
        cut = (h == 1) & (k == 0)

        @pl.when(cut)
        def _():
            for n in range(2):
                part = w.at[RIGHT + 2 + n, :, :, :, pl.ds(HB, HB)]
                arrival(part, row_r.at[6 + n]).wait_recv()

        @pl.when(jnp.logical_not(cut))
        def _():
            for n in range(2):
                arrival(w.at[RIGHT + 2 * h + n], row_r.at[4 + 2 * h + n]).wait_recv()

        def right_corner(n, carry):
            real, imag = pair(w, UPPER + 4 * n + i, RIGHT + 2 * h + n)
            sent_q[h, n, :ST, :] = real.astype(jnp.bfloat16)
            sent_q[h, n, ST:, :] = imag.astype(jnp.bfloat16)
            return carry

        lax.fori_loop(0, 2, right_corner, 0)

        def right_pair(n, carry):
            a, far = n // 2, n % 2
            put(a, b, 3 + far - a, pair(w, chip_block(a, i), RIGHT + 2 * h + far))
            return carry

        lax.fori_loop(0, 4, right_pair, 0)

    def stage(h, carry):
        common(h)

        @pl.when(has_left)
        def _():
            from_left(h, h)

        own_column(h)

        @pl.when(has_left)
        def _():
            for n in range(2):
                return_p(h, n).start()

        b = turn(h, k)
        i = b // 2
        common(i)

        @pl.when(has_right)
        def _():
            from_right(h, i, b)

        hand_e(h, 2 * h + k).start()
        own_column(i)

        @pl.when(has_right)
        def _():
            hand_d(h, b, o).start()

        @pl.when(has_right & has_above)
        def _():
            return_q(h, 0).start()

        @pl.when(has_right & has_below)
        def _():
            return_q(h, 1).start()

        @pl.when(h == 1)
        def _():
            hand_e(turn(0, k) // 2, turn(0, k)).start()

        return carry

    lax.fori_loop(0, 2, stage, 0)

    def half_products(c):
        i = CUT // 2
        for n in range(2):
            part = w.at[HALF + n, :, :, pl.ds(c * HR, HR), pl.ds(0, HB)]
            arrival(part, half_r.at[c, n]).wait_recv()

        def half_put(own, code, y):
            real, imag = pair(w, HALF + own, y, c * HR, HR, HB)
            sent_m[own, code, 0, c * HR:(c + 1) * HR, :] = real.astype(jnp.bfloat16)
            sent_m[own, code, 1, c * HR:(c + 1) * HR, :] = imag.astype(jnp.bfloat16)

        def half_pair(n, carry):
            own, a = n // 2, n % 2
            half_put(own, 1 + a - own, chip_block(a, i))
            return carry

        lax.fori_loop(0, 4, half_pair, 0)

        def half_corner(own, carry):
            half_put(own, 2 * own, UPPER + 4 * own + i)
            return carry

        lax.fori_loop(0, 2, half_corner, 0)

    def combine(b):
        load_old(b).wait()
        for s in range(SLOTS):
            which = codes[s] + 1
            flags = mask[s]
            out[s, b, :ST, :] = out[s, b, :ST, :] + flags * pick[which, :ST, :]
            out[s, b, ST:, :] = out[s, b, ST:, :] + flags * pick[which, ST:, :]

    def await_q(n, b):
        h, j = n // 2, lax.rem(n, 2)

        @pl.when(j == o)
        def _():
            arrival(cross.at[0, b, 1], e_r.at[b // 2]).wait_recv()

        @pl.when((j == o) & has_right)
        def _():
            arrival(cross.at[0, b, pl.ds(3 - k, 2)], d_r.at[h]).wait_recv()

        @pl.when(swaps & has_right)
        def _():
            arrival(got_q.at[n], q_r.at[n]).wait_recv()

    def finish_q(n):
        b = turn(n // 2, lax.rem(n, 2))
        await_q(n, b)
        pick[1] = cross[0, b, 0]
        pick[2] = cross[0, b, 1]
        pick[4] = cross[0, b, 3]
        pick[pl.ds(3 + 2 * o, 1)] = cross[0, b, pl.ds(2 + 2 * o, 1)]
        pick[pl.ds(3 + 2 * k, 1)] = got_q[pl.ds(n, 1)].astype(jnp.float32)
        combine(b)

    for c in range(2):

        @pl.when(has_left & (k == 0))
        def _():
            half_products(c)

        finish_q(c)
        if c == 0:
            hand_e(turn(1, k) // 2, turn(1, k)).start()

        @pl.when(has_left & (k == 0))
        def _():
            for n in range(2):
                return_m(c, n).start()

    finish_q(3)

    def finish_p(b, carry):
        i, j = b // 2, lax.rem(b, 2)

        @pl.when(j == o)
        def _():
            arrival(cross.at[0, b, 1], e_r.at[i]).wait_recv()

        @pl.when(has_right)
        def _():
            arrival(got_p.at[b], p_r.at[b]).wait_recv()

        pick[1] = cross[0, b, 0]
        pick[2] = cross[0, b, 1]
        for n in range(3):
            pick[3 + n] = got_p[b, n].astype(jnp.float32)
        combine(b)
        return carry

    lax.fori_loop(0, 4, finish_p, 0)

    await_q(2, CUT)

    @pl.when(has_right)
    def _():
        for c in range(2):
            arrival(got_m.at[:, :, pl.ds(c * HR, HR)], m_r.at[c]).wait_recv()

    pick[1] = cross[0, CUT, 0]
    pick[2] = cross[0, CUT, 1]
    for n in range(3):
        partial = got_m[n].reshape(2 * ST, ST).astype(jnp.float32)
        near = got_q[2].astype(jnp.float32)
        pick[3 + n] = partial + jnp.where(k * 2 == n, near, cross[0, CUT, 2 + n])
    combine(CUT)

    for i in range(4):
        die(i).wait_send()
        hand_e(i, 2 * i + k).wait_send()

    @pl.when(has_above)
    def _():
        for i in range(4):
            vertical(0, i).wait_send()

    @pl.when(has_below)
    def _():
        for i in range(4):
            vertical(1, i).wait_send()

    @pl.when(has_left)
    def _():
        for b in range(4):
            across(4 + b).wait_send()
        for h in range(2):
            for n in range(2):
                return_p(h, n).wait_send()

    @pl.when(has_left & (k == 0))
    def _():
        for c in range(2):
            for n in range(2):
                return_m(c, n).wait_send()

    @pl.when(has_right)
    def _():
        for b in range(4):
            across(b).wait_send()
        for h in range(2):
            hand_d(h, turn(h, k), o).wait_send()
        for c in range(2):
            half(c).wait_send()

    for h in range(2):

        @pl.when(has_right & has_above)
        def _():
            return_q(h, 0).wait_send()

        @pl.when(has_right & has_below)
        def _():
            return_q(h, 1).wait_send()


def body(spectra, partner_codes, range_bits, old_stacks):
    codes = partner_codes.reshape(SLOTS)
    bits = jnp.transpose(range_bits, (0, 2, 4, 1, 3)).reshape(SLOTS * WORDS, 1, ST)
    blocks = spectra.reshape(SEG, 2, ST, BANDS * BW)
    old = old_stacks.reshape(SLOTS, BANDS, 2 * ST, ST)
    dma = pltpu.SemaphoreType.DMA
    updated = pl.pallas_call(
        kernel,
        out_shape=pltpu.VMEM((SLOTS, BANDS, 2 * ST, ST), jnp.float32),
        in_specs=[
            pl.BlockSpec(memory_space=pltpu.SMEM),
            pl.BlockSpec(memory_space=pltpu.VMEM),
            pl.BlockSpec(memory_space=pl.ANY),
            pl.BlockSpec(memory_space=pl.ANY),
        ],
        out_specs=pl.BlockSpec(memory_space=pltpu.VMEM),
        scratch_shapes=[
            pltpu.VMEM((PLACES, SEG, 2, ST, BW), jnp.bfloat16),
            pltpu.VMEM((2, BANDS, SLOTS, 2 * ST, ST), jnp.float32),
            pltpu.VMEM((SLOTS, ST, ST), jnp.float32),
            pltpu.VMEM((SLOTS + 1, 2 * ST, ST), jnp.float32),
            pltpu.VMEM((2, 2, 3, 2 * ST, ST), jnp.bfloat16),
            pltpu.VMEM((4, 3, 2 * ST, ST), jnp.bfloat16),
            pltpu.VMEM((2, 2, 2 * ST, ST), jnp.bfloat16),
            pltpu.VMEM((4, 2 * ST, ST), jnp.bfloat16),
            pltpu.VMEM((2, 3, 2, ST, ST), jnp.bfloat16),
            pltpu.VMEM((3, 2, ST, ST), jnp.bfloat16),
            dma((BANDS,)), dma((BANDS,)),
            dma((4,)), dma((4,)), dma((8,)), dma((8,)), dma((2, 4)), dma((8,)),
            dma((2, 2)), dma((4,)), dma((2, 2)), dma((4,)),
            dma((4,)), dma((4,)), dma((2,)), dma((2,)),
            dma((2,)), dma((2, 2)), dma((2, 2)), dma((2,)),
            pltpu.SemaphoreType.REGULAR, pltpu.SemaphoreType.REGULAR,
        ],
        compiler_params=pltpu.CompilerParams(
            collective_id=0, has_side_effects=True, vmem_limit_bytes=52 * 1024 * 1024
        ),
    )(codes, bits, blocks, old)
    return updated.reshape(old_stacks.shape)


def solution(mesh):
    return jax.shard_map(
        body,
        mesh=mesh,
        in_specs=(
            P("gx", "gy", None, None, None, None),
            P("gx", "gy", None),
            P("gx", "gy", None, None, None),
            P("gx", "gy", None, None, None, None, None),
        ),
        out_specs=P("gx", "gy", None, None, None, None, None),
        check_vma=False,
    )
```

```python
import math

import jax
import jax.numpy as jnp
from jax import lax
from jax.experimental import pallas as pl
from jax.experimental.pallas import tpu as pltpu
from jax.sharding import PartitionSpec as P

EPSILON = 1e-06
MESH = pl.DeviceIdType.MESH
ROWS = 8
COLS = 16
ST = 128
SEG = 3
BANDS = 8
BW = 512
SLOTS = 5
WORDS = 5
SCALE = 1.0 / math.sqrt(SEG * BW)

OWN, OTHER, UPPER, LOWER, LEFT, RIGHT, HALF, PLACES = 0, 8, 12, 16, 20, 24, 28, 30
CUT = 4
RAW = (0, 5)
HB = BW // 2
HR = ST // 2


def whiten(w, place, first=0, last=ST // 16):
    def rows_of(t, carry):
        rows = pl.ds(pl.multiple_of(t * 16, 16), 16)
        total = jnp.zeros((16, BW), jnp.float32)
        for s in range(SEG):
            for c in range(2):
                x = w[place, s, c, rows, :].astype(jnp.float32)
                total = total + x * x
        power = jnp.sum(total, axis=-1, keepdims=True) * (1.0 / (SEG * 2 * BW))
        gain = lax.rsqrt(power + EPSILON)
        for s in range(SEG):
            for c in range(2):
                x = w[place, s, c, rows, :].astype(jnp.float32)
                w[place, s, c, rows, :] = (x * gain).astype(jnp.bfloat16)
        return carry

    lax.fori_loop(first, last, rows_of, 0, unroll=4)


def pair(w, x, y, first=0, rows=ST, bins=BW):
    total = None
    for s in range(SEG):
        part = lax.dot_general(
            w[x, s, :, first:first + rows, :bins].reshape(2 * rows, bins),
            w[y, s, :, :, :bins].reshape(2 * ST, bins),
            (((1,), (1,)), ((), ())), preferred_element_type=jnp.float32,
        )
        total = part if total is None else total + part
    real = (total[:rows, :ST] + total[rows:, ST:]) * SCALE
    imag = (total[rows:, :ST] - total[:rows, ST:]) * SCALE
    return real, imag


def turn(h, core):
    return jnp.where(h == 0, 6 - core, CUT + 3 * core)


def kernel(
    codes, bits, spectra, old, out,
    w, cross, mask, pick, sent_p, got_p, sent_q, got_q, sent_m, got_m,
    load_sem, old_sem,
    die_s, die_r, row_s, row_r, col_s, col_r,
    p_s, p_r, q_s, q_r, e_s, e_r, d_s, d_r,
    half_s, half_r, m_s, m_r, ready_right, ready_below,
):
    gx = lax.axis_index("gx")
    gy = lax.axis_index("gy")
    k = lax.rem(gx, 2)
    o = 1 - k
    base = gx - k
    right = lax.rem(gy + 1, COLS)
    left = lax.rem(gy + COLS - 1, COLS)
    above = lax.rem(base + ROWS - 2, ROWS)
    below = lax.rem(base + 2, ROWS)
    has_left, has_right = gy > 0, gy < COLS - 1
    has_above, has_below = base > 0, base < ROWS - 2
    swaps = jnp.where(k == 0, base > 0, base < ROWS - 2)

    def remote(src, dst, send, recv, row, col):
        return pltpu.make_async_remote_copy(
            src_ref=src, dst_ref=dst, send_sem=send, recv_sem=recv,
            device_id=(row, col), device_id_type=MESH,
        )

    def load(b):
        bins = pl.ds(b * BW, BW)
        return pltpu.make_async_copy(spectra.at[:, :, :, bins], w.at[OWN + b], load_sem.at[b])

    def load_old(b):
        return pltpu.make_async_copy(old.at[:, b], out.at[:, b], old_sem.at[b])

    def die(i):
        return remote(
            w.at[OWN + 2 * i + o], w.at[OTHER + i], die_s.at[i], die_r.at[i], base + o, gy
        )

    def across(b):
        if b == CUT:
            part = pl.ds(HB, HB)
            at = RIGHT + 2 + k
            return remote(
                w.at[OWN + CUT, :, :, :, part], w.at[at, :, :, :, part],
                row_s.at[b], row_r.at[at - LEFT], base, left,
            )
        h, j = {0: 0, 1: 0, 2: 1, 3: 1, 6: 0, 5: 0, 7: 1}[b], b % 2
        at = (LEFT if b < CUT else RIGHT) + 2 * h + k
        return remote(
            spectra.at[:, :, :, pl.ds(b * BW, BW)] if b in RAW else w.at[OWN + b],
            w.at[at], row_s.at[b], row_r.at[at - LEFT],
            base + j, right if b < CUT else left,
        )

    def half(c):
        rows, part = pl.ds(c * HR, HR), pl.ds(0, HB)
        return remote(
            w.at[OWN + CUT, :, :, rows, part], w.at[HALF + k, :, :, rows, part],
            half_s.at[c], half_r.at[c, k], base, right,
        )

    def return_m(c, i):
        rows = pl.ds(c * HR, HR)
        return remote(
            sent_m.at[i, :, :, rows], got_m.at[:, :, rows], m_s.at[c, i], m_r.at[c],
            base + i, left,
        )

    def chip_block(a, i):
        return jnp.where(a == k, OWN + 2 * i + k, OTHER + i)

    def vertical(a, i):
        row, at = (above, LOWER) if a == 0 else (below, UPPER)
        return remote(
            w.at[chip_block(a, i)], w.at[at + i], col_s.at[a, i], col_r.at[at + i - UPPER],
            row + k, gy,
        )

    def return_p(h, i):
        return remote(
            sent_p.at[h, i], got_p.at[2 * h + k], p_s.at[h, i], p_r.at[2 * h + k],
            base + i, left,
        )

    def return_q(h, i):
        row = above + 1 if i == 0 else below
        return remote(
            sent_q.at[h, i], got_q.at[2 * h + k], q_s.at[h, i], q_r.at[2 * h + k], row, gy
        )

    def hand_e(i, b):
        return remote(
            cross.at[1, b, 1], cross.at[0, b, 1], e_s.at[i], e_r.at[i], base + o, gy
        )

    def hand_d(h, b, owner):
        part = pl.ds(3 - owner, 2)
        return remote(
            cross.at[1, b, part], cross.at[0, b, part], d_s.at[h], d_r.at[h], base + o, gy
        )

    def arrival(dst, sem):
        return remote(dst, dst, load_sem.at[0], sem, base + o, gy)

    barrier = pltpu.get_barrier_semaphore()

    def greet(there, sem, row, col):
        @pl.when(there)
        def _():
            pl.semaphore_signal(sem, inc=1, device_id=(row, col), device_id_type=MESH)

    def count(there):
        return there.astype(jnp.int32)

    pl.semaphore_signal(barrier, inc=1, device_id=(base + o, gy), device_id_type=MESH)
    for n in range(2):
        greet(has_right, barrier, base + n, right)
    greet(has_below, barrier, below, gy)
    greet(has_below & (k == 1), barrier, below + 1, gy)

    order = (0, 5, 1, 6, 2, 3, CUT, 7)
    for b in order:
        load(b).start()

    pl.semaphore_wait(barrier, 1 + 2 * count(has_left) + (2 - k) * count(has_above))
    for n in range(2):
        greet(has_left, ready_right, base + n, left)
    greet(has_above, ready_below, above + 1, gy)
    greet(has_above & (k == 0), ready_below, above, gy)

    @pl.when(has_left)
    def _():
        across(5).start()

    @pl.when(has_right)
    def _():
        pl.semaphore_wait(ready_right, 2)
        across(0).start()

    @pl.when(has_below)
    def _():
        pl.semaphore_wait(ready_below, 1 + k)

    def send(b):
        @pl.when(k != b % 2)
        def _():
            die(b // 2).start()

        there = has_above if b % 2 == 0 else has_below

        @pl.when(there & (k == b % 2))
        def _():
            vertical(b % 2, b // 2).start()

        if b not in RAW:

            @pl.when(has_right if b < CUT else has_left)
            def _():
                across(b).start()

        if b == CUT:

            @pl.when(has_right)
            def _():
                for c in range(2):
                    half(c).start()

    for n, b in enumerate(order):
        load(b).wait()
        whiten(w, OWN + b, 0, 4)
        if n >= 1:
            send(order[n - 1])
        whiten(w, OWN + b, 4, 8)

    def start_old(b, carry):
        load_old(b).start()
        return carry

    lax.fori_loop(0, BANDS, start_old, 0)

    send(order[-1])

    def pass_on(a):
        for n in range(4):
            i = ((2, 0, 1, 3), (0, 3, 1, 2))[a][n]
            arrival(w.at[OTHER + i], die_r.at[i]).wait_recv()

            @pl.when(has_below if a == 1 else has_above)
            def _():
                vertical(a, i).start()

    for a in range(2):

        @pl.when(a != k)
        def _():
            pass_on(a)

    column = lax.broadcasted_iota(jnp.int32, (ST, ST), 0)
    word = column // 30
    shift = column - word * 30
    for s in range(SLOTS):
        chosen = jnp.zeros((ST, ST), jnp.int32)
        for n in range(WORDS):
            chosen = jnp.where(word == n, bits[s * WORDS + n], chosen)
        flags = (lax.shift_right_logical(chosen, shift) & 1).astype(jnp.float32)
        mask[s] = flags.T
    pick[0] = jnp.zeros((2 * ST, ST), jnp.float32)

    def own_band(b, carry):
        real, imag = pair(w, OWN + b, OWN + b)
        cross[0, b, 0, :ST, :] = real
        cross[0, b, 0, ST:, :] = imag
        return carry

    lax.fori_loop(0, BANDS, own_band, 0)

    @pl.when(k == 0)
    def _():
        for n in range(2):
            w[RIGHT + 2 + n, :, :, :, :HB] = jnp.zeros((SEG, 2, ST, HB), jnp.bfloat16)

    def put(owner, b, code, value):
        side = jnp.where(owner == k, 0, 1)
        cross[side, b, code, :ST, :] = value[0]
        cross[side, b, code, ST:, :] = value[1]

    def common(i):
        @pl.when(has_above)
        def _():
            arrival(w.at[UPPER + i], col_r.at[i]).wait_recv()

        @pl.when(has_below)
        def _():
            arrival(w.at[LOWER + i], col_r.at[4 + i]).wait_recv()

    def own_column(i):
        def below_pair(a, carry):
            x = chip_block(a, i)
            y = jnp.where(a == 0, chip_block(1, i), LOWER + i)
            put(a, 2 * i + k, 1, pair(w, x, y))
            return carry

        lax.fori_loop(0, 2, below_pair, 0)

    def whiten_two(place):
        def whiten_one(n, carry):
            whiten(w, place + n)
            return carry

        lax.fori_loop(0, 2, whiten_one, 0)

    def partner(own, t, i):
        corner = t == 2
        y = jnp.where(corner, UPPER + 4 * own + i, chip_block(t, i))
        return y, jnp.where(corner, 2 * own, 1 + t - own)

    def from_left(h, i):
        for n in range(2):
            arrival(w.at[LEFT + 2 * h + n], row_r.at[2 * h + n]).wait_recv()

        @pl.when((h == 0) & (k == 0))
        def _():
            whiten_two(LEFT)

        def left_pair(n, carry):
            own, t = n // 3, n % 3
            y, code = partner(own, t, i)
            real, imag = pair(w, LEFT + 2 * h + own, y)
            sent_p[h, own, code, :ST, :] = real.astype(jnp.bfloat16)
            sent_p[h, own, code, ST:, :] = imag.astype(jnp.bfloat16)
            return carry

        lax.fori_loop(0, 6, left_pair, 0)
        for n in range(2):
            return_p(h, n).start()

    def from_right(h, i, b):
        cut = (h == 1) & (k == 0)

        @pl.when(cut)
        def _():
            for n in range(2):
                part = w.at[RIGHT + 2 + n, :, :, :, pl.ds(HB, HB)]
                arrival(part, row_r.at[6 + n]).wait_recv()

        @pl.when(jnp.logical_not(cut))
        def _():
            for n in range(2):
                arrival(w.at[RIGHT + 2 * h + n], row_r.at[4 + 2 * h + n]).wait_recv()

        @pl.when((h == 0) & (k == 1))
        def _():
            whiten_two(RIGHT)

        def right_corner(n, carry):
            real, imag = pair(w, UPPER + 4 * n + i, RIGHT + 2 * h + n)
            sent_q[h, n, :ST, :] = real.astype(jnp.bfloat16)
            sent_q[h, n, ST:, :] = imag.astype(jnp.bfloat16)
            return carry

        lax.fori_loop(0, 2, right_corner, 0)

        def right_pair(n, carry):
            a, far = n // 2, n % 2
            put(a, b, 3 + far - a, pair(w, chip_block(a, i), RIGHT + 2 * h + far))
            return carry

        lax.fori_loop(0, 4, right_pair, 0)

    def stage(h, carry):
        common(h)

        @pl.when(has_left)
        def _():
            from_left(h, h)

        own_column(h)
        b = turn(h, k)
        i = b // 2
        common(i)

        @pl.when(has_right)
        def _():
            from_right(h, i, b)

        hand_e(h, 2 * h + k).start()
        own_column(i)

        @pl.when(has_right)
        def _():
            hand_d(h, b, o).start()

        @pl.when(has_right & has_above)
        def _():
            return_q(h, 0).start()

        @pl.when(has_right & has_below)
        def _():
            return_q(h, 1).start()

        @pl.when(h == 1)
        def _():
            hand_e(turn(0, k) // 2, turn(0, k)).start()

        return carry

    lax.fori_loop(0, 2, stage, 0)

    def half_products(c):
        i = CUT // 2
        for n in range(2):
            part = w.at[HALF + n, :, :, pl.ds(c * HR, HR), pl.ds(0, HB)]
            arrival(part, half_r.at[c, n]).wait_recv()

        def half_pair(n, carry):
            own, t = n // 3, n % 3
            y, code = partner(own, t, i)
            real, imag = pair(w, HALF + own, y, c * HR, HR, HB)
            sent_m[own, code, 0, c * HR:(c + 1) * HR, :] = real.astype(jnp.bfloat16)
            sent_m[own, code, 1, c * HR:(c + 1) * HR, :] = imag.astype(jnp.bfloat16)
            return carry

        lax.fori_loop(0, 6, half_pair, 0)
        for n in range(2):
            return_m(c, n).start()

    def combine(b):
        load_old(b).wait()
        for s in range(SLOTS):
            which = codes[s] + 1
            flags = mask[s]
            out[s, b, :ST, :] = out[s, b, :ST, :] + flags * pick[which, :ST, :]
            out[s, b, ST:, :] = out[s, b, ST:, :] + flags * pick[which, ST:, :]

    def await_q(n, b):
        h, j = n // 2, lax.rem(n, 2)

        @pl.when(j == o)
        def _():
            arrival(cross.at[0, b, 1], e_r.at[b // 2]).wait_recv()

        @pl.when((j == o) & has_right)
        def _():
            arrival(cross.at[0, b, pl.ds(3 - k, 2)], d_r.at[h]).wait_recv()

        @pl.when(swaps & has_right)
        def _():
            arrival(got_q.at[n], q_r.at[n]).wait_recv()

    def finish_q(n):
        b = turn(n // 2, lax.rem(n, 2))
        await_q(n, b)
        pick[1] = cross[0, b, 0]
        pick[2] = cross[0, b, 1]
        pick[4] = cross[0, b, 3]
        pick[pl.ds(3 + 2 * o, 1)] = cross[0, b, pl.ds(2 + 2 * o, 1)]
        pick[pl.ds(3 + 2 * k, 1)] = got_q[pl.ds(n, 1)].astype(jnp.float32)
        combine(b)

    finish_q(0)
    hand_e(turn(1, k) // 2, turn(1, k)).start()
    finish_q(1)

    @pl.when(has_left & (k == 0))
    def _():
        for c in range(2):
            half_products(c)

    finish_q(3)

    def finish_p(b, carry):
        i, j = b // 2, lax.rem(b, 2)

        @pl.when(j == o)
        def _():
            arrival(cross.at[0, b, 1], e_r.at[i]).wait_recv()

        @pl.when(has_right)
        def _():
            arrival(got_p.at[b], p_r.at[b]).wait_recv()

        pick[1] = cross[0, b, 0]
        pick[2] = cross[0, b, 1]
        for n in range(3):
            pick[3 + n] = got_p[b, n].astype(jnp.float32)
        combine(b)
        return carry

    lax.fori_loop(0, 4, finish_p, 0)

    await_q(2, CUT)

    @pl.when(has_right)
    def _():
        for c in range(2):
            arrival(got_m.at[:, :, pl.ds(c * HR, HR)], m_r.at[c]).wait_recv()

    pick[1] = cross[0, CUT, 0]
    pick[2] = cross[0, CUT, 1]
    for n in range(3):
        partial = got_m[n].reshape(2 * ST, ST).astype(jnp.float32)
        near = got_q[2].astype(jnp.float32)
        pick[3 + n] = partial + jnp.where(k * 2 == n, near, cross[0, CUT, 2 + n])
    combine(CUT)

    for i in range(4):
        die(i).wait_send()
        hand_e(i, 2 * i + k).wait_send()

    @pl.when(has_above)
    def _():
        for i in range(4):
            vertical(0, i).wait_send()

    @pl.when(has_below)
    def _():
        for i in range(4):
            vertical(1, i).wait_send()

    @pl.when(has_left)
    def _():
        for b in range(4):
            across(4 + b).wait_send()
        for h in range(2):
            for n in range(2):
                return_p(h, n).wait_send()

    @pl.when(has_left & (k == 0))
    def _():
        for c in range(2):
            for n in range(2):
                return_m(c, n).wait_send()

    @pl.when(has_right)
    def _():
        for b in range(4):
            across(b).wait_send()
        for h in range(2):
            hand_d(h, turn(h, k), o).wait_send()
        for c in range(2):
            half(c).wait_send()

    for h in range(2):

        @pl.when(has_right & has_above)
        def _():
            return_q(h, 0).wait_send()

        @pl.when(has_right & has_below)
        def _():
            return_q(h, 1).wait_send()


def body(spectra, partner_codes, range_bits, old_stacks):
    codes = partner_codes.reshape(SLOTS)
    bits = jnp.transpose(range_bits, (0, 2, 4, 1, 3)).reshape(SLOTS * WORDS, 1, ST)
    blocks = spectra.reshape(SEG, 2, ST, BANDS * BW)
    old = old_stacks.reshape(SLOTS, BANDS, 2 * ST, ST)
    dma = pltpu.SemaphoreType.DMA
    updated = pl.pallas_call(
        kernel,
        out_shape=pltpu.VMEM((SLOTS, BANDS, 2 * ST, ST), jnp.float32),
        in_specs=[
            pl.BlockSpec(memory_space=pltpu.SMEM),
            pl.BlockSpec(memory_space=pltpu.VMEM),
            pl.BlockSpec(memory_space=pl.ANY),
            pl.BlockSpec(memory_space=pl.ANY),
        ],
        out_specs=pl.BlockSpec(memory_space=pltpu.VMEM),
        scratch_shapes=[
            pltpu.VMEM((PLACES, SEG, 2, ST, BW), jnp.bfloat16),
            pltpu.VMEM((2, BANDS, SLOTS, 2 * ST, ST), jnp.float32),
            pltpu.VMEM((SLOTS, ST, ST), jnp.float32),
            pltpu.VMEM((SLOTS + 1, 2 * ST, ST), jnp.float32),
            pltpu.VMEM((2, 2, 3, 2 * ST, ST), jnp.bfloat16),
            pltpu.VMEM((4, 3, 2 * ST, ST), jnp.bfloat16),
            pltpu.VMEM((2, 2, 2 * ST, ST), jnp.bfloat16),
            pltpu.VMEM((4, 2 * ST, ST), jnp.bfloat16),
            pltpu.VMEM((2, 3, 2, ST, ST), jnp.bfloat16),
            pltpu.VMEM((3, 2, ST, ST), jnp.bfloat16),
            dma((BANDS,)), dma((BANDS,)),
            dma((4,)), dma((4,)), dma((8,)), dma((8,)), dma((2, 4)), dma((8,)),
            dma((2, 2)), dma((4,)), dma((2, 2)), dma((4,)),
            dma((4,)), dma((4,)), dma((2,)), dma((2,)),
            dma((2,)), dma((2, 2)), dma((2, 2)), dma((2,)),
            pltpu.SemaphoreType.REGULAR, pltpu.SemaphoreType.REGULAR,
        ],
        compiler_params=pltpu.CompilerParams(
            collective_id=0, has_side_effects=True, vmem_limit_bytes=52 * 1024 * 1024
        ),
    )(codes, bits, blocks, old)
    return updated.reshape(old_stacks.shape)


def solution(mesh):
    return jax.shard_map(
        body,
        mesh=mesh,
        in_specs=(
            P("gx", "gy", None, None, None, None),
            P("gx", "gy", None),
            P("gx", "gy", None, None, None),
            P("gx", "gy", None, None, None, None, None),
        ),
        out_specs=P("gx", "gy", None, None, None, None, None),
        check_vma=False,
    )
```

```python
import math

import jax
import jax.numpy as jnp
from jax import lax
from jax.experimental import pallas as pl
from jax.experimental.pallas import tpu as pltpu
from jax.sharding import PartitionSpec as P

EPSILON = 1e-06
MESH = pl.DeviceIdType.MESH
ROWS = 8
COLS = 16
ST = 128
SEG = 3
BANDS = 8
BW = 512
SLOTS = 5
WORDS = 5
SCALE = 1.0 / math.sqrt(SEG * BW)

OWN, OTHER, UPPER, LOWER, LEFT, RIGHT, HALF, PLACES = 0, 8, 12, 16, 20, 24, 28, 30
CUT = 4
RAW = (0, 5)
HR = ST // 2


def whiten(w, place, first=0, last=ST // 16):
    def rows_of(t, carry):
        rows = pl.ds(pl.multiple_of(t * 16, 16), 16)
        total = jnp.zeros((16, BW), jnp.float32)
        for s in range(SEG):
            for c in range(2):
                x = w[place, s, c, rows, :].astype(jnp.float32)
                total = total + x * x
        power = jnp.sum(total, axis=-1, keepdims=True) * (1.0 / (SEG * 2 * BW))
        gain = lax.rsqrt(power + EPSILON)
        for s in range(SEG):
            for c in range(2):
                x = w[place, s, c, rows, :].astype(jnp.float32)
                w[place, s, c, rows, :] = (x * gain).astype(jnp.bfloat16)
        return carry

    lax.fori_loop(first, last, rows_of, 0, unroll=4)


def pair(w, x, y, first=0, rows=ST, segments=SEG):
    total = None
    for s in range(segments):
        part = lax.dot_general(
            w[x, s, :, first:first + rows].reshape(2 * rows, BW),
            w[y, s].reshape(2 * ST, BW),
            (((1,), (1,)), ((), ())), preferred_element_type=jnp.float32,
        )
        total = part if total is None else total + part
    real = (total[:rows, :ST] + total[rows:, ST:]) * SCALE
    imag = (total[rows:, :ST] - total[:rows, ST:]) * SCALE
    return real, imag


def turn(h, core):
    return jnp.where(h == 0, 6 - core, CUT + 3 * core)


def kernel(
    codes, bits, spectra, old, out,
    w, cross, mask, pick, sent_p, got_p, sent_q, got_q, sent_m, got_m,
    load_sem, old_sem,
    die_s, die_r, left_s, left_r, right_s, right_r, col_s, col_r,
    p_s, p_r, q_s, q_r, e_s, e_r, d_s, d_r,
    m_s, m_r, ready_right, ready_below,
):
    gx = lax.axis_index("gx")
    gy = lax.axis_index("gy")
    k = lax.rem(gx, 2)
    o = 1 - k
    base = gx - k
    right = lax.rem(gy + 1, COLS)
    left = lax.rem(gy + COLS - 1, COLS)
    above = lax.rem(base + ROWS - 2, ROWS)
    below = lax.rem(base + 2, ROWS)
    has_left, has_right = gy > 0, gy < COLS - 1
    has_above, has_below = base > 0, base < ROWS - 2
    swaps = jnp.where(k == 0, base > 0, base < ROWS - 2)

    def remote(src, dst, send, recv, row, col):
        return pltpu.make_async_remote_copy(
            src_ref=src, dst_ref=dst, send_sem=send, recv_sem=recv,
            device_id=(row, col), device_id_type=MESH,
        )

    def load(b):
        bins = pl.ds(b * BW, BW)
        return pltpu.make_async_copy(spectra.at[:, :, :, bins], w.at[OWN + b], load_sem.at[b])

    def load_old(b):
        return pltpu.make_async_copy(old.at[:, b], out.at[:, b], old_sem.at[b])

    def die(i):
        return remote(
            w.at[OWN + 2 * i + o], w.at[OTHER + i], die_s.at[i], die_r.at[i], base + o, gy
        )

    def leftward(b):
        h, j = {6: 0, 5: 0, CUT: 1, 7: 1}[b], b % 2
        at = RIGHT + 2 * h + k
        if b == CUT:
            src, dst = w.at[OWN + b, pl.ds(1, 2)], w.at[at, pl.ds(1, 2)]
        else:
            src = spectra.at[:, :, :, pl.ds(b * BW, BW)] if b in RAW else w.at[OWN + b]
            dst = w.at[at]
        return remote(src, dst, left_s.at[h, j], left_r.at[h, k], base + j, left)

    def rightward(b, c):
        rows = pl.ds(c * HR, HR)
        h, j = b // 2, b % 2
        if b == CUT:
            src = w.at[OWN + b, pl.ds(0, 1), :, rows]
            dst = w.at[HALF + k, pl.ds(0, 1), :, rows]
        else:
            dst = w.at[LEFT + 2 * h + k, :, :, rows]
            if b in RAW:
                src = spectra.at[:, :, rows, pl.ds(b * BW, BW)]
            else:
                src = w.at[OWN + b, :, :, rows]
        return remote(src, dst, right_s.at[b, c], right_r.at[h, c, k], base + j, right)

    def return_m(c, i):
        rows = pl.ds(c * HR, HR)
        return remote(
            sent_m.at[i, :, :, rows], got_m.at[:, :, rows], m_s.at[c, i], m_r.at[c],
            base + i, left,
        )

    def chip_block(a, i):
        return jnp.where(a == k, OWN + 2 * i + k, OTHER + i)

    def vertical(a, i):
        row, at = (above, LOWER) if a == 0 else (below, UPPER)
        return remote(
            w.at[chip_block(a, i)], w.at[at + i], col_s.at[a, i], col_r.at[at + i - UPPER],
            row + k, gy,
        )

    def return_p(h, c, i):
        rows = pl.ds(c * HR, HR)
        return remote(
            sent_p.at[h, i, :, :, rows], got_p.at[2 * h + k, :, :, rows],
            p_s.at[h, c, i], p_r.at[2 * h + k, c], base + i, left,
        )

    def return_q(h, i):
        row = above + 1 if i == 0 else below
        return remote(
            sent_q.at[h, i], got_q.at[2 * h + k], q_s.at[h, i], q_r.at[2 * h + k], row, gy
        )

    def hand_e(i, b):
        return remote(
            cross.at[1, b, 1], cross.at[0, b, 1], e_s.at[i], e_r.at[i], base + o, gy
        )

    def hand_d(h, b, owner):
        part = pl.ds(3 - owner, 2)
        return remote(
            cross.at[1, b, part], cross.at[0, b, part], d_s.at[h], d_r.at[h], base + o, gy
        )

    def arrival(dst, sem):
        return remote(dst, dst, load_sem.at[0], sem, base + o, gy)

    barrier = pltpu.get_barrier_semaphore()

    def greet(there, sem, row, col):
        @pl.when(there)
        def _():
            pl.semaphore_signal(sem, inc=1, device_id=(row, col), device_id_type=MESH)

    def count(there):
        return there.astype(jnp.int32)

    pl.semaphore_signal(barrier, inc=1, device_id=(base + o, gy), device_id_type=MESH)
    for n in range(2):
        greet(has_right, barrier, base + n, right)
    greet(has_below, barrier, below, gy)
    greet(has_below & (k == 1), barrier, below + 1, gy)

    order = (0, 5, 1, 6, 2, 3, CUT, 7)
    for b in order:
        load(b).start()

    pl.semaphore_wait(barrier, 1 + 2 * count(has_left) + (2 - k) * count(has_above))
    for n in range(2):
        greet(has_left, ready_right, base + n, left)
    greet(has_above, ready_below, above + 1, gy)
    greet(has_above & (k == 0), ready_below, above, gy)

    @pl.when(has_left)
    def _():
        leftward(5).start()

    @pl.when(has_right)
    def _():
        pl.semaphore_wait(ready_right, 2)
        for c in range(2):
            rightward(0, c).start()

    @pl.when(has_below)
    def _():
        pl.semaphore_wait(ready_below, 1 + k)

    def send(b):
        @pl.when(k != b % 2)
        def _():
            die(b // 2).start()

        there = has_above if b % 2 == 0 else has_below

        @pl.when(there & (k == b % 2))
        def _():
            vertical(b % 2, b // 2).start()

        if b >= CUT and b not in RAW:

            @pl.when(has_left)
            def _():
                leftward(b).start()

        if b <= CUT and b not in RAW:

            @pl.when(has_right)
            def _():
                for c in range(2):
                    rightward(b, c).start()

    for n, b in enumerate(order):
        load(b).wait()
        whiten(w, OWN + b, 0, 4)
        if n >= 1:
            send(order[n - 1])
        whiten(w, OWN + b, 4, 8)

    def start_old(b, carry):
        load_old(b).start()
        return carry

    lax.fori_loop(0, BANDS, start_old, 0)

    send(order[-1])

    def pass_on(a):
        for n in range(4):
            i = ((2, 0, 1, 3), (0, 3, 1, 2))[a][n]
            arrival(w.at[OTHER + i], die_r.at[i]).wait_recv()

            @pl.when(has_below if a == 1 else has_above)
            def _():
                vertical(a, i).start()

    for a in range(2):

        @pl.when(a != k)
        def _():
            pass_on(a)

    column = lax.broadcasted_iota(jnp.int32, (ST, ST), 0)
    word = column // 30
    shift = column - word * 30
    for s in range(SLOTS):
        chosen = jnp.zeros((ST, ST), jnp.int32)
        for n in range(WORDS):
            chosen = jnp.where(word == n, bits[s * WORDS + n], chosen)
        flags = (lax.shift_right_logical(chosen, shift) & 1).astype(jnp.float32)
        mask[s] = flags.T
    pick[0] = jnp.zeros((2 * ST, ST), jnp.float32)

    def own_band(b, carry):
        real, imag = pair(w, OWN + b, OWN + b)
        cross[0, b, 0, :ST, :] = real
        cross[0, b, 0, ST:, :] = imag
        return carry

    lax.fori_loop(0, BANDS, own_band, 0)

    @pl.when(k == 0)
    def _():
        for n in range(2):
            w[RIGHT + 2 + n, 0] = jnp.zeros((2, ST, BW), jnp.bfloat16)

    def put(owner, b, code, value):
        side = jnp.where(owner == k, 0, 1)
        cross[side, b, code, :ST, :] = value[0]
        cross[side, b, code, ST:, :] = value[1]

    def common(i):
        @pl.when(has_above)
        def _():
            arrival(w.at[UPPER + i], col_r.at[i]).wait_recv()

        @pl.when(has_below)
        def _():
            arrival(w.at[LOWER + i], col_r.at[4 + i]).wait_recv()

    def own_column(i):
        def below_pair(n, carry):
            a = jnp.where(n == 0, o, k)
            x = chip_block(a, i)
            y = jnp.where(a == 0, chip_block(1, i), LOWER + i)
            put(a, 2 * i + k, 1, pair(w, x, y))
            return carry

        lax.fori_loop(0, 2, below_pair, 0)

    def whiten_two(place, first, last):
        def whiten_one(n, carry):
            whiten(w, place + n, first, last)
            return carry

        lax.fori_loop(0, 2, whiten_one, 0)

    def partner(own, t, i):
        corner = t == 2
        y = jnp.where(corner, UPPER + 4 * own + i, chip_block(t, i))
        return y, jnp.where(corner, 2 * own, 1 + t - own)

    def from_left(h, i):
        for c in range(2):
            for n in range(2):
                part = w.at[LEFT + 2 * h + n, :, :, pl.ds(c * HR, HR)]
                arrival(part, right_r.at[h, c, n]).wait_recv()

            @pl.when((h == 0) & (k == 0))
            def _():
                whiten_two(LEFT, 4 * c, 4 * c + 4)

            def left_pair(n, carry):
                own, t = n // 3, n % 3
                y, code = partner(own, t, i)
                real, imag = pair(w, LEFT + 2 * h + own, y, c * HR, HR)
                sent_p[h, own, code, 0, c * HR:(c + 1) * HR, :] = real.astype(jnp.bfloat16)
                sent_p[h, own, code, 1, c * HR:(c + 1) * HR, :] = imag.astype(jnp.bfloat16)
                return carry

            lax.fori_loop(0, 6, left_pair, 0)
            for n in range(2):
                return_p(h, c, n).start()

    def from_right(h, i, b):
        cut = (h == 1) & (k == 0)

        @pl.when(cut)
        def _():
            for n in range(2):
                arrival(w.at[RIGHT + 2 + n, pl.ds(1, 2)], left_r.at[1, n]).wait_recv()

        @pl.when(jnp.logical_not(cut))
        def _():
            for n in range(2):
                arrival(w.at[RIGHT + 2 * h + n], left_r.at[h, n]).wait_recv()

        @pl.when((h == 0) & (k == 1))
        def _():
            whiten_two(RIGHT, 0, ST // 16)

        def right_corner(n, carry):
            real, imag = pair(w, UPPER + 4 * n + i, RIGHT + 2 * h + n)
            sent_q[h, n, :ST, :] = real.astype(jnp.bfloat16)
            sent_q[h, n, ST:, :] = imag.astype(jnp.bfloat16)
            return carry

        lax.fori_loop(0, 2, right_corner, 0)

        def right_pair(n, carry):
            a, far = jnp.where(n < 2, o, k), n % 2
            put(a, b, 3 + far - a, pair(w, chip_block(a, i), RIGHT + 2 * h + far))
            return carry

        lax.fori_loop(0, 4, right_pair, 0)

    def stage(h, carry):
        common(h)

        @pl.when(has_left)
        def _():
            from_left(h, h)

        own_column(h)
        hand_e(h, 2 * h + k).start()
        b = turn(h, k)
        i = b // 2
        common(i)

        @pl.when(has_right)
        def _():
            from_right(h, i, b)

        own_column(i)
        hand_e(i, b).start()

        @pl.when(has_right)
        def _():
            hand_d(h, b, o).start()

        @pl.when(has_right & has_above)
        def _():
            return_q(h, 0).start()

        @pl.when(has_right & has_below)
        def _():
            return_q(h, 1).start()

        return carry

    lax.fori_loop(0, 2, stage, 0)

    def half_products(c):
        i = CUT // 2
        for n in range(2):
            part = w.at[HALF + n, pl.ds(0, 1), :, pl.ds(c * HR, HR)]
            arrival(part, right_r.at[2, c, n]).wait_recv()

        def half_pair(n, carry):
            own, t = n // 3, n % 3
            y, code = partner(own, t, i)
            real, imag = pair(w, HALF + own, y, c * HR, HR, 1)
            sent_m[own, code, 0, c * HR:(c + 1) * HR, :] = real.astype(jnp.bfloat16)
            sent_m[own, code, 1, c * HR:(c + 1) * HR, :] = imag.astype(jnp.bfloat16)
            return carry

        lax.fori_loop(0, 6, half_pair, 0)
        for n in range(2):
            return_m(c, n).start()

    def combine(b):
        load_old(b).wait()
        for s in range(SLOTS):
            which = codes[s] + 1
            flags = mask[s]
            out[s, b, :ST, :] = out[s, b, :ST, :] + flags * pick[which, :ST, :]
            out[s, b, ST:, :] = out[s, b, ST:, :] + flags * pick[which, ST:, :]

    def await_q(n, b):
        h, j = n // 2, lax.rem(n, 2)

        @pl.when(j == o)
        def _():
            arrival(cross.at[0, b, 1], e_r.at[b // 2]).wait_recv()

        @pl.when((j == o) & has_right)
        def _():
            arrival(cross.at[0, b, pl.ds(3 - k, 2)], d_r.at[h]).wait_recv()

        @pl.when(swaps & has_right)
        def _():
            arrival(got_q.at[n], q_r.at[n]).wait_recv()

    def finish_q(n):
        b = turn(n // 2, lax.rem(n, 2))
        await_q(n, b)
        pick[1] = cross[0, b, 0]
        pick[2] = cross[0, b, 1]
        pick[4] = cross[0, b, 3]
        pick[pl.ds(3 + 2 * o, 1)] = cross[0, b, pl.ds(2 + 2 * o, 1)]
        pick[pl.ds(3 + 2 * k, 1)] = got_q[pl.ds(n, 1)].astype(jnp.float32)
        combine(b)

    @pl.when(has_left & (k == 0))
    def _():
        for c in range(2):
            half_products(c)

    finish_q(0)
    finish_q(1)
    finish_q(3)

    def finish_p(b, carry):
        i, j = b // 2, lax.rem(b, 2)

        @pl.when(j == o)
        def _():
            arrival(cross.at[0, b, 1], e_r.at[i]).wait_recv()

        @pl.when(has_right)
        def _():
            for c in range(2):
                arrival(got_p.at[b, :, :, pl.ds(c * HR, HR)], p_r.at[b, c]).wait_recv()

        pick[1] = cross[0, b, 0]
        pick[2] = cross[0, b, 1]
        for n in range(3):
            pick[3 + n] = got_p[b, n].reshape(2 * ST, ST).astype(jnp.float32)
        combine(b)
        return carry

    lax.fori_loop(0, 4, finish_p, 0)

    await_q(2, CUT)

    @pl.when(has_right)
    def _():
        for c in range(2):
            arrival(got_m.at[:, :, pl.ds(c * HR, HR)], m_r.at[c]).wait_recv()

    pick[1] = cross[0, CUT, 0]
    pick[2] = cross[0, CUT, 1]
    for n in range(3):
        partial = got_m[n].reshape(2 * ST, ST).astype(jnp.float32)
        near = got_q[2].astype(jnp.float32)
        pick[3 + n] = partial + jnp.where(k * 2 == n, near, cross[0, CUT, 2 + n])
    combine(CUT)

    for i in range(4):
        die(i).wait_send()
        hand_e(i, 2 * i + k).wait_send()

    @pl.when(has_above)
    def _():
        for i in range(4):
            vertical(0, i).wait_send()

    @pl.when(has_below)
    def _():
        for i in range(4):
            vertical(1, i).wait_send()

    @pl.when(has_left)
    def _():
        for b in range(CUT, BANDS):
            leftward(b).wait_send()
        for c in range(2):
            for n in range(2):
                for h in range(2):
                    return_p(h, c, n).wait_send()

    @pl.when(has_left & (k == 0))
    def _():
        for c in range(2):
            for n in range(2):
                return_m(c, n).wait_send()

    @pl.when(has_right)
    def _():
        for b in range(CUT + 1):
            for c in range(2):
                rightward(b, c).wait_send()
        for h in range(2):
            hand_d(h, turn(h, k), o).wait_send()

    for h in range(2):

        @pl.when(has_right & has_above)
        def _():
            return_q(h, 0).wait_send()

        @pl.when(has_right & has_below)
        def _():
            return_q(h, 1).wait_send()


def body(spectra, partner_codes, range_bits, old_stacks):
    codes = partner_codes.reshape(SLOTS)
    bits = jnp.transpose(range_bits, (0, 2, 4, 1, 3)).reshape(SLOTS * WORDS, 1, ST)
    blocks = spectra.reshape(SEG, 2, ST, BANDS * BW)
    old = old_stacks.reshape(SLOTS, BANDS, 2 * ST, ST)
    dma = pltpu.SemaphoreType.DMA
    updated = pl.pallas_call(
        kernel,
        out_shape=pltpu.VMEM((SLOTS, BANDS, 2 * ST, ST), jnp.float32),
        in_specs=[
            pl.BlockSpec(memory_space=pltpu.SMEM),
            pl.BlockSpec(memory_space=pltpu.VMEM),
            pl.BlockSpec(memory_space=pl.ANY),
            pl.BlockSpec(memory_space=pl.ANY),
        ],
        out_specs=pl.BlockSpec(memory_space=pltpu.VMEM),
        scratch_shapes=[
            pltpu.VMEM((PLACES, SEG, 2, ST, BW), jnp.bfloat16),
            pltpu.VMEM((2, BANDS, SLOTS, 2 * ST, ST), jnp.float32),
            pltpu.VMEM((SLOTS, ST, ST), jnp.float32),
            pltpu.VMEM((SLOTS + 1, 2 * ST, ST), jnp.float32),
            pltpu.VMEM((2, 2, 3, 2, ST, ST), jnp.bfloat16),
            pltpu.VMEM((4, 3, 2, ST, ST), jnp.bfloat16),
            pltpu.VMEM((2, 2, 2 * ST, ST), jnp.bfloat16),
            pltpu.VMEM((4, 2 * ST, ST), jnp.bfloat16),
            pltpu.VMEM((2, 3, 2, ST, ST), jnp.bfloat16),
            pltpu.VMEM((3, 2, ST, ST), jnp.bfloat16),
            dma((BANDS,)), dma((BANDS,)),
            dma((4,)), dma((4,)), dma((2, 2)), dma((2, 2)), dma((5, 2)), dma((3, 2, 2)),
            dma((2, 4)), dma((8,)),
            dma((2, 2, 2)), dma((4, 2)), dma((2, 2)), dma((4,)),
            dma((4,)), dma((4,)), dma((2,)), dma((2,)),
            dma((2, 2)), dma((2,)),
            pltpu.SemaphoreType.REGULAR, pltpu.SemaphoreType.REGULAR,
        ],
        compiler_params=pltpu.CompilerParams(
            collective_id=0, has_side_effects=True, vmem_limit_bytes=52 * 1024 * 1024
        ),
    )(codes, bits, blocks, old)
    return updated.reshape(old_stacks.shape)


def solution(mesh):
    return jax.shard_map(
        body,
        mesh=mesh,
        in_specs=(
            P("gx", "gy", None, None, None, None),
            P("gx", "gy", None),
            P("gx", "gy", None, None, None),
            P("gx", "gy", None, None, None, None, None),
        ),
        out_specs=P("gx", "gy", None, None, None, None, None),
        check_vma=False,
    )
```

```python
import math

import jax
import jax.numpy as jnp
from jax import lax
from jax.experimental import pallas as pl
from jax.experimental.pallas import tpu as pltpu
from jax.sharding import PartitionSpec as P

EPSILON = 1e-06
MESH = pl.DeviceIdType.MESH
ROWS = 8
COLS = 16
ST = 128
SEG = 3
BANDS = 8
BW = 512
SLOTS = 5
WORDS = 5
SCALE = 1.0 / math.sqrt(SEG * BW)

OWN, OTHER, UPPER, LOWER, LEFT, RIGHT, HALF, PLACES = 0, 8, 12, 16, 20, 24, 28, 30
CUT = 4
RAW = (0, 5)
HR = ST // 2
HB = BW // 2
PIECES = 4
PR = ST // PIECES
XLINE = 4


def whiten(w, place, first=0, last=ST // 16):
    def rows_of(t, carry):
        rows = pl.ds(pl.multiple_of(t * 16, 16), 16)
        total = jnp.zeros((16, BW), jnp.float32)
        for s in range(SEG):
            for c in range(2):
                x = w[place, s, c, rows, :].astype(jnp.float32)
                total = total + x * x
        power = jnp.sum(total, axis=-1, keepdims=True) * (1.0 / (SEG * 2 * BW))
        gain = lax.rsqrt(power + EPSILON)
        for s in range(SEG):
            for c in range(2):
                x = w[place, s, c, rows, :].astype(jnp.float32)
                w[place, s, c, rows, :] = (x * gain).astype(jnp.bfloat16)
        return carry

    lax.fori_loop(first, last, rows_of, 0, unroll=4)


def pair(w, x, y, first=0, rows=ST, bins=BW):
    total = None
    for s in range(SEG):
        part = lax.dot_general(
            w[x, s, :, first:first + rows, :bins].reshape(2 * rows, bins),
            w[y, s, :, :, :bins].reshape(2 * ST, bins),
            (((1,), (1,)), ((), ())), preferred_element_type=jnp.float32,
        )
        total = part if total is None else total + part
    real = (total[:rows, :ST] + total[rows:, ST:]) * SCALE
    imag = (total[rows:, :ST] - total[:rows, ST:]) * SCALE
    return real, imag


def pairs(w, x, y, count, first, rows, bins):
    total = None
    for s in range(SEG):
        part = lax.dot_general(
            w[pl.ds(x, count), s, :, first:first + rows, :bins].reshape(count * 2 * rows, bins),
            w[y, s, :, :, :bins].reshape(2 * ST, bins),
            (((1,), (1,)), ((), ())), preferred_element_type=jnp.float32,
        )
        total = part if total is None else total + part
    products = []
    for n in range(count):
        top = total[2 * n * rows:(2 * n + 1) * rows]
        low = total[(2 * n + 1) * rows:(2 * n + 2) * rows]
        products.append(((top[:, :ST] + low[:, ST:]) * SCALE, (low[:, :ST] - top[:, ST:]) * SCALE))
    return products


def turn(h, core):
    return jnp.where(h == 0, 6 - core, CUT + 3 * core)


def kernel(
    codes, bits, spectra, old, out,
    w, cross, mask, pick, sent_p, got_p, sent_q, got_q, sent_m, got_m,
    load_sem, old_sem,
    die_s, die_r, left_s, left_r, right_s, right_r, col_s, col_r,
    p_s, p_r, q_s, q_r, e_s, e_r, d_s, d_r,
    half_s, half_r, m_s, m_r, ready_right, ready_below,
):
    gx = lax.axis_index("gx")
    gy = lax.axis_index("gy")
    k = lax.rem(gx, 2)
    o = 1 - k
    base = gx - k
    right = lax.rem(gy + 1, COLS)
    left = lax.rem(gy + COLS - 1, COLS)
    above = lax.rem(base + ROWS - 2, ROWS)
    below = lax.rem(base + 2, ROWS)
    has_left, has_right = gy > 0, gy < COLS - 1
    wrap_left = has_left & (lax.rem(gy, XLINE) == 0)
    wrap_right = has_right & (lax.rem(gy, XLINE) == XLINE - 1)
    has_above, has_below = base > 0, base < ROWS - 2
    swaps = jnp.where(k == 0, base > 0, base < ROWS - 2)

    def remote(src, dst, send, recv, row, col):
        return pltpu.make_async_remote_copy(
            src_ref=src, dst_ref=dst, send_sem=send, recv_sem=recv,
            device_id=(row, col), device_id_type=MESH,
        )

    def load(b):
        bins = pl.ds(b * BW, BW)
        return pltpu.make_async_copy(spectra.at[:, :, :, bins], w.at[OWN + b], load_sem.at[b])

    def load_old(b):
        return pltpu.make_async_copy(old.at[:, b], out.at[:, b], old_sem.at[b])

    def die(i):
        return remote(
            w.at[OWN + 2 * i + o], w.at[OTHER + i], die_s.at[i], die_r.at[i], base + o, gy
        )

    def leftward(b):
        h, j = {6: 0, 5: 0, CUT: 1, 7: 1}[b], b % 2
        at = RIGHT + 2 * h + k
        if b == CUT:
            bins = pl.ds(HB, HB)
            src, dst = w.at[OWN + b, :, :, :, bins], w.at[at, :, :, :, bins]
        else:
            src = spectra.at[:, :, :, pl.ds(b * BW, BW)] if b in RAW else w.at[OWN + b]
            dst = w.at[at]
        return remote(src, dst, left_s.at[h, j], left_r.at[h, k], base + j, left)

    def rightward(b, c):
        rows = pl.ds(c * HR, HR)
        h, j = b // 2, b % 2
        dst = w.at[LEFT + 2 * h + k, :, :, rows]
        if b in RAW:
            src = spectra.at[:, :, rows, pl.ds(b * BW, BW)]
        else:
            src = w.at[OWN + b, :, :, rows]
        return remote(src, dst, right_s.at[b, c], right_r.at[h, c, k], base + j, right)

    def half(c):
        rows, bins = pl.ds(c * PR, PR), pl.ds(0, HB)
        return remote(
            w.at[OWN + CUT, :, :, rows, bins], w.at[HALF + k, :, :, rows, bins],
            half_s.at[c], half_r.at[c, k], base, right,
        )

    def return_m(c, i):
        rows = pl.ds(c * PR, PR)
        return remote(
            sent_m.at[i, :, :, rows], got_m.at[:, :, rows], m_s.at[c, i], m_r.at[c],
            base + i, left,
        )

    def chip_block(a, i):
        return jnp.where(a == k, OWN + 2 * i + k, OTHER + i)

    def vertical(a, i):
        row, at = (above, LOWER) if a == 0 else (below, UPPER)
        return remote(
            w.at[chip_block(a, i)], w.at[at + i], col_s.at[a, i], col_r.at[at + i - UPPER],
            row + k, gy,
        )

    def return_p(h, c, i):
        rows = pl.ds(c * HR, HR)
        return remote(
            sent_p.at[h, i, :, :, rows], got_p.at[2 * h + k, :, :, rows],
            p_s.at[h, c, i], p_r.at[2 * h + k, c], base + i, left,
        )

    def return_q(h, i):
        row = above + 1 if i == 0 else below
        return remote(
            sent_q.at[h, i], got_q.at[2 * h + k], q_s.at[h, i], q_r.at[2 * h + k], row, gy
        )

    def hand_e(i, b):
        return remote(
            cross.at[1, b, 1], cross.at[0, b, 1], e_s.at[i], e_r.at[i], base + o, gy
        )

    def hand_d(h, b, owner):
        part = pl.ds(3 - owner, 2)
        return remote(
            cross.at[1, b, part], cross.at[0, b, part], d_s.at[h], d_r.at[h], base + o, gy
        )

    def arrival(dst, sem):
        return remote(dst, dst, load_sem.at[0], sem, base + o, gy)

    barrier = pltpu.get_barrier_semaphore()

    def greet(there, sem, row, col):
        @pl.when(there)
        def _():
            pl.semaphore_signal(sem, inc=1, device_id=(row, col), device_id_type=MESH)

    def count(there):
        return there.astype(jnp.int32)

    pl.semaphore_signal(barrier, inc=1, device_id=(base + o, gy), device_id_type=MESH)
    for n in range(2):
        greet(has_right, barrier, base + n, right)
        greet(wrap_left, barrier, base + n, left)
    greet(has_below, barrier, below, gy)
    greet(has_below & (k == 1), barrier, below + 1, gy)

    order = (0, 5, 1, 6, 2, 3, CUT, 7)
    for b in order[:2]:
        load(b).start()

    heard = 1 + 2 * (count(has_left) + count(wrap_right)) + (2 - k) * count(has_above)
    pl.semaphore_wait(barrier, heard)
    for n in range(2):
        greet(has_left & jnp.logical_not(wrap_left), ready_right, base + n, left)
    greet(has_above, ready_below, above + 1, gy)
    greet(has_above & (k == 0), ready_below, above, gy)

    @pl.when(has_left)
    def _():
        leftward(5).start()

    @pl.when(has_right & jnp.logical_not(wrap_right))
    def _():
        pl.semaphore_wait(ready_right, 2)

    @pl.when(has_right)
    def _():
        for c in range(2):
            rightward(0, c).start()

    for b in order[2:]:
        load(b).start()

    @pl.when(has_below)
    def _():
        pl.semaphore_wait(ready_below, 1 + k)

    def send(b):
        @pl.when(k != b % 2)
        def _():
            die(b // 2).start()

        there = has_above if b % 2 == 0 else has_below

        @pl.when(there & (k == b % 2))
        def _():
            vertical(b % 2, b // 2).start()

        if b >= CUT and b not in RAW:

            @pl.when(has_left)
            def _():
                leftward(b).start()

        if b < CUT and b not in RAW:

            @pl.when(has_right)
            def _():
                for c in range(2):
                    rightward(b, c).start()

        if b == CUT:

            @pl.when(has_right)
            def _():
                for c in range(PIECES):
                    half(c).start()

    for n, b in enumerate(order):
        load(b).wait()
        whiten(w, OWN + b, 0, 4)
        if n >= 1:
            send(order[n - 1])
        whiten(w, OWN + b, 4, 8)

    def start_old(b, carry):
        load_old(b).start()
        return carry

    lax.fori_loop(0, BANDS, start_old, 0)

    send(order[-1])

    def pass_on(a):
        for n in range(4):
            i = ((2, 0, 1, 3), (0, 3, 1, 2))[a][n]
            arrival(w.at[OTHER + i], die_r.at[i]).wait_recv()

            @pl.when(has_below if a == 1 else has_above)
            def _():
                vertical(a, i).start()

    for a in range(2):

        @pl.when(a != k)
        def _():
            pass_on(a)

    column = lax.broadcasted_iota(jnp.int32, (ST, ST), 0)
    word = column // 30
    shift = column - word * 30
    for s in range(SLOTS):
        chosen = jnp.zeros((ST, ST), jnp.int32)
        for n in range(WORDS):
            chosen = jnp.where(word == n, bits[s * WORDS + n], chosen)
        flags = (lax.shift_right_logical(chosen, shift) & 1).astype(jnp.float32)
        mask[s] = flags.T
    pick[0] = jnp.zeros((2 * ST, ST), jnp.float32)

    def own_band(b, carry):
        real, imag = pair(w, OWN + b, OWN + b)
        cross[0, b, 0, :ST, :] = real
        cross[0, b, 0, ST:, :] = imag
        return carry

    lax.fori_loop(0, BANDS, own_band, 0)

    @pl.when(k == 0)
    def _():
        for n in range(2):
            w[RIGHT + 2 + n, :, :, :, :HB] = jnp.zeros((SEG, 2, ST, HB), jnp.bfloat16)

    def put(owner, b, code, value):
        side = jnp.where(owner == k, 0, 1)
        cross[side, b, code, :ST, :] = value[0]
        cross[side, b, code, ST:, :] = value[1]

    def common(i):
        @pl.when(has_above)
        def _():
            arrival(w.at[UPPER + i], col_r.at[i]).wait_recv()

        @pl.when(has_below)
        def _():
            arrival(w.at[LOWER + i], col_r.at[4 + i]).wait_recv()

    def own_column(i):
        def below_pair(n, carry):
            a = jnp.where(n == 0, o, k)
            x = chip_block(a, i)
            y = jnp.where(a == 0, chip_block(1, i), LOWER + i)
            put(a, 2 * i + k, 1, pair(w, x, y))
            return carry

        lax.fori_loop(0, 2, below_pair, 0)

    def whiten_two(place, first, last):
        def whiten_one(n, carry):
            whiten(w, place + n, first, last)
            return carry

        lax.fori_loop(0, 2, whiten_one, 0)

    def left_products(place, i, first, rows, bins, dst):
        def store(own, code, value):
            for n in range(2):
                dst[own, code, n, first:first + rows, :] = value[n].astype(jnp.bfloat16)

        for a in range(2):
            both = pairs(w, place, chip_block(a, i), 2, first, rows, bins)
            for own in range(2):
                store(own, 1 + a - own, both[own])
        for own in range(2):
            corner = pairs(w, place + own, UPPER + 4 * own + i, 1, first, rows, bins)
            store(own, 2 * own, corner[0])

    def from_left(h, i):
        for c in range(2):
            for n in range(2):
                part = w.at[LEFT + 2 * h + n, :, :, pl.ds(c * HR, HR)]
                arrival(part, right_r.at[h, c, n]).wait_recv()

            @pl.when((h == 0) & (k == 0))
            def _():
                whiten_two(LEFT, 4 * c, 4 * c + 4)

            left_products(LEFT + 2 * h, i, c * HR, HR, BW, sent_p.at[h])
            for n in range(2):
                return_p(h, c, n).start()

    def from_right(h, i, b):
        cut = (h == 1) & (k == 0)

        @pl.when(cut)
        def _():
            for n in range(2):
                part = w.at[RIGHT + 2 + n, :, :, :, pl.ds(HB, HB)]
                arrival(part, left_r.at[1, n]).wait_recv()

        @pl.when(jnp.logical_not(cut))
        def _():
            for n in range(2):
                arrival(w.at[RIGHT + 2 * h + n], left_r.at[h, n]).wait_recv()

        @pl.when((h == 0) & (k == 1))
        def _():
            whiten_two(RIGHT, 0, ST // 16)

        def right_corner(n, carry):
            real, imag = pair(w, UPPER + 4 * n + i, RIGHT + 2 * h + n)
            sent_q[h, n, :ST, :] = real.astype(jnp.bfloat16)
            sent_q[h, n, ST:, :] = imag.astype(jnp.bfloat16)
            return carry

        lax.fori_loop(0, 2, right_corner, 0)

        def right_pair(n, carry):
            a, far = jnp.where(n < 2, o, k), n % 2
            put(a, b, 3 + far - a, pair(w, chip_block(a, i), RIGHT + 2 * h + far))
            return carry

        lax.fori_loop(0, 4, right_pair, 0)

    def stage(h, carry):
        common(h)

        @pl.when(has_left)
        def _():
            from_left(h, h)

        own_column(h)
        hand_e(h, 2 * h + k).start()
        b = turn(h, k)
        i = b // 2
        common(i)

        @pl.when(has_right)
        def _():
            from_right(h, i, b)

        own_column(i)
        hand_e(i, b).start()

        @pl.when(has_right)
        def _():
            hand_d(h, b, o).start()

        @pl.when(has_right & has_above)
        def _():
            return_q(h, 0).start()

        @pl.when(has_right & has_below)
        def _():
            return_q(h, 1).start()

        return carry

    lax.fori_loop(0, 2, stage, 0)

    def half_products(c):
        i = CUT // 2
        for n in range(2):
            part = w.at[HALF + n, :, :, pl.ds(c * PR, PR), pl.ds(0, HB)]
            arrival(part, half_r.at[c, n]).wait_recv()

        left_products(HALF, i, c * PR, PR, HB, sent_m)
        for n in range(2):
            return_m(c, n).start()

    def combine(b):
        load_old(b).wait()
        for s in range(SLOTS):
            which = codes[s] + 1
            flags = mask[s]
            out[s, b, :ST, :] = out[s, b, :ST, :] + flags * pick[which, :ST, :]
            out[s, b, ST:, :] = out[s, b, ST:, :] + flags * pick[which, ST:, :]

    def await_q(n, b):
        h, j = n // 2, lax.rem(n, 2)

        @pl.when(j == o)
        def _():
            arrival(cross.at[0, b, 1], e_r.at[b // 2]).wait_recv()

        @pl.when((j == o) & has_right)
        def _():
            arrival(cross.at[0, b, pl.ds(3 - k, 2)], d_r.at[h]).wait_recv()

        @pl.when(swaps & has_right)
        def _():
            arrival(got_q.at[n], q_r.at[n]).wait_recv()

    def finish_q(n):
        b = turn(n // 2, lax.rem(n, 2))
        await_q(n, b)
        pick[1] = cross[0, b, 0]
        pick[2] = cross[0, b, 1]
        pick[4] = cross[0, b, 3]
        pick[pl.ds(3 + 2 * o, 1)] = cross[0, b, pl.ds(2 + 2 * o, 1)]
        pick[pl.ds(3 + 2 * k, 1)] = got_q[pl.ds(n, 1)].astype(jnp.float32)
        combine(b)

    @pl.when(has_left & (k == 0))
    def _():
        for c in range(PIECES):
            half_products(c)

    finish_q(0)
    finish_q(1)
    finish_q(3)

    def finish_p(b, carry):
        i, j = b // 2, lax.rem(b, 2)

        @pl.when(j == o)
        def _():
            arrival(cross.at[0, b, 1], e_r.at[i]).wait_recv()

        @pl.when(has_right)
        def _():
            for c in range(2):
                arrival(got_p.at[b, :, :, pl.ds(c * HR, HR)], p_r.at[b, c]).wait_recv()

        pick[1] = cross[0, b, 0]
        pick[2] = cross[0, b, 1]
        for n in range(3):
            pick[3 + n] = got_p[b, n].reshape(2 * ST, ST).astype(jnp.float32)
        combine(b)
        return carry

    lax.fori_loop(0, 4, finish_p, 0)

    await_q(2, CUT)

    @pl.when(has_right)
    def _():
        for c in range(PIECES):
            arrival(got_m.at[:, :, pl.ds(c * PR, PR)], m_r.at[c]).wait_recv()

    pick[1] = cross[0, CUT, 0]
    pick[2] = cross[0, CUT, 1]
    for n in range(3):
        partial = got_m[n].reshape(2 * ST, ST).astype(jnp.float32)
        near = got_q[2].astype(jnp.float32)
        pick[3 + n] = partial + jnp.where(k * 2 == n, near, cross[0, CUT, 2 + n])
    combine(CUT)

    for i in range(4):
        die(i).wait_send()
        hand_e(i, 2 * i + k).wait_send()

    @pl.when(has_above)
    def _():
        for i in range(4):
            vertical(0, i).wait_send()

    @pl.when(has_below)
    def _():
        for i in range(4):
            vertical(1, i).wait_send()

    @pl.when(has_left)
    def _():
        for b in range(CUT, BANDS):
            leftward(b).wait_send()
        for c in range(2):
            for n in range(2):
                for h in range(2):
                    return_p(h, c, n).wait_send()

    @pl.when(has_left & (k == 0))
    def _():
        for c in range(PIECES):
            for n in range(2):
                return_m(c, n).wait_send()

    @pl.when(has_right)
    def _():
        for b in range(CUT):
            for c in range(2):
                rightward(b, c).wait_send()
        for c in range(PIECES):
            half(c).wait_send()
        for h in range(2):
            hand_d(h, turn(h, k), o).wait_send()

    for h in range(2):

        @pl.when(has_right & has_above)
        def _():
            return_q(h, 0).wait_send()

        @pl.when(has_right & has_below)
        def _():
            return_q(h, 1).wait_send()


def body(spectra, partner_codes, range_bits, old_stacks):
    codes = partner_codes.reshape(SLOTS)
    bits = jnp.transpose(range_bits, (0, 2, 4, 1, 3)).reshape(SLOTS * WORDS, 1, ST)
    blocks = spectra.reshape(SEG, 2, ST, BANDS * BW)
    old = old_stacks.reshape(SLOTS, BANDS, 2 * ST, ST)
    dma = pltpu.SemaphoreType.DMA
    updated = pl.pallas_call(
        kernel,
        out_shape=pltpu.VMEM((SLOTS, BANDS, 2 * ST, ST), jnp.float32),
        in_specs=[
            pl.BlockSpec(memory_space=pltpu.SMEM),
            pl.BlockSpec(memory_space=pltpu.VMEM),
            pl.BlockSpec(memory_space=pl.ANY),
            pl.BlockSpec(memory_space=pl.ANY),
        ],
        out_specs=pl.BlockSpec(memory_space=pltpu.VMEM),
        scratch_shapes=[
            pltpu.VMEM((PLACES, SEG, 2, ST, BW), jnp.bfloat16),
            pltpu.VMEM((2, BANDS, SLOTS, 2 * ST, ST), jnp.float32),
            pltpu.VMEM((SLOTS, ST, ST), jnp.float32),
            pltpu.VMEM((SLOTS + 1, 2 * ST, ST), jnp.float32),
            pltpu.VMEM((2, 2, 3, 2, ST, ST), jnp.bfloat16),
            pltpu.VMEM((4, 3, 2, ST, ST), jnp.bfloat16),
            pltpu.VMEM((2, 2, 2 * ST, ST), jnp.bfloat16),
            pltpu.VMEM((4, 2 * ST, ST), jnp.bfloat16),
            pltpu.VMEM((2, 3, 2, ST, ST), jnp.bfloat16),
            pltpu.VMEM((3, 2, ST, ST), jnp.bfloat16),
            dma((BANDS,)), dma((BANDS,)),
            dma((4,)), dma((4,)), dma((2, 2)), dma((2, 2)), dma((4, 2)), dma((2, 2, 2)),
            dma((2, 4)), dma((8,)),
            dma((2, 2, 2)), dma((4, 2)), dma((2, 2)), dma((4,)),
            dma((4,)), dma((4,)), dma((2,)), dma((2,)),
            dma((PIECES,)), dma((PIECES, 2)), dma((PIECES, 2)), dma((PIECES,)),
            pltpu.SemaphoreType.REGULAR, pltpu.SemaphoreType.REGULAR,
        ],
        compiler_params=pltpu.CompilerParams(
            collective_id=0, has_side_effects=True, vmem_limit_bytes=52 * 1024 * 1024
        ),
    )(codes, bits, blocks, old)
    return updated.reshape(old_stacks.shape)


def solution(mesh):
    return jax.shard_map(
        body,
        mesh=mesh,
        in_specs=(
            P("gx", "gy", None, None, None, None),
            P("gx", "gy", None),
            P("gx", "gy", None, None, None),
            P("gx", "gy", None, None, None, None, None),
        ),
        out_specs=P("gx", "gy", None, None, None, None, None),
        check_vma=False,
    )
```

```python
import math

import jax
import jax.numpy as jnp
from jax import lax
from jax.experimental import pallas as pl
from jax.experimental.pallas import tpu as pltpu
from jax.sharding import PartitionSpec as P

EPSILON = 1e-06
MESH = pl.DeviceIdType.MESH
ROWS = 8
COLS = 16
ST = 128
SEG = 3
BANDS = 8
BW = 512
SLOTS = 5
WORDS = 5
SCALE = 1.0 / math.sqrt(SEG * BW)

OWN, OTHER, UPPER, LOWER, LEFT, RIGHT, HALF, PLACES = 0, 8, 12, 16, 20, 24, 28, 30
CUT = 4
RAW = (0, 5)
HR = ST // 2
HB = BW // 2
PIECES = 4
PR = ST // PIECES
XLINE = 4


def whiten(w, place, first=0, last=ST // 16, source=None):
    source = w.at[place] if source is None else source

    def rows_of(t, carry):
        rows = pl.ds(pl.multiple_of(t * 16, 16), 16)
        total = jnp.zeros((16, BW), jnp.float32)
        for s in range(SEG):
            for c in range(2):
                x = source[s, c, rows, :].astype(jnp.float32)
                total = total + x * x
        power = jnp.sum(total, axis=-1, keepdims=True) * (1.0 / (SEG * 2 * BW))
        gain = lax.rsqrt(power + EPSILON)
        for s in range(SEG):
            for c in range(2):
                x = source[s, c, rows, :].astype(jnp.float32)
                w[place, s, c, rows, :] = (x * gain).astype(jnp.bfloat16)
        return carry

    lax.fori_loop(first, last, rows_of, 0, unroll=4)


def pair(w, x, y, first=0, rows=ST, bins=BW):
    total = None
    for s in range(SEG):
        part = lax.dot_general(
            w[x, s, :, first:first + rows, :bins].reshape(2 * rows, bins),
            w[y, s, :, :, :bins].reshape(2 * ST, bins),
            (((1,), (1,)), ((), ())), preferred_element_type=jnp.float32,
        )
        total = part if total is None else total + part
    real = (total[:rows, :ST] + total[rows:, ST:]) * SCALE
    imag = (total[rows:, :ST] - total[:rows, ST:]) * SCALE
    return real, imag


def pairs(w, x, y, count, first, rows, bins):
    total = None
    for s in range(SEG):
        part = lax.dot_general(
            w[pl.ds(x, count), s, :, first:first + rows, :bins].reshape(count * 2 * rows, bins),
            w[y, s, :, :, :bins].reshape(2 * ST, bins),
            (((1,), (1,)), ((), ())), preferred_element_type=jnp.float32,
        )
        total = part if total is None else total + part
    products = []
    for n in range(count):
        top = total[2 * n * rows:(2 * n + 1) * rows]
        low = total[(2 * n + 1) * rows:(2 * n + 2) * rows]
        products.append(((top[:, :ST] + low[:, ST:]) * SCALE, (low[:, :ST] - top[:, ST:]) * SCALE))
    return products


def turn(h, core):
    return jnp.where(h == 0, 6 - core, CUT + 3 * core)


def kernel(
    codes_in, bits_in, spectra, old, out,
    w, raw, cross, mask, pick, sent_p, got_p, sent_q, got_q, sent_m, got_m,
    load_sem, old_sem,
    die_s, die_r, left_s, left_r, right_s, right_r, col_s, col_r,
    p_s, p_r, q_s, q_r, e_s, e_r, d_s, d_r,
    half_s, half_r, m_s, m_r, ready_right, ready_below, codes, bits, small_sem,
):
    gx = lax.axis_index("gx")
    gy = lax.axis_index("gy")
    k = lax.rem(gx, 2)
    o = 1 - k
    base = gx - k
    right = lax.rem(gy + 1, COLS)
    left = lax.rem(gy + COLS - 1, COLS)
    above = lax.rem(base + ROWS - 2, ROWS)
    below = lax.rem(base + 2, ROWS)
    has_left, has_right = gy > 0, gy < COLS - 1
    wrap_left = has_left & (lax.rem(gy, XLINE) == 0)
    wrap_right = has_right & (lax.rem(gy, XLINE) == XLINE - 1)
    has_above, has_below = base > 0, base < ROWS - 2
    swaps = jnp.where(k == 0, base > 0, base < ROWS - 2)

    def remote(src, dst, send, recv, row, col):
        return pltpu.make_async_remote_copy(
            src_ref=src, dst_ref=dst, send_sem=send, recv_sem=recv,
            device_id=(row, col), device_id_type=MESH,
        )

    def load(b):
        bins = pl.ds(b * BW, BW)
        place = raw.at[RAW.index(b)] if b in RAW else w.at[OWN + b]
        return pltpu.make_async_copy(spectra.at[:, :, :, bins], place, load_sem.at[b])

    def load_old(b):
        return pltpu.make_async_copy(old.at[:, b], out.at[:, b], old_sem.at[b])

    def die(i):
        return remote(
            w.at[OWN + 2 * i + o], w.at[OTHER + i], die_s.at[i], die_r.at[i], base + o, gy
        )

    def leftward(b):
        h, j = {6: 0, 5: 0, CUT: 1, 7: 1}[b], b % 2
        at = RIGHT + 2 * h + k
        if b == CUT:
            bins = pl.ds(HB, HB)
            src, dst = w.at[OWN + b, :, :, :, bins], w.at[at, :, :, :, bins]
        else:
            src = raw.at[RAW.index(b)] if b in RAW else w.at[OWN + b]
            dst = w.at[at]
        return remote(src, dst, left_s.at[h, j], left_r.at[h, k], base + j, left)

    def rightward(b, c):
        rows = pl.ds(c * HR, HR)
        h, j = b // 2, b % 2
        dst = w.at[LEFT + 2 * h + k, :, :, rows]
        if b in RAW:
            src = raw.at[RAW.index(b), :, :, rows]
        else:
            src = w.at[OWN + b, :, :, rows]
        return remote(src, dst, right_s.at[b, c], right_r.at[h, c, k], base + j, right)

    def half(c):
        rows, bins = pl.ds(c * PR, PR), pl.ds(0, HB)
        return remote(
            w.at[OWN + CUT, :, :, rows, bins], w.at[HALF + k, :, :, rows, bins],
            half_s.at[c], half_r.at[c, k], base, right,
        )

    def return_m(c, i):
        rows = pl.ds(c * PR, PR)
        return remote(
            sent_m.at[i, :, :, rows], got_m.at[:, :, rows], m_s.at[c, i], m_r.at[c],
            base + i, left,
        )

    def chip_block(a, i):
        return jnp.where(a == k, OWN + 2 * i + k, OTHER + i)

    def vertical(a, i):
        row, at = (above, LOWER) if a == 0 else (below, UPPER)
        return remote(
            w.at[chip_block(a, i)], w.at[at + i], col_s.at[a, i], col_r.at[at + i - UPPER],
            row + k, gy,
        )

    def return_p(h, c, i):
        rows = pl.ds(c * HR, HR)
        return remote(
            sent_p.at[h, i, :, :, rows], got_p.at[2 * h + k, :, :, rows],
            p_s.at[h, c, i], p_r.at[2 * h + k, c], base + i, left,
        )

    def return_q(h, i):
        row = above + 1 if i == 0 else below
        return remote(
            sent_q.at[h, i], got_q.at[2 * h + k], q_s.at[h, i], q_r.at[2 * h + k], row, gy
        )

    def hand_e(i, b):
        return remote(
            cross.at[1, b, 1], cross.at[0, b, 1], e_s.at[i], e_r.at[i], base + o, gy
        )

    def hand_d(h, b, owner):
        part = pl.ds(3 - owner, 2)
        return remote(
            cross.at[1, b, part], cross.at[0, b, part], d_s.at[h], d_r.at[h], base + o, gy
        )

    def arrival(dst, sem):
        return remote(dst, dst, load_sem.at[0], sem, base + o, gy)

    small = (
        pltpu.make_async_copy(codes_in, codes, small_sem.at[0]),
        pltpu.make_async_copy(bits_in, bits, small_sem.at[1]),
    )
    barrier = pltpu.get_barrier_semaphore()

    def greet(there, sem, row, col):
        @pl.when(there)
        def _():
            pl.semaphore_signal(sem, inc=1, device_id=(row, col), device_id_type=MESH)

    def count(there):
        return there.astype(jnp.int32)

    pl.semaphore_signal(barrier, inc=1, device_id=(base + o, gy), device_id_type=MESH)
    for n in range(2):
        greet(has_right, barrier, base + n, right)
        greet(wrap_left, barrier, base + n, left)
    greet(has_below, barrier, below, gy)
    greet(has_below & (k == 1), barrier, below + 1, gy)

    order = (0, 5, 1, 6, 2, 3, CUT, 7)
    for b in order[:2]:
        load(b).start()

    heard = 1 + 2 * (count(has_left) + count(wrap_right)) + (2 - k) * count(has_above)
    pl.semaphore_wait(barrier, heard)
    for n in range(2):
        greet(has_left & jnp.logical_not(wrap_left), ready_right, base + n, left)
    greet(has_above, ready_below, above + 1, gy)
    greet(has_above & (k == 0), ready_below, above, gy)

    for b in RAW:
        load(b).wait()

    @pl.when(has_left)
    def _():
        leftward(5).start()

    @pl.when(has_right & jnp.logical_not(wrap_right))
    def _():
        pl.semaphore_wait(ready_right, 2)

    @pl.when(has_right)
    def _():
        for c in range(2):
            rightward(0, c).start()

    for b in order[2:]:
        load(b).start()

    @pl.when(has_below)
    def _():
        pl.semaphore_wait(ready_below, 1 + k)

    def send(b):
        @pl.when(k != b % 2)
        def _():
            die(b // 2).start()

        there = has_above if b % 2 == 0 else has_below

        @pl.when(there & (k == b % 2))
        def _():
            vertical(b % 2, b // 2).start()

        if b >= CUT and b not in RAW:

            @pl.when(has_left)
            def _():
                leftward(b).start()

        if b < CUT and b not in RAW:

            @pl.when(has_right)
            def _():
                for c in range(2):
                    rightward(b, c).start()

        if b == CUT:

            @pl.when(has_right)
            def _():
                for c in range(PIECES):
                    half(c).start()

    for n, b in enumerate(order):
        if b not in RAW:
            load(b).wait()
        source = raw.at[RAW.index(b)] if b in RAW else None
        whiten(w, OWN + b, 0, 4, source)
        if n >= 1:
            send(order[n - 1])
        whiten(w, OWN + b, 4, 8, source)

    for copy in small:
        copy.start()

    def start_old(b, carry):
        load_old(b).start()
        return carry

    lax.fori_loop(0, BANDS, start_old, 0)

    send(order[-1])

    def pass_on(a):
        for n in range(4):
            i = ((2, 0, 1, 3), (0, 3, 1, 2))[a][n]
            arrival(w.at[OTHER + i], die_r.at[i]).wait_recv()

            @pl.when(has_below if a == 1 else has_above)
            def _():
                vertical(a, i).start()

    for a in range(2):

        @pl.when(a != k)
        def _():
            pass_on(a)

    for copy in small:
        copy.wait()
    column = lax.broadcasted_iota(jnp.int32, (ST, ST), 0)
    word = column // 30
    shift = column - word * 30
    for s in range(SLOTS):
        chosen = jnp.zeros((ST, ST), jnp.int32)
        for n in range(WORDS):
            chosen = jnp.where(word == n, bits[s * WORDS + n], chosen)
        flags = (lax.shift_right_logical(chosen, shift) & 1).astype(jnp.float32)
        mask[s] = flags.T
    pick[0] = jnp.zeros((2 * ST, ST), jnp.float32)

    def own_band(b, carry):
        real, imag = pair(w, OWN + b, OWN + b)
        cross[0, b, 0, :ST, :] = real
        cross[0, b, 0, ST:, :] = imag
        return carry

    lax.fori_loop(0, BANDS, own_band, 0)

    @pl.when(k == 0)
    def _():
        for n in range(2):
            w[RIGHT + 2 + n, :, :, :, :HB] = jnp.zeros((SEG, 2, ST, HB), jnp.bfloat16)

    def put(owner, b, code, value):
        side = jnp.where(owner == k, 0, 1)
        cross[side, b, code, :ST, :] = value[0]
        cross[side, b, code, ST:, :] = value[1]

    def common(i):
        @pl.when(has_above)
        def _():
            arrival(w.at[UPPER + i], col_r.at[i]).wait_recv()

        @pl.when(has_below)
        def _():
            arrival(w.at[LOWER + i], col_r.at[4 + i]).wait_recv()

    def own_column(i):
        def below_pair(n, carry):
            a = jnp.where(n == 0, o, k)
            x = chip_block(a, i)
            y = jnp.where(a == 0, chip_block(1, i), LOWER + i)
            put(a, 2 * i + k, 1, pair(w, x, y))
            return carry

        lax.fori_loop(0, 2, below_pair, 0)

    def whiten_two(place, first, last):
        def whiten_one(n, carry):
            whiten(w, place + n, first, last)
            return carry

        lax.fori_loop(0, 2, whiten_one, 0)

    def left_products(place, i, first, rows, bins, dst):
        def store(own, code, value):
            for n in range(2):
                dst[own, code, n, first:first + rows, :] = value[n].astype(jnp.bfloat16)

        for a in range(2):
            both = pairs(w, place, chip_block(a, i), 2, first, rows, bins)
            for own in range(2):
                store(own, 1 + a - own, both[own])
        for own in range(2):
            corner = pairs(w, place + own, UPPER + 4 * own + i, 1, first, rows, bins)
            store(own, 2 * own, corner[0])

    def from_left(h, i):
        for c in range(2):
            for n in range(2):
                part = w.at[LEFT + 2 * h + n, :, :, pl.ds(c * HR, HR)]
                arrival(part, right_r.at[h, c, n]).wait_recv()

            @pl.when((h == 0) & (k == 0))
            def _():
                whiten_two(LEFT, 4 * c, 4 * c + 4)

            left_products(LEFT + 2 * h, i, c * HR, HR, BW, sent_p.at[h])
            for n in range(2):
                return_p(h, c, n).start()

    def from_right(h, i, b):
        cut = (h == 1) & (k == 0)

        @pl.when(cut)
        def _():
            for n in range(2):
                part = w.at[RIGHT + 2 + n, :, :, :, pl.ds(HB, HB)]
                arrival(part, left_r.at[1, n]).wait_recv()

        @pl.when(jnp.logical_not(cut))
        def _():
            for n in range(2):
                arrival(w.at[RIGHT + 2 * h + n], left_r.at[h, n]).wait_recv()

        @pl.when((h == 0) & (k == 1))
        def _():
            whiten_two(RIGHT, 0, ST // 16)

        def right_corner(n, carry):
            real, imag = pair(w, UPPER + 4 * n + i, RIGHT + 2 * h + n)
            sent_q[h, n, :ST, :] = real.astype(jnp.bfloat16)
            sent_q[h, n, ST:, :] = imag.astype(jnp.bfloat16)
            return carry

        lax.fori_loop(0, 2, right_corner, 0)

        def right_pair(n, carry):
            a, far = jnp.where(n < 2, o, k), n % 2
            put(a, b, 3 + far - a, pair(w, chip_block(a, i), RIGHT + 2 * h + far))
            return carry

        lax.fori_loop(0, 4, right_pair, 0)

    def stage(h, carry):
        common(h)

        @pl.when(has_left)
        def _():
            from_left(h, h)

        own_column(h)
        hand_e(h, 2 * h + k).start()
        b = turn(h, k)
        i = b // 2
        common(i)

        @pl.when(has_right)
        def _():
            from_right(h, i, b)

        own_column(i)
        hand_e(i, b).start()

        @pl.when(has_right)
        def _():
            hand_d(h, b, o).start()

        @pl.when(has_right & has_above)
        def _():
            return_q(h, 0).start()

        @pl.when(has_right & has_below)
        def _():
            return_q(h, 1).start()

        return carry

    lax.fori_loop(0, 2, stage, 0)

    def half_products(c):
        i = CUT // 2
        for n in range(2):
            part = w.at[HALF + n, :, :, pl.ds(c * PR, PR), pl.ds(0, HB)]
            arrival(part, half_r.at[c, n]).wait_recv()

        left_products(HALF, i, c * PR, PR, HB, sent_m)
        for n in range(2):
            return_m(c, n).start()

    def combine(b):
        load_old(b).wait()
        for s in range(SLOTS):
            which = codes[s] + 1
            flags = mask[s]
            out[s, b, :ST, :] = out[s, b, :ST, :] + flags * pick[which, :ST, :]
            out[s, b, ST:, :] = out[s, b, ST:, :] + flags * pick[which, ST:, :]

    def await_q(n, b):
        h, j = n // 2, lax.rem(n, 2)

        @pl.when(j == o)
        def _():
            arrival(cross.at[0, b, 1], e_r.at[b // 2]).wait_recv()

        @pl.when((j == o) & has_right)
        def _():
            arrival(cross.at[0, b, pl.ds(3 - k, 2)], d_r.at[h]).wait_recv()

        @pl.when(swaps & has_right)
        def _():
            arrival(got_q.at[n], q_r.at[n]).wait_recv()

    def finish_q(n):
        b = turn(n // 2, lax.rem(n, 2))
        await_q(n, b)
        pick[1] = cross[0, b, 0]
        pick[2] = cross[0, b, 1]
        pick[4] = cross[0, b, 3]
        pick[pl.ds(3 + 2 * o, 1)] = cross[0, b, pl.ds(2 + 2 * o, 1)]
        pick[pl.ds(3 + 2 * k, 1)] = got_q[pl.ds(n, 1)].astype(jnp.float32)
        combine(b)

    @pl.when(has_left & (k == 0))
    def _():
        for c in range(PIECES):
            half_products(c)

    finish_q(0)
    finish_q(1)
    finish_q(3)

    def finish_p(b, carry):
        i, j = b // 2, lax.rem(b, 2)

        @pl.when(j == o)
        def _():
            arrival(cross.at[0, b, 1], e_r.at[i]).wait_recv()

        @pl.when(has_right)
        def _():
            for c in range(2):
                arrival(got_p.at[b, :, :, pl.ds(c * HR, HR)], p_r.at[b, c]).wait_recv()

        pick[1] = cross[0, b, 0]
        pick[2] = cross[0, b, 1]
        for n in range(3):
            pick[3 + n] = got_p[b, n].reshape(2 * ST, ST).astype(jnp.float32)
        combine(b)
        return carry

    lax.fori_loop(0, 4, finish_p, 0)

    await_q(2, CUT)
    load_old(CUT).wait()
    pick[1] = cross[0, CUT, 0]
    pick[2] = cross[0, CUT, 1]
    near = got_q[2].astype(jnp.float32)
    for n in range(3):
        pick[3 + n] = jnp.where(k * 2 == n, near, cross[0, CUT, 2 + n])

    for c in range(PIECES):

        @pl.when(has_right)
        def _():
            arrival(got_m.at[:, :, pl.ds(c * PR, PR)], m_r.at[c]).wait_recv()

        for part in range(2):
            rows = slice(c * PR, (c + 1) * PR)
            both = slice(part * ST + c * PR, part * ST + (c + 1) * PR)
            for n in range(3):
                pick[3 + n, both] = pick[3 + n, both] + got_m[n, part, rows].astype(jnp.float32)
            for s in range(SLOTS):
                which = codes[s] + 1
                out[s, CUT, both] = out[s, CUT, both] + mask[s, rows] * pick[which, both]

    for i in range(4):
        die(i).wait_send()
        hand_e(i, 2 * i + k).wait_send()

    @pl.when(has_above)
    def _():
        for i in range(4):
            vertical(0, i).wait_send()

    @pl.when(has_below)
    def _():
        for i in range(4):
            vertical(1, i).wait_send()

    @pl.when(has_left)
    def _():
        for b in range(CUT, BANDS):
            leftward(b).wait_send()
        for c in range(2):
            for n in range(2):
                for h in range(2):
                    return_p(h, c, n).wait_send()

    @pl.when(has_left & (k == 0))
    def _():
        for c in range(PIECES):
            for n in range(2):
                return_m(c, n).wait_send()

    @pl.when(has_right)
    def _():
        for b in range(CUT):
            for c in range(2):
                rightward(b, c).wait_send()
        for c in range(PIECES):
            half(c).wait_send()
        for h in range(2):
            hand_d(h, turn(h, k), o).wait_send()

    for h in range(2):

        @pl.when(has_right & has_above)
        def _():
            return_q(h, 0).wait_send()

        @pl.when(has_right & has_below)
        def _():
            return_q(h, 1).wait_send()


def body(spectra, partner_codes, range_bits, old_stacks):
    codes = partner_codes.reshape(SLOTS)
    bits = jnp.transpose(range_bits, (0, 2, 4, 1, 3)).reshape(SLOTS * WORDS, 1, ST)
    blocks = spectra.reshape(SEG, 2, ST, BANDS * BW)
    old = old_stacks.reshape(SLOTS, BANDS, 2 * ST, ST)
    dma = pltpu.SemaphoreType.DMA
    updated = pl.pallas_call(
        kernel,
        out_shape=pltpu.VMEM((SLOTS, BANDS, 2 * ST, ST), jnp.float32),
        in_specs=[
            pl.BlockSpec(memory_space=pl.ANY),
            pl.BlockSpec(memory_space=pl.ANY),
            pl.BlockSpec(memory_space=pl.ANY),
            pl.BlockSpec(memory_space=pl.ANY),
        ],
        out_specs=pl.BlockSpec(memory_space=pltpu.VMEM),
        scratch_shapes=[
            pltpu.VMEM((PLACES, SEG, 2, ST, BW), jnp.bfloat16),
            pltpu.VMEM((len(RAW), SEG, 2, ST, BW), jnp.bfloat16),
            pltpu.VMEM((2, BANDS, SLOTS, 2 * ST, ST), jnp.float32),
            pltpu.VMEM((SLOTS, ST, ST), jnp.float32),
            pltpu.VMEM((SLOTS + 1, 2 * ST, ST), jnp.float32),
            pltpu.VMEM((2, 2, 3, 2, ST, ST), jnp.bfloat16),
            pltpu.VMEM((4, 3, 2, ST, ST), jnp.bfloat16),
            pltpu.VMEM((2, 2, 2 * ST, ST), jnp.bfloat16),
            pltpu.VMEM((4, 2 * ST, ST), jnp.bfloat16),
            pltpu.VMEM((2, 3, 2, ST, ST), jnp.bfloat16),
            pltpu.VMEM((3, 2, ST, ST), jnp.bfloat16),
            dma((BANDS,)), dma((BANDS,)),
            dma((4,)), dma((4,)), dma((2, 2)), dma((2, 2)), dma((4, 2)), dma((2, 2, 2)),
            dma((2, 4)), dma((8,)),
            dma((2, 2, 2)), dma((4, 2)), dma((2, 2)), dma((4,)),
            dma((4,)), dma((4,)), dma((2,)), dma((2,)),
            dma((PIECES,)), dma((PIECES, 2)), dma((PIECES, 2)), dma((PIECES,)),
            pltpu.SemaphoreType.REGULAR, pltpu.SemaphoreType.REGULAR,
            pltpu.SMEM((SLOTS,), jnp.int32),
            pltpu.VMEM((SLOTS * WORDS, 1, ST), jnp.int32),
            dma((2,)),
        ],
        compiler_params=pltpu.CompilerParams(
            collective_id=0, has_side_effects=True, vmem_limit_bytes=52 * 1024 * 1024
        ),
    )(codes, bits, blocks, old)
    return updated.reshape(old_stacks.shape)


def solution(mesh):
    return jax.shard_map(
        body,
        mesh=mesh,
        in_specs=(
            P("gx", "gy", None, None, None, None),
            P("gx", "gy", None),
            P("gx", "gy", None, None, None),
            P("gx", "gy", None, None, None, None, None),
        ),
        out_specs=P("gx", "gy", None, None, None, None, None),
        check_vma=False,
    )
```

```python
import math

import jax
import jax.numpy as jnp
from jax import lax
from jax.experimental import pallas as pl
from jax.experimental.pallas import tpu as pltpu
from jax.sharding import PartitionSpec as P

EPSILON = 1e-06
MESH = pl.DeviceIdType.MESH
ROWS = 8
COLS = 16
ST = 128
SEG = 3
BANDS = 8
BW = 512
SLOTS = 5
WORDS = 5
SCALE = 1.0 / math.sqrt(SEG * BW)

OWN, OTHER, UPPER, LOWER, LEFT, RIGHT, HALF, PLACES = 0, 8, 12, 16, 20, 24, 28, 30
CUT = 4
RAW = (0, 5)
HR = ST // 2
HB = BW // 2
PIECES = 4
PR = ST // PIECES
XLINE = 4


def whiten(w, place, first=0, last=ST // 16, source=None):
    source = w.at[place] if source is None else source

    def rows_of(t, carry):
        rows = pl.ds(pl.multiple_of(t * 16, 16), 16)
        total = jnp.zeros((16, BW), jnp.float32)
        for s in range(SEG):
            for c in range(2):
                x = source[s, c, rows, :].astype(jnp.float32)
                total = total + x * x
        power = jnp.sum(total, axis=-1, keepdims=True) * (1.0 / (SEG * 2 * BW))
        gain = lax.rsqrt(power + EPSILON)
        for s in range(SEG):
            for c in range(2):
                x = source[s, c, rows, :].astype(jnp.float32)
                w[place, s, c, rows, :] = (x * gain).astype(jnp.bfloat16)
        return carry

    lax.fori_loop(first, last, rows_of, 0, unroll=4)


def pair(w, x, y, first=0, rows=ST, bins=BW):
    total = None
    for s in range(SEG):
        part = lax.dot_general(
            w[x, s, :, first:first + rows, :bins].reshape(2 * rows, bins),
            w[y, s, :, :, :bins].reshape(2 * ST, bins),
            (((1,), (1,)), ((), ())), preferred_element_type=jnp.float32,
        )
        total = part if total is None else total + part
    real = (total[:rows, :ST] + total[rows:, ST:]) * SCALE
    imag = (total[rows:, :ST] - total[:rows, ST:]) * SCALE
    return real, imag


def pairs(w, x, y, count, first, rows, bins):
    total = None
    for s in range(SEG):
        part = lax.dot_general(
            w[pl.ds(x, count), s, :, first:first + rows, :bins].reshape(count * 2 * rows, bins),
            w[y, s, :, :, :bins].reshape(2 * ST, bins),
            (((1,), (1,)), ((), ())), preferred_element_type=jnp.float32,
        )
        total = part if total is None else total + part
    products = []
    for n in range(count):
        top = total[2 * n * rows:(2 * n + 1) * rows]
        low = total[(2 * n + 1) * rows:(2 * n + 2) * rows]
        products.append(((top[:, :ST] + low[:, ST:]) * SCALE, (low[:, :ST] - top[:, ST:]) * SCALE))
    return products


def turn(h, core):
    return jnp.where(h == 0, 6 - core, CUT + 3 * core)


def kernel(
    codes_in, bits_in, spectra, old, out,
    w, raw, cross, mask, pick, sent_p, got_p, sent_q, got_q, sent_m, got_m,
    load_sem, old_sem,
    die_s, die_r, left_s, left_r, right_s, right_r, col_s, col_r,
    p_s, p_r, q_s, q_r, e_s, e_r, d_s, d_r,
    half_s, half_r, m_s, m_r, ready_right, ready_below, codes, bits, small_sem,
):
    gx = lax.axis_index("gx")
    gy = lax.axis_index("gy")
    k = lax.rem(gx, 2)
    o = 1 - k
    base = gx - k
    right = lax.rem(gy + 1, COLS)
    left = lax.rem(gy + COLS - 1, COLS)
    above = lax.rem(base + ROWS - 2, ROWS)
    below = lax.rem(base + 2, ROWS)
    has_left, has_right = gy > 0, gy < COLS - 1
    wrap_left = has_left
    wrap_right = has_right
    has_above, has_below = base > 0, base < ROWS - 2
    swaps = jnp.where(k == 0, base > 0, base < ROWS - 2)

    def remote(src, dst, send, recv, row, col):
        return pltpu.make_async_remote_copy(
            src_ref=src, dst_ref=dst, send_sem=send, recv_sem=recv,
            device_id=(row, col), device_id_type=MESH,
        )

    def load(b):
        bins = pl.ds(b * BW, BW)
        place = raw.at[RAW.index(b)] if b in RAW else w.at[OWN + b]
        return pltpu.make_async_copy(spectra.at[:, :, :, bins], place, load_sem.at[b])

    def load_old(b):
        return pltpu.make_async_copy(old.at[:, b], out.at[:, b], old_sem.at[b])

    def die(i):
        return remote(
            w.at[OWN + 2 * i + o], w.at[OTHER + i], die_s.at[i], die_r.at[i], base + o, gy
        )

    def leftward(b):
        h, j = {6: 0, 5: 0, CUT: 1, 7: 1}[b], b % 2
        at = RIGHT + 2 * h + k
        if b == CUT:
            bins = pl.ds(HB, HB)
            src, dst = w.at[OWN + b, :, :, :, bins], w.at[at, :, :, :, bins]
        else:
            src = raw.at[RAW.index(b)] if b in RAW else w.at[OWN + b]
            dst = w.at[at]
        return remote(src, dst, left_s.at[h, j], left_r.at[h, k], base + j, left)

    def rightward(b, c):
        rows = pl.ds(c * HR, HR)
        h, j = b // 2, b % 2
        dst = w.at[LEFT + 2 * h + k, :, :, rows]
        if b in RAW:
            src = raw.at[RAW.index(b), :, :, rows]
        else:
            src = w.at[OWN + b, :, :, rows]
        return remote(src, dst, right_s.at[b, c], right_r.at[h, c, k], base + j, right)

    def half(c):
        rows, bins = pl.ds(c * PR, PR), pl.ds(0, HB)
        return remote(
            w.at[OWN + CUT, :, :, rows, bins], w.at[HALF + k, :, :, rows, bins],
            half_s.at[c], half_r.at[c, k], base, right,
        )

    def return_m(c, i):
        rows = pl.ds(c * PR, PR)
        return remote(
            sent_m.at[i, :, :, rows], got_m.at[:, :, rows], m_s.at[c, i], m_r.at[c],
            base + i, left,
        )

    def chip_block(a, i):
        return jnp.where(a == k, OWN + 2 * i + k, OTHER + i)

    def vertical(a, i):
        row, at = (above, LOWER) if a == 0 else (below, UPPER)
        return remote(
            w.at[chip_block(a, i)], w.at[at + i], col_s.at[a, i], col_r.at[at + i - UPPER],
            row + k, gy,
        )

    def return_p(h, c, i):
        rows = pl.ds(c * HR, HR)
        return remote(
            sent_p.at[h, i, :, :, rows], got_p.at[2 * h + k, :, :, rows],
            p_s.at[h, c, i], p_r.at[2 * h + k, c], base + i, left,
        )

    def return_q(h, i):
        row = above + 1 if i == 0 else below
        return remote(
            sent_q.at[h, i], got_q.at[2 * h + k], q_s.at[h, i], q_r.at[2 * h + k], row, gy
        )

    def hand_e(i, b):
        return remote(
            cross.at[1, b, 1], cross.at[0, b, 1], e_s.at[i], e_r.at[i], base + o, gy
        )

    def hand_d(h, b, owner):
        part = pl.ds(3 - owner, 2)
        return remote(
            cross.at[1, b, part], cross.at[0, b, part], d_s.at[h], d_r.at[h], base + o, gy
        )

    def arrival(dst, sem):
        return remote(dst, dst, load_sem.at[0], sem, base + o, gy)

    small = (
        pltpu.make_async_copy(codes_in, codes, small_sem.at[0]),
        pltpu.make_async_copy(bits_in, bits, small_sem.at[1]),
    )
    barrier = pltpu.get_barrier_semaphore()

    def greet(there, sem, row, col):
        @pl.when(there)
        def _():
            pl.semaphore_signal(sem, inc=1, device_id=(row, col), device_id_type=MESH)

    def count(there):
        return there.astype(jnp.int32)

    pl.semaphore_signal(barrier, inc=1, device_id=(base + o, gy), device_id_type=MESH)
    for n in range(2):
        greet(has_right, barrier, base + n, right)
        greet(wrap_left, barrier, base + n, left)
    greet(has_below, barrier, below, gy)
    greet(has_below & (k == 1), barrier, below + 1, gy)

    order = (0, 5, 1, 6, 2, 3, CUT, 7)
    for b in order[:2]:
        load(b).start()

    heard = 1 + 2 * (count(has_left) + count(wrap_right)) + (2 - k) * count(has_above)
    pl.semaphore_wait(barrier, heard)
    for n in range(2):
        greet(has_left & jnp.logical_not(wrap_left), ready_right, base + n, left)
    greet(has_above, ready_below, above + 1, gy)
    greet(has_above & (k == 0), ready_below, above, gy)

    for b in RAW:
        load(b).wait()

    @pl.when(has_left)
    def _():
        leftward(5).start()

    @pl.when(has_right & jnp.logical_not(wrap_right))
    def _():
        pl.semaphore_wait(ready_right, 2)

    @pl.when(has_right)
    def _():
        for c in range(2):
            rightward(0, c).start()

    for b in order[2:]:
        load(b).start()

    @pl.when(has_below)
    def _():
        pl.semaphore_wait(ready_below, 1 + k)

    def send(b):
        @pl.when(k != b % 2)
        def _():
            die(b // 2).start()

        there = has_above if b % 2 == 0 else has_below

        @pl.when(there & (k == b % 2))
        def _():
            vertical(b % 2, b // 2).start()

        if b >= CUT and b not in RAW:

            @pl.when(has_left)
            def _():
                leftward(b).start()

        if b < CUT and b not in RAW:

            @pl.when(has_right)
            def _():
                for c in range(2):
                    rightward(b, c).start()

        if b == CUT:

            @pl.when(has_right)
            def _():
                for c in range(PIECES):
                    half(c).start()

    for n, b in enumerate(order):
        if b not in RAW:
            load(b).wait()
        source = raw.at[RAW.index(b)] if b in RAW else None
        whiten(w, OWN + b, 0, 4, source)
        if n >= 1:
            send(order[n - 1])
        whiten(w, OWN + b, 4, 8, source)

    for copy in small:
        copy.start()

    def start_old(b, carry):
        load_old(b).start()
        return carry

    lax.fori_loop(0, BANDS, start_old, 0)

    send(order[-1])

    def pass_on(a):
        for n in range(4):
            i = ((2, 0, 1, 3), (0, 3, 1, 2))[a][n]
            arrival(w.at[OTHER + i], die_r.at[i]).wait_recv()

            @pl.when(has_below if a == 1 else has_above)
            def _():
                vertical(a, i).start()

    for a in range(2):

        @pl.when(a != k)
        def _():
            pass_on(a)

    for copy in small:
        copy.wait()
    column = lax.broadcasted_iota(jnp.int32, (ST, ST), 0)
    word = column // 30
    shift = column - word * 30
    for s in range(SLOTS):
        chosen = jnp.zeros((ST, ST), jnp.int32)
        for n in range(WORDS):
            chosen = jnp.where(word == n, bits[s * WORDS + n], chosen)
        flags = (lax.shift_right_logical(chosen, shift) & 1).astype(jnp.float32)
        mask[s] = flags.T
    pick[0] = jnp.zeros((2 * ST, ST), jnp.float32)

    def own_band(b, carry):
        real, imag = pair(w, OWN + b, OWN + b)
        cross[0, b, 0, :ST, :] = real
        cross[0, b, 0, ST:, :] = imag
        return carry

    lax.fori_loop(0, BANDS, own_band, 0)

    @pl.when(k == 0)
    def _():
        for n in range(2):
            w[RIGHT + 2 + n, :, :, :, :HB] = jnp.zeros((SEG, 2, ST, HB), jnp.bfloat16)

    def put(owner, b, code, value):
        side = jnp.where(owner == k, 0, 1)
        cross[side, b, code, :ST, :] = value[0]
        cross[side, b, code, ST:, :] = value[1]

    def common(i):
        @pl.when(has_above)
        def _():
            arrival(w.at[UPPER + i], col_r.at[i]).wait_recv()

        @pl.when(has_below)
        def _():
            arrival(w.at[LOWER + i], col_r.at[4 + i]).wait_recv()

    def own_column(i):
        def below_pair(n, carry):
            a = jnp.where(n == 0, o, k)
            x = chip_block(a, i)
            y = jnp.where(a == 0, chip_block(1, i), LOWER + i)
            put(a, 2 * i + k, 1, pair(w, x, y))
            return carry

        lax.fori_loop(0, 2, below_pair, 0)

    def whiten_two(place, first, last):
        def whiten_one(n, carry):
            whiten(w, place + n, first, last)
            return carry

        lax.fori_loop(0, 2, whiten_one, 0)

    def left_products(place, i, first, rows, bins, dst):
        def store(own, code, value):
            for n in range(2):
                dst[own, code, n, first:first + rows, :] = value[n].astype(jnp.bfloat16)

        for a in range(2):
            both = pairs(w, place, chip_block(a, i), 2, first, rows, bins)
            for own in range(2):
                store(own, 1 + a - own, both[own])
        for own in range(2):
            corner = pairs(w, place + own, UPPER + 4 * own + i, 1, first, rows, bins)
            store(own, 2 * own, corner[0])

    def from_left(h, i):
        for c in range(2):
            for n in range(2):
                part = w.at[LEFT + 2 * h + n, :, :, pl.ds(c * HR, HR)]
                arrival(part, right_r.at[h, c, n]).wait_recv()

            @pl.when((h == 0) & (k == 0))
            def _():
                whiten_two(LEFT, 4 * c, 4 * c + 4)

            left_products(LEFT + 2 * h, i, c * HR, HR, BW, sent_p.at[h])
            for n in range(2):
                return_p(h, c, n).start()

    def from_right(h, i, b):
        cut = (h == 1) & (k == 0)

        @pl.when(cut)
        def _():
            for n in range(2):
                part = w.at[RIGHT + 2 + n, :, :, :, pl.ds(HB, HB)]
                arrival(part, left_r.at[1, n]).wait_recv()

        @pl.when(jnp.logical_not(cut))
        def _():
            for n in range(2):
                arrival(w.at[RIGHT + 2 * h + n], left_r.at[h, n]).wait_recv()

        @pl.when((h == 0) & (k == 1))
        def _():
            whiten_two(RIGHT, 0, ST // 16)

        def right_corner(n, carry):
            real, imag = pair(w, UPPER + 4 * n + i, RIGHT + 2 * h + n)
            sent_q[h, n, :ST, :] = real.astype(jnp.bfloat16)
            sent_q[h, n, ST:, :] = imag.astype(jnp.bfloat16)
            return carry

        lax.fori_loop(0, 2, right_corner, 0)

        def right_pair(n, carry):
            a, far = jnp.where(n < 2, o, k), n % 2
            put(a, b, 3 + far - a, pair(w, chip_block(a, i), RIGHT + 2 * h + far))
            return carry

        lax.fori_loop(0, 4, right_pair, 0)

    def stage(h, carry):
        common(h)

        @pl.when(has_left)
        def _():
            from_left(h, h)

        own_column(h)
        hand_e(h, 2 * h + k).start()
        b = turn(h, k)
        i = b // 2
        common(i)

        @pl.when(has_right)
        def _():
            from_right(h, i, b)

        own_column(i)
        hand_e(i, b).start()

        @pl.when(has_right)
        def _():
            hand_d(h, b, o).start()

        @pl.when(has_right & has_above)
        def _():
            return_q(h, 0).start()

        @pl.when(has_right & has_below)
        def _():
            return_q(h, 1).start()

        return carry

    lax.fori_loop(0, 2, stage, 0)

    def half_products(c):
        i = CUT // 2
        for n in range(2):
            part = w.at[HALF + n, :, :, pl.ds(c * PR, PR), pl.ds(0, HB)]
            arrival(part, half_r.at[c, n]).wait_recv()

        left_products(HALF, i, c * PR, PR, HB, sent_m)
        for n in range(2):
            return_m(c, n).start()

    def combine(b):
        load_old(b).wait()
        for s in range(SLOTS):
            which = codes[s] + 1
            flags = mask[s]
            out[s, b, :ST, :] = out[s, b, :ST, :] + flags * pick[which, :ST, :]
            out[s, b, ST:, :] = out[s, b, ST:, :] + flags * pick[which, ST:, :]

    def await_q(n, b):
        h, j = n // 2, lax.rem(n, 2)

        @pl.when(j == o)
        def _():
            arrival(cross.at[0, b, 1], e_r.at[b // 2]).wait_recv()

        @pl.when((j == o) & has_right)
        def _():
            arrival(cross.at[0, b, pl.ds(3 - k, 2)], d_r.at[h]).wait_recv()

        @pl.when(swaps & has_right)
        def _():
            arrival(got_q.at[n], q_r.at[n]).wait_recv()

    def finish_q(n):
        b = turn(n // 2, lax.rem(n, 2))
        await_q(n, b)
        pick[1] = cross[0, b, 0]
        pick[2] = cross[0, b, 1]
        pick[4] = cross[0, b, 3]
        pick[pl.ds(3 + 2 * o, 1)] = cross[0, b, pl.ds(2 + 2 * o, 1)]
        pick[pl.ds(3 + 2 * k, 1)] = got_q[pl.ds(n, 1)].astype(jnp.float32)
        combine(b)

    @pl.when(has_left & (k == 0))
    def _():
        for c in range(PIECES):
            half_products(c)

    finish_q(0)
    finish_q(1)
    finish_q(3)

    def finish_p(b, carry):
        i, j = b // 2, lax.rem(b, 2)

        @pl.when(j == o)
        def _():
            arrival(cross.at[0, b, 1], e_r.at[i]).wait_recv()

        @pl.when(has_right)
        def _():
            for c in range(2):
                arrival(got_p.at[b, :, :, pl.ds(c * HR, HR)], p_r.at[b, c]).wait_recv()

        pick[1] = cross[0, b, 0]
        pick[2] = cross[0, b, 1]
        for n in range(3):
            pick[3 + n] = got_p[b, n].reshape(2 * ST, ST).astype(jnp.float32)
        combine(b)
        return carry

    lax.fori_loop(0, 4, finish_p, 0)

    await_q(2, CUT)
    load_old(CUT).wait()
    pick[1] = cross[0, CUT, 0]
    pick[2] = cross[0, CUT, 1]
    near = got_q[2].astype(jnp.float32)
    for n in range(3):
        pick[3 + n] = jnp.where(k * 2 == n, near, cross[0, CUT, 2 + n])

    for c in range(PIECES):

        @pl.when(has_right)
        def _():
            arrival(got_m.at[:, :, pl.ds(c * PR, PR)], m_r.at[c]).wait_recv()

        for part in range(2):
            rows = slice(c * PR, (c + 1) * PR)
            both = slice(part * ST + c * PR, part * ST + (c + 1) * PR)
            for n in range(3):
                pick[3 + n, both] = pick[3 + n, both] + got_m[n, part, rows].astype(jnp.float32)
            for s in range(SLOTS):
                which = codes[s] + 1
                out[s, CUT, both] = out[s, CUT, both] + mask[s, rows] * pick[which, both]

    for i in range(4):
        die(i).wait_send()
        hand_e(i, 2 * i + k).wait_send()

    @pl.when(has_above)
    def _():
        for i in range(4):
            vertical(0, i).wait_send()

    @pl.when(has_below)
    def _():
        for i in range(4):
            vertical(1, i).wait_send()

    @pl.when(has_left)
    def _():
        for b in range(CUT, BANDS):
            leftward(b).wait_send()
        for c in range(2):
            for n in range(2):
                for h in range(2):
                    return_p(h, c, n).wait_send()

    @pl.when(has_left & (k == 0))
    def _():
        for c in range(PIECES):
            for n in range(2):
                return_m(c, n).wait_send()

    @pl.when(has_right)
    def _():
        for b in range(CUT):
            for c in range(2):
                rightward(b, c).wait_send()
        for c in range(PIECES):
            half(c).wait_send()
        for h in range(2):
            hand_d(h, turn(h, k), o).wait_send()

    for h in range(2):

        @pl.when(has_right & has_above)
        def _():
            return_q(h, 0).wait_send()

        @pl.when(has_right & has_below)
        def _():
            return_q(h, 1).wait_send()


def body(spectra, partner_codes, range_bits, old_stacks):
    codes = partner_codes.reshape(SLOTS)
    bits = jnp.transpose(range_bits, (0, 2, 4, 1, 3)).reshape(SLOTS * WORDS, 1, ST)
    blocks = spectra.reshape(SEG, 2, ST, BANDS * BW)
    old = old_stacks.reshape(SLOTS, BANDS, 2 * ST, ST)
    dma = pltpu.SemaphoreType.DMA
    updated = pl.pallas_call(
        kernel,
        out_shape=pltpu.VMEM((SLOTS, BANDS, 2 * ST, ST), jnp.float32),
        in_specs=[
            pl.BlockSpec(memory_space=pl.ANY),
            pl.BlockSpec(memory_space=pl.ANY),
            pl.BlockSpec(memory_space=pl.ANY),
            pl.BlockSpec(memory_space=pl.ANY),
        ],
        out_specs=pl.BlockSpec(memory_space=pltpu.VMEM),
        scratch_shapes=[
            pltpu.VMEM((PLACES, SEG, 2, ST, BW), jnp.bfloat16),
            pltpu.VMEM((len(RAW), SEG, 2, ST, BW), jnp.bfloat16),
            pltpu.VMEM((2, BANDS, SLOTS, 2 * ST, ST), jnp.float32),
            pltpu.VMEM((SLOTS, ST, ST), jnp.float32),
            pltpu.VMEM((SLOTS + 1, 2 * ST, ST), jnp.float32),
            pltpu.VMEM((2, 2, 3, 2, ST, ST), jnp.bfloat16),
            pltpu.VMEM((4, 3, 2, ST, ST), jnp.bfloat16),
            pltpu.VMEM((2, 2, 2 * ST, ST), jnp.bfloat16),
            pltpu.VMEM((4, 2 * ST, ST), jnp.bfloat16),
            pltpu.VMEM((2, 3, 2, ST, ST), jnp.bfloat16),
            pltpu.VMEM((3, 2, ST, ST), jnp.bfloat16),
            dma((BANDS,)), dma((BANDS,)),
            dma((4,)), dma((4,)), dma((2, 2)), dma((2, 2)), dma((4, 2)), dma((2, 2, 2)),
            dma((2, 4)), dma((8,)),
            dma((2, 2, 2)), dma((4, 2)), dma((2, 2)), dma((4,)),
            dma((4,)), dma((4,)), dma((2,)), dma((2,)),
            dma((PIECES,)), dma((PIECES, 2)), dma((PIECES, 2)), dma((PIECES,)),
            pltpu.SemaphoreType.REGULAR, pltpu.SemaphoreType.REGULAR,
            pltpu.SMEM((SLOTS,), jnp.int32),
            pltpu.VMEM((SLOTS * WORDS, 1, ST), jnp.int32),
            dma((2,)),
        ],
        compiler_params=pltpu.CompilerParams(
            collective_id=0, has_side_effects=True, vmem_limit_bytes=52 * 1024 * 1024
        ),
    )(codes, bits, blocks, old)
    return updated.reshape(old_stacks.shape)


def solution(mesh):
    return jax.shard_map(
        body,
        mesh=mesh,
        in_specs=(
            P("gx", "gy", None, None, None, None),
            P("gx", "gy", None),
            P("gx", "gy", None, None, None),
            P("gx", "gy", None, None, None, None, None),
        ),
        out_specs=P("gx", "gy", None, None, None, None, None),
        check_vma=False,
    )
```
